256 devices in a mesh: blk: 256 (over z, y, x, core).
Axes of the slice: x: 4, y: 4, z: 8, core: 2. Of those that a mesh axis runs over, the one named last changes fastest.
Arguments:
- populations: float32 [1024, 27, 4096], P('blk'), may hold values from 0.6 to 1.4
- scalars: float32 [1024, 9, 4096], P('blk'), may hold values from 0 to 1
- coarse_old: float32 [1024, 27, 512], P('blk'), may hold values from 0.6 to 1.4
- coarse_new: float32 [1024, 27, 512], P('blk'), may hold values from 0.6 to 1.4
- levels: int32 [1024], replicated, may hold values 0 or 1
- neighbours: int32 [1024, 6], P('blk'), may hold values from 0 to 1023, as said below
- relax_rates: float32 [27], replicated, may hold values from 0.5 to 1.9
- diffusivity: float32 [9], replicated, may hold values from 0.02 to 0.15
- stoichiometry: float32 [9], replicated, may hold values from -1 to 1
Outputs:
- new_populations: float32 [1024, 27, 4096], P('blk')
- new_scalars: float32 [1024, 9, 4096], P('blk')
- coarse_return: float32 [1024, 3456], P('blk')
The draws below stay inside these ranges and needn't reach their ends.
Inputs may be any that keep to these rules, and one draw needn't show every extreme that they name: `neighbours`: block k lies in slot k % 4 of device k // 4. The blocks 4 * 2 * L up to 4 * 2 * (L + 1) - 1 form layer L (0 <= L < 128), held by devices 2 L and 2 L + 1; the blocks beside a block of layer L on sides 0 to 3 lie in layer L, the one on side 4 in layer L - 1 and the one on side 5 in layer L + 1, taken modulo 128. The relation is symmetric: if m is beside k on side q, k is beside m on side q xor 1. Hence the device of every listed block is at most 3 devices from the device of block k, counting cyclically over all devices.
All inputs are finite; a program needn't handle non-finite values.
Results may differ from the reference program's by a relative error of at most 0.0001.
Values sent between devices are 32-bit elements; how exact they have to be, the bound alone decides.
No kernel may reach another device: no remote copies, remote signals or barrier semaphores. Data moves between devices by JAX's collectives and lax.ppermute only.
A program may use at most 128 MiB of HBM per device.

```python
import math
import jax
import jax.numpy as jnp
import numpy as np
from jax import lax

BLOCK_EDGE = 16
HALF_EDGE = 8
VELOCITIES = 27
SCALARS = 9
LAYER_X = 4
LAYER_Y = 2
LAYERS = 128
BLOCKS = 1024


def layer_order(layer_key):
    return jax.random.permutation(layer_key, LAYER_X * LAYER_Y)


def draw_neighbours(key, part):
    per_layer = LAYER_X * LAYER_Y
    layer_keys = jax.random.split(jax.random.fold_in(key, 17), LAYERS)
    placed = jax.vmap(layer_order)(layer_keys).astype(jnp.int32)
    inverse_place = jnp.argsort(placed, axis=1).astype(jnp.int32)
    numbers = jnp.arange(BLOCKS, dtype=jnp.int32)
    layer_index = numbers // per_layer
    position = placed[layer_index, numbers % per_layer]
    column_x = position % LAYER_X
    column_y = position // LAYER_X

    def number_at(layer_at, x_at, y_at):
        wrapped = layer_at % LAYERS
        return wrapped * per_layer + inverse_place[wrapped, y_at % LAYER_Y * LAYER_X + x_at % LAYER_X]
    columns = [number_at(layer_index, column_x - 1, column_y), number_at(layer_index, column_x + 1, column_y), number_at(layer_index, column_x, column_y - 1), number_at(layer_index, column_x, column_y + 1), number_at(layer_index - 1, column_x, column_y), number_at(layer_index + 1, column_x, column_y)]
    return jnp.stack(columns, axis=1).astype(jnp.int32)


def touch_ends(values, stream_key, least, largest):
    longest = values.shape.index(max(values.shape))
    spots = []
    for shift in (0, 1):
        where = [jax.random.randint(jax.random.fold_in(stream_key, axis), (), 0, length) for axis, length in enumerate(values.shape)]
        where[longest] = (where[longest] + shift) % values.shape[longest]
        spots.append(tuple(where))
    return values.at[spots[0]].set(least).at[spots[1]].set(largest)


def block_scale(stream_key, dims, shards, least, top_value):
    factor_of = 1.0
    for dim, parts in shards:
        heights = jax.random.uniform(jax.random.fold_in(jax.random.fold_in(stream_key, 6), dim), (parts,), jnp.float32, least / len(shards), top_value / len(shards))
        factor_of = factor_of * jnp.repeat(jnp.exp(heights), dims[dim] // parts).reshape((-1,) + (1,) * (len(dims) - 1 - dim))
    return factor_of


def setup_inputs(seed: int = 0) -> dict:
    key_list = jax.random.split(jax.random.key(seed), 10)
    return {
        "populations": jnp.clip(0.6 + 0.79999995 * jax.random.uniform(key_list[0], (BLOCKS, VELOCITIES, BLOCK_EDGE ** 3), jnp.float32) ** block_scale(key_list[0], (BLOCKS, VELOCITIES, BLOCK_EDGE ** 3), ((0, 256),), -0.2, 0.2), 0.6, 1.4),
        "scalars": jnp.clip(1.0 * jax.random.uniform(key_list[1], (BLOCKS, SCALARS, BLOCK_EDGE ** 3), jnp.float32) ** block_scale(key_list[1], (BLOCKS, SCALARS, BLOCK_EDGE ** 3), ((0, 256),), -0.2, 0.2), 0.0, 1.0),
        "coarse_old": jnp.clip(0.6 + 0.79999995 * jax.random.uniform(key_list[2], (BLOCKS, VELOCITIES, HALF_EDGE ** 3), jnp.float32) ** block_scale(key_list[2], (BLOCKS, VELOCITIES, HALF_EDGE ** 3), ((0, 256),), -0.2, 0.2), 0.6, 1.4),
        "coarse_new": jnp.clip(0.6 + 0.79999995 * jax.random.uniform(key_list[3], (BLOCKS, VELOCITIES, HALF_EDGE ** 3), jnp.float32) ** block_scale(key_list[3], (BLOCKS, VELOCITIES, HALF_EDGE ** 3), ((0, 256),), -0.2, 0.2), 0.6, 1.4),
        "levels": touch_ends((jax.random.randint(key_list[4], (BLOCKS,), 0, 5) < 3).astype(jnp.int32), jax.random.fold_in(key_list[4], 1), 0, 1),
        "neighbours": draw_neighbours(jax.random.fold_in(key_list[9], 71), 0),
        "relax_rates": jnp.clip(jnp.exp(jax.random.uniform(key_list[6], (VELOCITIES,), jnp.float32, math.log(0.5), math.log(1.9))), 0.5, 1.9),
        "diffusivity": jnp.clip(jnp.exp(jax.random.uniform(key_list[7], (SCALARS,), jnp.float32, math.log(0.02), math.log(0.15))), 0.02, 0.15),
        "stoichiometry": jnp.clip(jax.random.uniform(key_list[8], (SCALARS,), jnp.float32, -1.0, 1.0), -1.0, 1.0),
    }


PREFACTOR = 1.0
ZELDOVICH = 4.0


def lattice_tables():
    steps_one = (-1.0, 0.0, 1.0)
    velocities = np.array([[a, b, c] for a in steps_one for b in steps_one for c in steps_one])
    weights = np.prod(np.where(velocities == 0, 2.0 / 3.0, 1.0 / 6.0), axis=1)
    vander = np.array([[1.0, 1.0, 1.0], [-1.0, 0.0, 1.0], [1.0, 0.0, 1.0]])
    moments = np.kron(np.kron(vander, vander), vander)
    inverse = np.array([[0.0, -0.5, 0.5], [1.0, 0.0, -1.0], [0.0, 0.5, 0.5]])
    inverse_moments = np.kron(np.kron(inverse, inverse), inverse)
    return velocities, weights, moments, inverse_moments


def relaxation(relax_rates):
    velocities, weights, moments, inverse_moments = lattice_tables()
    left_part = jnp.asarray(inverse_moments / weights[:, None], jnp.float32)
    right_part = jnp.asarray(moments * weights[None, :], jnp.float32)
    return jnp.dot(left_part * relax_rates[None, :], right_part, precision=lax.Precision.HIGHEST, preferred_element_type=jnp.float32)


def moment_rows():
    velocities, weights, moments, inverse_moments = lattice_tables()
    return np.concatenate([weights[None, :], (velocities * weights[:, None]).T], axis=0)


def cell_stride(direction, extent):
    return extent ** (2 - direction)


def coordinate_of(direction, extent):
    return jnp.asarray((np.arange(extent ** 3) // cell_stride(direction, extent)) % extent, jnp.int32)


def layer_of(flat, direction, upward, extent):
    index = (extent - 1) * upward
    last_axis = flat.ndim - 1
    lead = flat.shape[:-1]
    if direction == 0:
        return lax.slice_in_dim(flat, index * extent * extent, (index + 1) * extent * extent, axis=last_axis)
    if direction == 1:
        shaped = flat.reshape(lead + (extent, extent * extent))
        picked = lax.slice_in_dim(shaped, index * extent, (index + 1) * extent, axis=last_axis + 1)
        return picked.reshape(lead + (extent * extent,))
    return lax.slice_in_dim(flat, index, flat.shape[-1], stride=extent, axis=last_axis)


def spread_face(face, direction, extent):
    lead = face.shape[:-1]
    if direction == 0:
        return jnp.tile(face, (1,) * len(lead) + (extent,))
    if direction == 1:
        square_face = face.reshape(lead + (extent, extent))
        tiled = jnp.tile(square_face, (1,) * (len(lead) + 1) + (extent,))
        return tiled.reshape(lead + (extent ** 3,))
    return jnp.repeat(face, extent, axis=len(lead))


def move_up(flat, face, direction, extent):
    stride = cell_stride(direction, extent)
    lead = flat.shape[:-1]
    shifted = jnp.concatenate([jnp.zeros(lead + (stride,), flat.dtype), flat[..., :-stride]], axis=len(lead))
    return jnp.where(coordinate_of(direction, extent) == 0, spread_face(face, direction, extent), shifted)


def move_down(flat, face, direction, extent):
    stride = cell_stride(direction, extent)
    lead = flat.shape[:-1]
    shifted = jnp.concatenate([flat[..., stride:], jnp.zeros(lead + (stride,), flat.dtype)], axis=len(lead))
    return jnp.where(coordinate_of(direction, extent) == extent - 1, spread_face(face, direction, extent), shifted)


def collide(lattice_state, operator_matrix):
    blocks = lattice_state.shape[0]
    velocities, weights, moments, inverse_moments = lattice_tables()
    flattened = lattice_state.reshape(blocks, 27, -1)
    moment_sums = jnp.einsum('pi,bic->bpc', jnp.asarray(moment_rows(), jnp.float32), flattened, precision=lax.Precision.HIGHEST)
    density = moment_sums[:, 0:1]
    current = moment_sums[:, 1:4]
    projected = jnp.einsum('id,bdc->bic', jnp.asarray(velocities, jnp.float32), current, precision=lax.Precision.HIGHEST)
    square = jnp.sum(current * current, axis=1, keepdims=True)
    balance = density + 3.0 * projected + 4.5 * projected * projected - 1.5 * square
    relaxed = flattened - jnp.einsum('ik,bkc->bic', operator_matrix, flattened - balance, precision=lax.Precision.HIGHEST)
    return relaxed.reshape(lattice_state.shape)


def outgoing(relaxed, extent):
    blocks = relaxed.shape[0]
    halved = extent // 2
    face_list = []
    for facing in range(6):
        direction = facing // 2
        upward = facing % 2
        moving = lax.index_in_dim(relaxed, 2 * upward, 1 + direction, keepdims=False).reshape(blocks, 9, -1)
        layer_face = layer_of(moving, direction, upward, extent)
        grouped = layer_face.reshape(blocks, 9, halved, 2, halved, 2)
        merged = jnp.sum(grouped, axis=(3, 5)) * 0.25
        face_list.append(merged.reshape(blocks, 9, halved * halved))
    return jnp.stack(face_list, axis=1)


def enlarge(face_values, halved):
    blocks = face_values.shape[0]
    square_face = face_values.reshape(blocks, 9, halved, halved)
    grown = jnp.repeat(jnp.repeat(square_face, 2, axis=2), 2, axis=3)
    return grown.reshape(blocks, 9, 4 * halved * halved)


def crossing_faces(read, coarse_now, fine_mask, direction, extent, halved):
    blocks = read.shape[0]
    high_face = layer_of(lax.index_in_dim(read, 2, 1 + direction, False).reshape(blocks, 9, -1), direction, 1, extent)
    low_face = layer_of(lax.index_in_dim(read, 0, 1 + direction, False).reshape(blocks, 9, -1), direction, 0, extent)
    coarse_high = enlarge(layer_of(lax.index_in_dim(coarse_now, 2, 1 + direction, False).reshape(blocks, 9, -1), direction, 1, halved), halved)
    coarse_low = enlarge(layer_of(lax.index_in_dim(coarse_now, 0, 1 + direction, False).reshape(blocks, 9, -1), direction, 0, halved), halved)
    keep_fine = fine_mask[:, None, None]
    high_face = jnp.where(keep_fine, high_face, coarse_high)
    low_face = jnp.where(keep_fine, low_face, coarse_low)
    return jnp.stack([high_face, low_face], axis=1)


def apply_section(read, from_low, from_high, direction, extent):
    forward = lax.index_in_dim(read, 2, 1 + direction, False)
    backward = lax.index_in_dim(read, 0, 1 + direction, False)
    middle = lax.index_in_dim(read, 1, 1 + direction, False)
    forward = move_up(forward, from_low, direction, extent)
    backward = move_down(backward, from_high, direction, extent)
    return jnp.stack([backward, middle, forward], axis=1 + direction)


def species_rims(species, extent):
    rim_list = []
    for facing in range(6):
        rim_list.append(layer_of(species, facing // 2, facing % 2, extent))
    return jnp.stack(rim_list, axis=1)


def advance_species(species, read, halo_faces, diffusivity, stoichiometry, extent):
    blocks = species.shape[0]
    flattened = read.reshape(blocks, 27, -1)
    current = jnp.einsum('pi,bic->bpc', jnp.asarray(moment_rows()[1:4], jnp.float32), flattened, precision=lax.Precision.HIGHEST)
    drift_term = jnp.zeros_like(species)
    spread = jnp.zeros_like(species)
    for direction in range(3):
        upper_cells = move_down(species, halo_faces[:, 2 * direction + 1], direction, extent)
        lower_cells = move_up(species, halo_faces[:, 2 * direction], direction, extent)
        drift_term = drift_term + current[:, direction][:, None] * (upper_cells - lower_cells) * 0.5
        spread = spread + (upper_cells + lower_cells - 2.0 * species)
    burning = PREFACTOR * species[:, 0] * species[:, 1] * jnp.exp(ZELDOVICH * (species[:, 8] - 1.0))
    return species - drift_term + diffusivity[None, :, None] * spread + stoichiometry[None, :, None] * burning[:, None]


def reference(populations, scalars, coarse_old, coarse_new, levels, neighbours, relax_rates, diffusivity, stoichiometry):
    blocks = populations.shape[0]
    extent = BLOCK_EDGE
    halved = HALF_EDGE
    operator_matrix = relaxation(relax_rates)
    fine_mask = levels == 1
    neighbour_fine = fine_mask[neighbours]
    lattice_state = populations.reshape(blocks, 3, 3, 3, -1)
    species = scalars
    old_coarse = coarse_old.reshape(blocks, 3, 3, 3, -1)
    new_coarse = coarse_new.reshape(blocks, 3, 3, 3, -1)
    returned = jnp.zeros((blocks, 6, 9, halved * halved), jnp.float32)
    for substep in range(2):
        coarse_now = old_coarse if substep == 0 else 0.5 * (old_coarse + new_coarse)
        relaxed = collide(lattice_state, operator_matrix)
        returned = returned + 0.5 * jnp.where(fine_mask[:, None, None, None], outgoing(relaxed, extent), 0.0)
        read = relaxed
        for direction in range(3):
            face_table = crossing_faces(read, coarse_now, fine_mask, direction, extent, halved)
            from_low = face_table[neighbours[:, 2 * direction], 0].reshape(blocks, 3, 3, extent * extent)
            from_high = face_table[neighbours[:, 2 * direction + 1], 1].reshape(blocks, 3, 3, extent * extent)
            read = apply_section(read, from_low, from_high, direction, extent)
        rim_faces = species_rims(species, extent)
        halo_list = []
        for facing in range(6):
            received = rim_faces[neighbours[:, facing], facing ^ 1]
            halo_list.append(jnp.where(neighbour_fine[:, facing][:, None, None], received, rim_faces[:, facing]))
        species = advance_species(species, read, jnp.stack(halo_list, axis=1), diffusivity, stoichiometry, extent)
        lattice_state = read
    coarse_list = [returned[neighbours[:, facing], facing ^ 1] for facing in range(6)]
    coarse_return = jnp.where(fine_mask[:, None, None, None], 0.0, jnp.stack(coarse_list, axis=1)).reshape(blocks, -1)
    new_populations = jnp.where(fine_mask[:, None, None], lattice_state.reshape(populations.shape), populations)
    new_scalars = jnp.where(fine_mask[:, None, None], species, scalars)
    return new_populations, new_scalars, coarse_return
```

```python
import jax
import jax.numpy as jnp
import numpy as np
from jax import lax
from jax.experimental import pallas as pl
from jax.experimental.pallas import tpu as pltpu
from jax.sharding import PartitionSpec as P

F32 = jnp.float32
VEL = [(a, b, c) for a in (-1, 0, 1) for b in (-1, 0, 1) for c in (-1, 0, 1)]
ROWS, LANES = 32, 128
CHUNK = 8


def shape_of(*dims):
    return jax.ShapeDtypeStruct(dims, F32)


def iota(rows, axis):
    return lax.broadcasted_iota(jnp.int32, (rows, LANES), axis)


def chunk_at(v):
    return pl.ds(pl.multiple_of(v * CHUNK, CHUNK), CHUNK)


def roll_lanes(x, by):
    if isinstance(by, int):
        by = by % LANES
        if by == 0:
            return x
    return pltpu.roll(x, by, 1)


def forward_moments(values):
    out = list(values)
    for stride in (9, 3, 1):
        for i in range(27):
            if (i // stride) % 3 == 0:
                low, mid, high = out[i], out[i + stride], out[i + 2 * stride]
                both = low + high
                out[i] = both + 4.0 * mid
                out[i + stride] = high - low
                out[i + 2 * stride] = both
    return out


def plus(x, y):
    if x is None:
        return y
    return x if y is None else x + y


def minus(x, y):
    if y is None:
        return x
    return -y if x is None else x - y


def backward_moments(values):
    out = list(values)
    for stride in (9, 3, 1):
        for i in range(27):
            if (i // stride) % 3 == 0:
                m0, m1, m2 = out[i], out[i + stride], out[i + 2 * stride]
                out[i] = minus(m2, m1)
                out[i + stride] = minus(m0, m2)
                out[i + 2 * stride] = plus(m1, m2)
    return out


def collide(g, rate):
    m = forward_moments(g)
    rho = m[0]
    j = (m[9], m[3], m[1])
    square = [x * x * (1.0 / 72.0) for x in j]
    relaxed = [None] * 27
    for k in range(27):
        digits = (k // 9, (k // 3) % 3, k % 3)
        odd = [d for d in range(3) if digits[d] == 1]
        twos = [d for d in range(3) if digits[d] == 2]
        if k in (0, 9, 3, 1):
            continue
        if not odd:
            level = rho
            for d in twos:
                level = level + square[d]
        elif len(odd) == 1:
            level = j[odd[0]]
        elif len(odd) == 2:
            level = j[odd[0]] * j[odd[1]] * (1.0 / 216.0)
        else:
            level = None
        if level is not None and twos:
            level = level * (3.0 ** -len(twos))
        relaxed[k] = minus(m[k], level) * (rate(k) * (1.0 / 64.0))
    back = backward_moments(relaxed)
    post = []
    for i, c in enumerate(VEL):
        factor = 2.0 ** sum(abs(x) for x in c)
        post.append(g[i] - (back[i] if factor == 1.0 else factor * back[i]))
    return post, j


def grow_index():
    r, l = iota(CHUNK, 0), iota(CHUNK, 1)
    return (r // 4) % 2 * 64 + r % 2 * 32 + l // 32 * 8 + l % 16 // 2


def grow_row(row, index):
    return jnp.take_along_axis(jnp.broadcast_to(row, (CHUNK, LANES)), index, axis=1)


PER_BLOCK = 36
FIELDS = 4 * PER_BLOCK + 1


def begin_kernel(
    info, levels_in, near_in, rates_in, pop, scal, old, new, out,
    pops, scals, olds, news, levels, near, rates, sems,
):
    layer, core = info[0], info[1]
    small = [
        pltpu.make_async_copy(a, b, sems.at[7 + i])
        for i, (a, b) in enumerate(((levels_in, levels), (near_in, near), (rates_in, rates)))
    ]
    for copy in small:
        copy.start()
    copies = []
    for v in range(4):
        rows = pl.ds(32 * v, 32)
        copies.append(pltpu.make_async_copy(pop.at[:, rows, :], pops.at[:, rows, :], sems.at[v]))
    copies.append(pltpu.make_async_copy(old, olds, sems.at[4]))
    copies.append(pltpu.make_async_copy(new, news, sems.at[5]))
    copies.append(pltpu.make_async_copy(scal, scals, sems.at[6]))
    for copy in copies:
        copy.start()
    index = grow_index()
    for copy in small:
        copy.wait()
    row, lane = iota(CHUNK, 0), iota(CHUNK, 1)
    meta = jnp.zeros((CHUNK, LANES), F32)
    for b in range(4):
        for q in range(6):
            here = jnp.logical_and(row == b, lane == q)
            meta = jnp.where(here, near[b, q].astype(F32), meta)
    out[FIELDS - 1, 0:8, :] = meta

    def fine_of(b):
        return levels[layer * 8 + core * 4 + b] == 1

    for v in range(4):
        copies[v].wait()

        @pl.loop(0, 4)
        def _(b):
            @pl.when(fine_of(b))
            def _():
                at = pl.ds(8 * v, 8)
                from_rows = pl.ds(32 * v + b, 8, stride=4)
                post, _j = collide([pops[p, from_rows, :] for p in range(27)], lambda k: rates[k])
                for p in range(27):
                    out[b * PER_BLOCK + p, at, :] = post[p]

    for copy in copies[4:]:
        copy.wait()

    @pl.loop(0, 4)
    def _(b):
        @pl.when(fine_of(b))
        def _():
            for m in range(9):
                for v in range(4):
                    out[b * PER_BLOCK + 27 + m, pl.ds(8 * v, 8), :] = scals[m, pl.ds(32 * v + b, 8, stride=4), :]

        @pl.when(jnp.logical_not(fine_of(b)))
        def _():
            for p in range(27):
                for v in range(4):
                    before = olds[p, pl.ds(4 * v + b, 1), :]
                    after = news[p, pl.ds(4 * v + b, 1), :]
                    out[b * PER_BLOCK + 27 + p // 8, pl.ds(p % 8 * 4 + v, 1), :] = 0.5 * (before + after)
                    out[b * PER_BLOCK + p, pl.ds(8 * v, 8), :] = grow_row(before, index)


def spot(block, core):
    return (block % 8) ^ (core * 4)


def y_up(own, beside, even, group):
    turned = jnp.where(even, pltpu.roll(beside, CHUNK - 1, 0), pltpu.roll(own, 1, 0))
    return roll_lanes(jnp.where(group < 7, own, turned), 16)


def y_down(own, beside, even, group):
    turned = jnp.where(even, pltpu.roll(own, CHUNK - 1, 0), pltpu.roll(beside, 1, 0))
    return roll_lanes(jnp.where(group > 0, own, turned), -16)


def chunks(ref, *lead):
    return [ref[(*lead, pl.ds(8 * v, 8), slice(None))] for v in range(4)]


def x_up(own, beyond, row):
    turned = [pltpu.roll(x, 2, 0) for x in own]
    before = [beyond] + turned[:3]
    return [jnp.where(row < 2, a, b) for a, b in zip(before, turned)]


def x_down(own, beyond, row):
    turned = [pltpu.roll(x, CHUNK - 2, 0) for x in own]
    after = turned[1:] + [beyond]
    return [jnp.where(row >= 6, a, b) for a, b in zip(after, turned)]


def put(ref, lead, values):
    for v in range(4):
        ref[(*lead, pl.ds(8 * v, 8), slice(None))] = values[v]


def sections_xy(halves, faces, mid, dest, near, core, fine_of):
    row = iota(CHUNK, 0)
    even = row % 2 == 0
    group = iota(CHUNK, 1) // 16

    for half, field in enumerate(halves):

        @pl.loop(0, 4)
        def _(i):
            for p, c in enumerate(VEL):
                ref, lead = field(i, p)
                if c[0] == 1:
                    faces[half * 4 + i, p] = pltpu.roll(ref[(*lead, pl.ds(24, 8), slice(None))], 2, 0)
                elif c[0] == -1:
                    faces[half * 4 + i, p] = pltpu.roll(ref[(*lead, pl.ds(0, 8), slice(None))], CHUNK - 2, 0)

    for half, field in enumerate(halves):

        @pl.loop(0, 4)
        def _(i):
            b = half * 4 + i
            fine = fine_of(b)

            @pl.when(fine)
            def _():
                low, high = spot(near[b, 0], core), spot(near[b, 1], core)
                for p, c in enumerate(VEL):
                    ref, lead = field(i, p)
                    values = chunks(ref, *lead)
                    if c[0] == 1:
                        values = x_up(values, faces[low, p], row)
                    elif c[0] == -1:
                        values = x_down(values, faces[high, p], row)
                    put(mid, (b, p), values)

            @pl.when(jnp.logical_not(fine))
            def _():
                for p in range(27):
                    ref, lead = field(i, p)
                    put(mid, (b, p), chunks(ref, *lead))

    @pl.loop(0, 8)
    def _(b):
        fine = fine_of(b)

        @pl.when(fine)
        def _():
            low, high = spot(near[b, 2], core), spot(near[b, 3], core)
            for p, c in enumerate(VEL):
                for v in range(4):
                    at = pl.ds(8 * v, 8)
                    value = mid[b, p, at, :]
                    if c[1] == 1:
                        value = y_up(value, mid[low, p, at, :], even, group)
                    elif c[1] == -1:
                        value = y_down(value, mid[high, p, at, :], even, group)
                    dest[b, p, at, :] = value

        @pl.when(jnp.logical_not(fine))
        def _():
            for p in range(27):
                if VEL[p][2] != 0:
                    put(dest, (b, p), chunks(mid, b, p))


def pack_into(fields, first_slot, start, lane):
    out = None
    for e, field in enumerate(fields):
        slot = first_slot + e
        moved = roll_lanes(field, slot - start)
        out = moved if out is None else jnp.where(lane == slot, moved, out)
    return out


def halves_of(own, other):
    return [lambda i, p: (own, (i * PER_BLOCK + p,)), lambda i, p: (other, (i * PER_BLOCK + p,))]


def plane_kernel(info, levels, near, own, other, dest, up, down, table, mid, faces, meta, sem):
    layer, core = info[0], info[1]
    copy = pltpu.make_async_copy(other.at[FIELDS - 1, pl.ds(0, 8), :], meta, sem)
    copy.start()
    copy.wait()
    for i in range(4):
        for q in range(6):
            table[i, q] = near[i, q]
            table[4 + i, q] = meta[i, q].astype(jnp.int32)

    def fine_of(b):
        return levels[layer * 8 + spot(b, core)] == 1

    sections_xy(halves_of(own, other), faces, mid, dest, table, core, fine_of)
    lane = iota(CHUNK, 1) % 16

    for half, ref_in in enumerate((own, other)):

        @pl.loop(0, 4)
        def _(i):
            b = half * 4 + i
            for v in range(4):
                at = pl.ds(8 * v, 8)
                for ref, digit, start in ((up, 2, 15), (down, 0, 0)):
                    fields = [dest[b, 3 * e + digit, at, :] for e in range(9)]
                    fields += [ref_in[i * PER_BLOCK + 27 + e, at, :] for e in range(7)]
                    ref[b, at, :] = pack_into(fields, 0, start, lane)
                    held = ref[8, at, :]
                    for e in range(2):
                        slot = 2 * b + e
                        moved = pltpu.roll(ref_in[i * PER_BLOCK + 34 + e, at, :], (slot - start) % LANES, 1)
                        held = jnp.where(lane == slot, moved, held)
                    ref[8, at, :] = held


def z_section(h, up, down, depth):
    g = []
    for p, c in enumerate(VEL):
        e = p // 3
        value = h(p)
        if c[2] == 1:
            value = jnp.where(depth == 0, roll_lanes(up, -e), roll_lanes(value, 1))
        elif c[2] == -1:
            value = jnp.where(depth == 15, roll_lanes(down, 15 - e), roll_lanes(value, -1))
        g.append(value)
    return g


def species_step(y_ref, b, sides, faces, flux, flags, diffusivity, stoichiometry, store):
    row, lanes = iota(CHUNK, 0), iota(CHUNK, 1)
    even = row % 2 == 0
    group, depth = lanes // 16, lanes % 16

    def gone(edge, q):
        return jnp.logical_and(edge, flags[q] != 1)

    lost = [
        gone(row < 2, 0), gone(row >= 6, 1),
        gone(jnp.logical_and(even, group == 0), 2), gone(jnp.logical_and(jnp.logical_not(even), group == 7), 3),
        gone(depth == 0, 4), gone(depth == 15, 5),
    ]
    burning = [
        a * c * jnp.exp(4.0 * (t - 1.0))
        for a, c, t in zip(chunks(y_ref, b, 0), chunks(y_ref, b, 1), chunks(y_ref, b, 8))
    ]
    for m in range(9):
        y = chunks(y_ref, b, m)
        low_x = pltpu.roll(y_ref[sides[0], m, pl.ds(24, 8), :], 2, 0)
        high_x = pltpu.roll(y_ref[sides[1], m, pl.ds(0, 8), :], CHUNK - 2, 0)
        lower_x, upper_x = x_up(y, low_x, row), x_down(y, high_x, row)
        lower_x[0] = jnp.where(lost[0], y[0], lower_x[0])
        upper_x[3] = jnp.where(lost[1], y[3], upper_x[3])
        for v in range(4):
            at = pl.ds(8 * v, 8)
            here = y[v]
            z_low, z_high = faces(m, at)
            pairs = [
                (lower_x[v], upper_x[v]),
                (
                    jnp.where(lost[2], here, y_up(here, y_ref[sides[2], m, at, :], even, group)),
                    jnp.where(lost[3], here, y_down(here, y_ref[sides[3], m, at, :], even, group)),
                ),
                (
                    jnp.where(lost[4], here, jnp.where(depth == 0, z_low, roll_lanes(here, 1))),
                    jnp.where(lost[5], here, jnp.where(depth == 15, z_high, roll_lanes(here, -1))),
                ),
            ]
            drift = spread = None
            for d, (lower, upper) in enumerate(pairs):
                part = flux[d, at, :] * (upper - lower)
                both = upper + lower
                drift = part if drift is None else drift + part
                spread = both if spread is None else spread + both
            value = here - drift + diffusivity[m] * (spread - 6.0 * here) + stoichiometry[m] * burning[v]
            store(m, v, value)


WIDE = 640


def reduce_tables():
    l = np.arange(LANES)[:, None]
    c = np.arange(WIDE)[None, :]
    e, cell = c // 64, c % 64
    live = c < 576
    along_x = (l // 32 * 8 + l % 16 // 2 == cell % 32) & live
    along_y = [(l // 16 + 8 * a == e) & (l % 16 // 2 == cell % 8) & live for a in range(2)]
    along_z = (l % 16 == e) & (l // 32 == cell % 4) & live
    side = np.concatenate([along_x, along_y[0], along_y[1]], axis=0)
    return jnp.asarray(side, F32), jnp.asarray(along_z, F32)


def wide_iota(axis):
    return lax.broadcasted_iota(jnp.int32, (ROWS, WIDE), axis)


def times(x, w):
    return jnp.dot(x, w, precision=lax.Precision.HIGHEST, preferred_element_type=F32)


def put_pair(out, s, base, first, second):
    moved = pltpu.roll(second, 64, 1)
    out[pl.ds(s, 1), pl.ds(base, 512)] = first[:, 0:512]
    out[pl.ds(s, 1), pl.ds(base + 512, 128)] = first[:, 512:640] + moved[:, 0:128]
    out[pl.ds(s, 1), pl.ds(base + 640, 512)] = moved[:, 128:640]


def middle_kernel(
    info, levels, near, rates, diffusivity, stoichiometry, own, other, held, up_in, down_in, tables,
    flow, species, up, down, sides_out,
    first, mid, old, faces, flux, edge_x, edge_y, inverse,
):
    layer, core = info[0], info[1]
    index = grow_index()
    depth = iota(CHUNK, 1) % 16

    def fine_of(b):
        return levels[layer * 8 + spot(b, core)] == 1

    @pl.loop(0, 8)
    def _(b):
        inverse[0, spot(near[b, 5], core)] = b
        inverse[1, spot(near[b, 4], core)] = b

    for half, ref_in in enumerate((own, other)):

        @pl.loop(0, 4)
        def _(i):
            for m in range(9):
                put(old, (half * 4 + i, m), chunks(ref_in, i * PER_BLOCK + 27 + m))

            @pl.when(jnp.logical_not(fine_of(half * 4 + i)))
            def _():
                for p in range(27):
                    for v in range(4):
                        line = ref_in[i * PER_BLOCK + 27 + p // 8, pl.ds(p % 8 * 4 + v, 1), :]
                        first[half * 4 + i, p, pl.ds(8 * v, 8), :] = grow_row(line, index)

    @pl.loop(0, 8)
    def _(b):
        @pl.when(fine_of(b))
        def _():
            below, above = spot(near[b, 4], core), spot(near[b, 5], core)

            @pl.loop(0, 4)
            def _(v):
                at = chunk_at(v)
                g = z_section(lambda p: held[b, p, at, :], up_in[below, at, :], down_in[above, at, :], depth)
                post, j = collide(g, lambda k: rates[k])
                for p in range(27):
                    first[b, p, at, :] = post[p]
                for d in range(3):
                    flux[d, at, :] = j[d] * (0.5 / 216.0)

            def z_faces(m, at):
                if m < 7:
                    slot = 9 + m
                    return roll_lanes(up_in[below, at, :], -slot), roll_lanes(down_in[above, at, :], 15 - slot)
                low = LANES - 2 * below - (m - 7)
                high = (LANES + 15 - 2 * above - (m - 7)) % LANES
                return pltpu.roll(up_in[8, at, :], low, 1), pltpu.roll(down_in[8, at, :], high, 1)

            def store(m, v, value):
                species[b, m, pl.ds(8 * v, 8), :] = value

            species_step(
                old, b, [spot(near[b, q], core) for q in range(4)], z_faces, flux,
                [levels[near[b, q]] for q in range(6)], diffusivity, stoichiometry, store,
            )

        @pl.when(jnp.logical_not(fine_of(b)))
        def _():
            species[b] = jnp.zeros((9, ROWS, LANES), F32)

    sections_xy([lambda i, p: (first, (i, p)), lambda i, p: (first, (4 + i, p))], faces, mid, flow, near, core, fine_of)

    for way, (ref, digit, start) in enumerate(((up, 2, 15), (down, 0, 0))):
        for half, ref_in in enumerate((own, other)):

            @pl.loop(0, 4)
            def _(i):
                b = half * 4 + i
                target = spot(near[b, 5 - way], core)

                @pl.when(target < 4)
                def _():
                    for v in range(4):
                        at = pl.ds(8 * v, 8)
                        fields = [flow[b, 3 * e + digit, at, :] for e in range(9)]
                        fields += [species[b, e, at, :] for e in range(7)]
                        ref[2 * target, at, :] = pack_into(fields, 0, start, depth)
                        fields = [
                            0.125 * (ref_in[i * PER_BLOCK + 3 * e + digit, at, :] + first[b, 3 * e + digit, at, :])
                            for e in range(9)
                        ]
                        fields += [species[b, 7, at, :], species[b, 8, at, :]]
                        ref[2 * target + 1, at, :] = pack_into(fields, 0, start, depth)

    group, odd = iota(CHUNK, 1) // 16, iota(CHUNK, 0) % 2 == 1
    for half, ref_in in enumerate((own, other)):

        @pl.loop(0, 4)
        def _(i):
            b = half * 4 + i

            @pl.when(fine_of(b))
            def _():
                for side in range(2):
                    at = pl.ds(30, 2) if side == 0 else pl.ds(0, 2)
                    for e in range(9):
                        p = 18 + e if side == 0 else e
                        edge_x[b, side, pl.ds(2 * e, 2), :] = ref_in[i * PER_BLOCK + p, at, :] + first[b, p, at, :]
                    edge_x[b, side, pl.ds(18, 14), :] = jnp.zeros((14, LANES), F32)
                for v in range(4):
                    at = pl.ds(8 * v, 8)
                    packs = [None, None]
                    for e in range(9):
                        p_low = 9 * (e // 3) + e % 3
                        p_high = p_low + 6
                        high = ref_in[i * PER_BLOCK + p_high, at, :] + first[b, p_high, at, :]
                        low = ref_in[i * PER_BLOCK + p_low, at, :] + first[b, p_low, at, :]
                        slot = e % 8
                        both = jnp.where(odd, roll_lanes(high, 16 * (slot - 7)), roll_lanes(low, 16 * slot))
                        held_pack = packs[e // 8]
                        packs[e // 8] = both if held_pack is None else jnp.where(group == slot, both, held_pack)
                    for a in range(2):
                        edge_y[b, a, at, :] = packs[a]

    row, col = wide_iota(0), wide_iota(1)
    e_of, cell = col // 64, col % 64
    keep_x = jnp.logical_and(row // 2 == e_of, row % 2 == cell // 32)
    keep_y = row // 4 == cell // 8
    odd_row = row % 2 == 1

    for s in range(4):
        coarse = jnp.logical_not(fine_of(s))

        @pl.when(coarse)
        def _(s=s):
            weight = [jnp.where(levels[near[s, q]] == 1, 0.125, 0.0) for q in range(4)]
            at = [spot(near[s, q], core) for q in range(4)]
            rows = []
            for q in range(2):
                face = jnp.where(levels[near[s, q]] == 1, edge_x[at[q], q], 0.0)
                spread = times(face, tables[0:128, :])
                rows.append(weight[q] * jnp.sum(jnp.where(keep_x, spread, 0.0), axis=0, keepdims=True))
            put_pair(sides_out, s, 0, rows[0], rows[1])
            rows = []
            for q in (2, 3):
                fine = levels[near[s, q]] == 1
                spread = times(jnp.where(fine, edge_y[at[q], 0], 0.0), tables[128:256, :])
                spread += times(jnp.where(fine, edge_y[at[q], 1], 0.0), tables[256:384, :])
                keep = jnp.logical_and(keep_y, odd_row if q == 2 else jnp.logical_not(odd_row))
                rows.append(weight[q] * jnp.sum(jnp.where(keep, spread, 0.0), axis=0, keepdims=True))
            put_pair(sides_out, s, 1152, rows[0], rows[1])

        @pl.when(jnp.logical_not(coarse))
        def _(s=s):
            sides_out[pl.ds(s, 1), :] = jnp.zeros((1, 2304), F32)


def end_kernel(
    info, levels, near, diffusivity, stoichiometry, held, species, up_in, down_in, sides, table, pop, scal,
    pop_out, scal_out, returned,
    pops, scals, flux, sems,
):
    layer, core = info[0], info[1]
    depth = iota(CHUNK, 1) % 16
    row, col = wide_iota(0), wide_iota(1)
    keep = row // 4 * 2 + row % 2 == col % 64 // 4

    def fine_of(s):
        return levels[layer * 8 + core * 4 + s] == 1

    copies = []
    for v in range(4):
        at = pl.ds(8 * v, 8)

        @pl.loop(0, 4)
        def _(s):
            rows = pl.ds(32 * v + s, 8, stride=4)

            @pl.when(fine_of(s))
            def _():
                g = z_section(lambda p: held[s, p, at, :], up_in[2 * s, at, :], down_in[2 * s, at, :], depth)
                for p in range(27):
                    pops[p, rows, :] = g[p]
                m = forward_moments(g)
                for d, i in enumerate((9, 3, 1)):
                    flux[s, d, at, :] = m[i] * (0.5 / 216.0)

            @pl.when(jnp.logical_not(fine_of(s)))
            def _():
                for p in range(27):
                    pops[p, rows, :] = pop[p, rows, :]

        rows = pl.ds(32 * v, 32)
        copies.append(pltpu.make_async_copy(pops.at[:, rows, :], pop_out.at[:, rows, :], sems.at[v]))
        copies[-1].start()

    @pl.loop(0, 4)
    def _(s):
        @pl.when(fine_of(s))
        def _():
            def z_faces(m, at):
                a, slot = (2 * s, 9 + m) if m < 7 else (2 * s + 1, 2 + m)
                return roll_lanes(up_in[a, at, :], -slot), roll_lanes(down_in[a, at, :], 15 - slot)

            def store(m, v, value):
                scals[m, pl.ds(32 * v + s, 8, stride=4), :] = value

            species_step(
                species, s, [spot(near[s, q], core) for q in range(4)], z_faces, flux.at[s],
                [levels[near[s, q]] for q in range(6)], diffusivity, stoichiometry, store,
            )

        @pl.when(jnp.logical_not(fine_of(s)))
        def _():
            for v in range(4):
                at = pl.ds(32 * v + s, 8, stride=4)
                for m in range(9):
                    scals[m, at, :] = scal[m, at, :]

    copies.append(pltpu.make_async_copy(scals, scal_out, sems.at[4]))
    copies[-1].start()
    returned[:, 0:2304] = sides[...]
    for s in range(4):
        coarse = levels[layer * 8 + core * 4 + s] != 1

        @pl.when(coarse)
        def _(s=s):
            rows = []
            for a, ref in enumerate((up_in, down_in)):
                face = jnp.where(levels[near[s, 4 + a]] == 1, ref[2 * s + 1], 0.0)
                rows.append(jnp.sum(jnp.where(keep, times(face, table[...]), 0.0), axis=0, keepdims=True))
            put_pair(returned, s, 2304, rows[0], rows[1])

        @pl.when(jnp.logical_not(coarse))
        def _(s=s):
            returned[pl.ds(s, 1), pl.ds(2304, 1152)] = jnp.zeros((1, 1152), F32)

    for copy in copies:
        copy.wait()


def specs(kinds):
    table = {
        "s": pl.BlockSpec(memory_space=pltpu.SMEM),
        "v": pl.BlockSpec(memory_space=pltpu.VMEM),
        "h": pl.BlockSpec(memory_space=pltpu.HBM),
    }
    return [table[kind] for kind in kinds]


def call(kernel, kinds, outs, out_kinds, scratch, name, megabytes, flops):
    return pl.pallas_call(
        kernel,
        in_specs=specs(kinds),
        out_specs=specs(out_kinds),
        out_shape=outs,
        scratch_shapes=scratch,
        name=name,
        compiler_params=pltpu.CompilerParams(vmem_limit_bytes=megabytes << 20),
        cost_estimate=pl.CostEstimate(flops=flops, transcendentals=0, bytes_accessed=8 << 20),
    )


def interleave(x):
    blocks, n, cells = x.shape
    x = x.reshape(blocks, n, cells // LANES, LANES)
    return jnp.transpose(x, (1, 2, 0, 3)).reshape(n, cells // LANES * blocks, LANES)


def separate(x):
    n, rows, _ = x.shape
    x = jnp.transpose(x.reshape(n, rows // 4, 4, LANES), (2, 0, 1, 3))
    return x.reshape(4, n, rows // 4 * LANES)


def local(
    populations, scalars, coarse_old, coarse_new, levels, neighbours, relax_rates, diffusivity, stoichiometry
):
    devices = lax.axis_size("blk")
    me = lax.axis_index("blk")
    info = jnp.stack([me // 2, me % 2]).astype(jnp.int32)
    swap = [(i, i ^ 1) for i in range(devices)]
    rise = [(i, (i + 2) % devices) for i in range(devices)]
    fall = [(i, (i - 2) % devices) for i in range(devices)]

    def move(x, pairs):
        return lax.ppermute(x, "blk", pairs)

    def vmem(*lead):
        return pltpu.VMEM((*lead, ROWS, LANES), F32)

    full = (ROWS, LANES)
    pop, scal = interleave(populations), interleave(scalars)
    old, new = interleave(coarse_old), interleave(coarse_new)
    side_table, z_table = reduce_tables()
    own = call(
        begin_kernel,
        "shhhhhhh",
        [shape_of(FIELDS, *full)],
        "v",
        [pltpu.VMEM(x.shape, F32) for x in (pop, scal, old, new)]
        + [pltpu.SMEM(x.shape, x.dtype) for x in (levels, neighbours, relax_rates)]
        + [pltpu.SemaphoreType.DMA((10,))],
        "begin",
        12,
        1 << 27,
    )(info, *[pltpu.with_memory_space_constraint(x, pltpu.HBM) for x in (levels, neighbours, relax_rates, pop, scal, old, new)])[0]
    other = move(own, swap)
    face = pltpu.VMEM((8, 27, CHUNK, LANES), F32)
    held, up, down, near = call(
        plane_kernel,
        "sssvv",
        [shape_of(8, 27, *full), shape_of(9, *full), shape_of(9, *full), jax.ShapeDtypeStruct((8, 6), jnp.int32)],
        "vvvs",
        [vmem(8, 27), face, pltpu.SMEM((8, LANES), F32), pltpu.SemaphoreType.DMA],
        "plane",
        16,
        1 << 27,
    )(info, levels, neighbours, own, other)
    up_in, down_in = move(up, rise), move(down, fall)
    flow, species, up, down, sides = call(
        middle_kernel,
        "ssssssvvvvvv",
        [shape_of(8, 27, *full), shape_of(8, 9, *full), shape_of(8, *full), shape_of(8, *full), shape_of(4, 2304)],
        "vvvvv",
        [
            vmem(8, 27), vmem(8, 27), vmem(8, 9), face, vmem(3), vmem(8, 2), vmem(8, 2), pltpu.SMEM((2, 8), jnp.int32),
        ],
        "middle",
        28,
        1 << 28,
    )(info, levels, near, relax_rates, diffusivity, stoichiometry, own, other, held, up_in, down_in, side_table)
    up_in, down_in = move(up, rise), move(down, fall)
    pop_out, scal_out, returned = call(
        end_kernel,
        "sssssvvvvvvvv",
        [shape_of(27, 128, LANES), shape_of(9, 128, LANES), shape_of(4, 3456)],
        "hhv",
        [pltpu.VMEM(pop.shape, F32), pltpu.VMEM(scal.shape, F32), vmem(4, 3), pltpu.SemaphoreType.DMA((5,))],
        "end",
        20,
        1 << 27,
    )(
        info, levels, neighbours, diffusivity, stoichiometry, flow, species, up_in, down_in, sides, z_table, pop, scal
    )
    return separate(pop_out), separate(scal_out), returned


def solution(mesh):
    in_specs = (
        P("blk", None, None), P("blk", None, None), P("blk", None, None), P("blk", None, None),
        P(), P("blk", None), P(), P(), P(),
    )
    out_specs = (P("blk", None, None), P("blk", None, None), P("blk", None))
    return jax.shard_map(local, mesh=mesh, in_specs=in_specs, out_specs=out_specs, check_vma=False)
```

```python
import jax
import jax.numpy as jnp
import numpy as np
from jax import lax
from jax.experimental import pallas as pl
from jax.experimental.pallas import tpu as pltpu
from jax.sharding import PartitionSpec as P

F32 = jnp.float32
VEL = [(a, b, c) for a in (-1, 0, 1) for b in (-1, 0, 1) for c in (-1, 0, 1)]
ROWS, LANES = 32, 128
CHUNK = 8


def shape_of(*dims):
    return jax.ShapeDtypeStruct(dims, F32)


def iota(rows, axis):
    return lax.broadcasted_iota(jnp.int32, (rows, LANES), axis)


def chunk_at(v):
    return pl.ds(pl.multiple_of(v * CHUNK, CHUNK), CHUNK)


def roll_lanes(x, by):
    if isinstance(by, int):
        by = by % LANES
        if by == 0:
            return x
    return pltpu.roll(x, by, 1)


def forward_moments(values):
    out = list(values)
    for stride in (9, 3, 1):
        for i in range(27):
            if (i // stride) % 3 == 0:
                low, mid, high = out[i], out[i + stride], out[i + 2 * stride]
                both = low + high
                out[i] = both + 4.0 * mid
                out[i + stride] = high - low
                out[i + 2 * stride] = both
    return out


def plus(x, y):
    if x is None:
        return y
    return x if y is None else x + y


def minus(x, y):
    if y is None:
        return x
    return -y if x is None else x - y


def backward_moments(values):
    out = list(values)
    for stride in (9, 3, 1):
        for i in range(27):
            if (i // stride) % 3 == 0:
                m0, m1, m2 = out[i], out[i + stride], out[i + 2 * stride]
                out[i] = minus(m2, m1)
                out[i + stride] = minus(m0, m2)
                out[i + 2 * stride] = plus(m1, m2)
    return out


def collide(g, rate):
    m = forward_moments(g)
    rho = m[0]
    j = (m[9], m[3], m[1])
    square = [x * x * (1.0 / 72.0) for x in j]
    relaxed = [None] * 27
    for k in range(27):
        digits = (k // 9, (k // 3) % 3, k % 3)
        odd = [d for d in range(3) if digits[d] == 1]
        twos = [d for d in range(3) if digits[d] == 2]
        if k in (0, 9, 3, 1):
            continue
        if not odd:
            level = rho
            for d in twos:
                level = level + square[d]
        elif len(odd) == 1:
            level = j[odd[0]]
        elif len(odd) == 2:
            level = j[odd[0]] * j[odd[1]] * (1.0 / 216.0)
        else:
            level = None
        if level is not None and twos:
            level = level * (3.0 ** -len(twos))
        relaxed[k] = minus(m[k], level) * (rate(k) * (1.0 / 64.0))
    back = backward_moments(relaxed)
    post = []
    for i, c in enumerate(VEL):
        factor = 2.0 ** sum(abs(x) for x in c)
        post.append(g[i] - (back[i] if factor == 1.0 else factor * back[i]))
    return post, j


def grow_index():
    r, l = iota(CHUNK, 0), iota(CHUNK, 1)
    return (r // 4) % 2 * 64 + r % 2 * 32 + l // 32 * 8 + l % 16 // 2


def grow_row(row, index):
    return jnp.take_along_axis(jnp.broadcast_to(row, (CHUNK, LANES)), index, axis=1)


PER_BLOCK = 36
FIELDS = 4 * PER_BLOCK + 1


def begin_kernel(
    info, levels_in, near_in, rates_in, pop, scal, old, new, out, up, down,
    pops, scals, olds, news, levels, near, rates, sems,
):
    layer, core = info[0], info[1]
    small = [
        pltpu.make_async_copy(a, b, sems.at[7 + i])
        for i, (a, b) in enumerate(((levels_in, levels), (near_in, near), (rates_in, rates)))
    ]
    for copy in small:
        copy.start()
    copies = []
    for v in range(4):
        rows = pl.ds(32 * v, 32)
        copies.append(pltpu.make_async_copy(pop.at[:, rows, :], pops.at[:, rows, :], sems.at[v]))
    copies.append(pltpu.make_async_copy(old, olds, sems.at[4]))
    copies.append(pltpu.make_async_copy(new, news, sems.at[5]))
    copies.append(pltpu.make_async_copy(scal, scals, sems.at[6]))
    for copy in copies:
        copy.start()
    index = grow_index()
    for copy in small:
        copy.wait()
    row, lane = iota(CHUNK, 0), iota(CHUNK, 1)
    meta = jnp.zeros((CHUNK, LANES), F32)
    for b in range(4):
        for q in range(6):
            here = jnp.logical_and(row == b, lane == q + 8)
            meta = jnp.where(here, near[b, q].astype(F32), meta)
    out[FIELDS - 1, 0:8, :] = meta

    def fine_of(b):
        return levels[layer * 8 + core * 4 + b] == 1

    for v in range(4):
        copies[v].wait()

        @pl.loop(0, 4)
        def _(b):
            @pl.when(fine_of(b))
            def _():
                at = pl.ds(8 * v, 8)
                from_rows = pl.ds(32 * v + b, 8, stride=4)
                post, _j = collide([pops[p, from_rows, :] for p in range(27)], lambda k: rates[k])
                for p in range(27):
                    out[b * PER_BLOCK + p, at, :] = post[p]

    for copy in copies[4:]:
        copy.wait()

    @pl.loop(0, 4)
    def _(b):
        @pl.when(fine_of(b))
        def _():
            for m in range(9):
                for v in range(4):
                    out[b * PER_BLOCK + 27 + m, pl.ds(8 * v, 8), :] = scals[m, pl.ds(32 * v + b, 8, stride=4), :]

        @pl.when(jnp.logical_not(fine_of(b)))
        def _():
            for p in range(27):
                for v in range(4):
                    before = olds[p, pl.ds(4 * v + b, 1), :]
                    after = news[p, pl.ds(4 * v + b, 1), :]
                    out[b * PER_BLOCK + 27 + p // 8, pl.ds(p % 8 * 4 + v, 1), :] = 0.5 * (before + after)
                    out[b * PER_BLOCK + p, pl.ds(8 * v, 8), :] = grow_row(before, index)


    pack_faces(out, up, down, meta)


def pack_faces(out, up, down, meta=None):
    lane = iota(CHUNK, 1) % 16

    @pl.loop(0, 4)
    def _(v):
        at = chunk_at(v)
        for ref, digit, start in ((up, 2, 15), (down, 0, 0)):
            for b in range(4):
                fields = [out[b * PER_BLOCK + 3 * e + digit, at, :] for e in range(9)]
                fields += [out[b * PER_BLOCK + 27 + e, at, :] for e in range(7)]
                ref[b, at, :] = pack_into(fields, 0, start, lane)
            rest = pack_into([out[b * PER_BLOCK + 34 + e, at, :] for b in range(4) for e in range(2)], 0, start, lane)
            ref[4, at, :] = rest if meta is None else jnp.where(lane < 8, rest, meta)


def spot(block, core):
    return (block % 8) ^ (core * 4)


def y_up(own, beside, even, group):
    turned = jnp.where(even, pltpu.roll(beside, CHUNK - 1, 0), pltpu.roll(own, 1, 0))
    return roll_lanes(jnp.where(group < 7, own, turned), 16)


def y_down(own, beside, even, group):
    turned = jnp.where(even, pltpu.roll(own, CHUNK - 1, 0), pltpu.roll(beside, 1, 0))
    return roll_lanes(jnp.where(group > 0, own, turned), -16)


def chunks(ref, *lead):
    return [ref[(*lead, pl.ds(8 * v, 8), slice(None))] for v in range(4)]


def x_up(own, beyond, row):
    turned = [pltpu.roll(x, 2, 0) for x in own]
    before = [beyond] + turned[:3]
    return [jnp.where(row < 2, a, b) for a, b in zip(before, turned)]


def x_down(own, beyond, row):
    turned = [pltpu.roll(x, CHUNK - 2, 0) for x in own]
    after = turned[1:] + [beyond]
    return [jnp.where(row >= 6, a, b) for a, b in zip(after, turned)]


def put(ref, lead, values):
    for v in range(4):
        ref[(*lead, pl.ds(8 * v, 8), slice(None))] = values[v]


def sections_xy(refs, faces, mid, dest, near, core, fine_of):
    row = iota(CHUNK, 0)
    even = row % 2 == 0
    group = iota(CHUNK, 1) // 16

    for half, ref in enumerate(refs):

        @pl.loop(0, 4)
        def _(i):
            for p, c in enumerate(VEL):
                if c[0] == 1:
                    faces[half * 4 + i, p] = pltpu.roll(ref[i * PER_BLOCK + p, pl.ds(24, 8), :], 2, 0)
                elif c[0] == -1:
                    faces[half * 4 + i, p] = pltpu.roll(ref[i * PER_BLOCK + p, pl.ds(0, 8), :], CHUNK - 2, 0)

    for half, ref in enumerate(refs):

        @pl.loop(0, 4)
        def _(i):
            b = half * 4 + i
            fine = fine_of(b)
            fields = [p for p in range(27) if half == 0 or VEL[p][1] != 0]

            @pl.when(fine)
            def _():
                low, high = spot(near[b, 0], core), spot(near[b, 1], core)
                for p in fields:
                    values = chunks(ref, i * PER_BLOCK + p)
                    if VEL[p][0] == 1:
                        values = x_up(values, faces[low, p], row)
                    elif VEL[p][0] == -1:
                        values = x_down(values, faces[high, p], row)
                    put(mid, (b, p), values)

            @pl.when(jnp.logical_not(fine))
            def _():
                for p in fields:
                    if VEL[p][1] != 0:
                        put(mid, (b, p), chunks(ref, i * PER_BLOCK + p))

    @pl.loop(0, 4)
    def _(b):
        @pl.when(fine_of(b))
        def _():
            low, high = spot(near[b, 2], core), spot(near[b, 3], core)
            for p, c in enumerate(VEL):
                for v in range(4):
                    at = pl.ds(8 * v, 8)
                    value = mid[b, p, at, :]
                    if c[1] == 1:
                        value = y_up(value, mid[low, p, at, :], even, group)
                    elif c[1] == -1:
                        value = y_down(value, mid[high, p, at, :], even, group)
                    dest[b, p, at, :] = value


def pack_into(fields, first_slot, start, lane):
    out = None
    for e, field in enumerate(fields):
        slot = first_slot + e
        moved = roll_lanes(field, slot - start)
        out = moved if out is None else jnp.where(lane == slot, moved, out)
    return out


def plane_kernel(info, levels, near, own, other, dest, table, mid, faces, meta, sem):
    layer, core = info[0], info[1]
    copy = pltpu.make_async_copy(other.at[FIELDS - 1, pl.ds(0, 8), :], meta, sem)
    copy.start()
    copy.wait()
    for i in range(4):
        for q in range(6):
            table[i, q] = near[i, q]
            table[4 + i, q] = meta[i, 8 + q].astype(jnp.int32)

    def fine_of(b):
        return levels[layer * 8 + spot(b, core)] == 1

    sections_xy((own, other), faces, mid, dest, table, core, fine_of)


def arrive(info, levels, table, core, incoming, raw, mid, done):
    row, slot = iota(CHUNK, 0), iota(CHUNK, 1) % 16
    even, group = row % 2 == 0, iota(CHUNK, 1) // 16
    x_plus, x_minus = jnp.logical_and(slot >= 6, slot < 9), slot < 3
    y_plus = jnp.logical_and(slot < 9, slot % 3 == 2)
    y_minus = jnp.logical_and(slot < 9, slot % 3 == 0)
    for way in range(2):
        for half in range(2):
            for i in range(4):
                put(raw, (way, half * 4 + i), chunks(incoming[way][half], i))

    for way in range(2):

        @pl.loop(0, 8)
        def _(b):
            fine = levels[info[2 + way] * 8 + spot(b, core)] == 1
            own = chunks(raw, way, b)

            @pl.when(fine)
            def _():
                low, high = spot(table[way * 8 + b, 0], core), spot(table[way * 8 + b, 1], core)
                before = x_up(own, pltpu.roll(raw[way, low, pl.ds(24, 8), :], 2, 0), row)
                after = x_down(own, pltpu.roll(raw[way, high, pl.ds(0, 8), :], CHUNK - 2, 0), row)
                values = [jnp.where(x_plus, x, jnp.where(x_minus, y, z)) for x, y, z in zip(before, after, own)]
                put(mid, (way, b), values)

            @pl.when(jnp.logical_not(fine))
            def _():
                put(mid, (way, b), own)

    for way in range(2):

        @pl.loop(0, 8)
        def _(b):
            fine = levels[info[2 + way] * 8 + spot(b, core)] == 1
            own = chunks(mid, way, b)

            @pl.when(fine)
            def _():
                low, high = spot(table[way * 8 + b, 2], core), spot(table[way * 8 + b, 3], core)
                values = []
                for v, here in enumerate(own):
                    at = pl.ds(8 * v, 8)
                    before = y_up(here, mid[way, low, at, :], even, group)
                    after = y_down(here, mid[way, high, at, :], even, group)
                    values.append(jnp.where(y_plus, before, jnp.where(y_minus, after, here)))
                put(done, (way, b), values)

            @pl.when(jnp.logical_not(fine))
            def _():
                put(done, (way, b), own)


def face_reader(done, rest, below, above):
    def faces(m, at):
        if m < 7:
            slot = 9 + m
            return roll_lanes(done[0, below, at, :], -slot), roll_lanes(done[1, above, at, :], 15 - slot)
        low = LANES - 2 * (below % 4) - (m - 7)
        high = (LANES + 15 - 2 * (above % 4) - (m - 7)) % LANES
        return pltpu.roll(rest[0, below // 4, at, :], low, 1), pltpu.roll(rest[1, above // 4, at, :], high, 1)

    return faces


def z_section(h, up, down, depth):
    g = []
    for p, c in enumerate(VEL):
        e = p // 3
        value = h(p)
        if c[2] == 1:
            value = jnp.where(depth == 0, roll_lanes(up, -e), roll_lanes(value, 1))
        elif c[2] == -1:
            value = jnp.where(depth == 15, roll_lanes(down, 15 - e), roll_lanes(value, -1))
        g.append(value)
    return g


def species_step(y_ref, b, sides, faces, flux, flags, diffusivity, stoichiometry, store):
    row, lanes = iota(CHUNK, 0), iota(CHUNK, 1)
    even = row % 2 == 0
    group, depth = lanes // 16, lanes % 16

    def gone(edge, q):
        return jnp.logical_and(edge, flags[q] != 1)

    lost = [
        gone(row < 2, 0), gone(row >= 6, 1),
        gone(jnp.logical_and(even, group == 0), 2), gone(jnp.logical_and(jnp.logical_not(even), group == 7), 3),
        gone(depth == 0, 4), gone(depth == 15, 5),
    ]
    burning = [
        a * c * jnp.exp(4.0 * (t - 1.0))
        for a, c, t in zip(chunks(y_ref, b, 0), chunks(y_ref, b, 1), chunks(y_ref, b, 8))
    ]
    for m in range(9):
        y = chunks(y_ref, b, m)
        low_x = pltpu.roll(y_ref[sides[0], m, pl.ds(24, 8), :], 2, 0)
        high_x = pltpu.roll(y_ref[sides[1], m, pl.ds(0, 8), :], CHUNK - 2, 0)
        lower_x, upper_x = x_up(y, low_x, row), x_down(y, high_x, row)
        lower_x[0] = jnp.where(lost[0], y[0], lower_x[0])
        upper_x[3] = jnp.where(lost[1], y[3], upper_x[3])
        for v in range(4):
            at = pl.ds(8 * v, 8)
            here = y[v]
            z_low, z_high = faces(m, at)
            pairs = [
                (lower_x[v], upper_x[v]),
                (
                    jnp.where(lost[2], here, y_up(here, y_ref[sides[2], m, at, :], even, group)),
                    jnp.where(lost[3], here, y_down(here, y_ref[sides[3], m, at, :], even, group)),
                ),
                (
                    jnp.where(lost[4], here, jnp.where(depth == 0, z_low, roll_lanes(here, 1))),
                    jnp.where(lost[5], here, jnp.where(depth == 15, z_high, roll_lanes(here, -1))),
                ),
            ]
            drift = spread = None
            for d, (lower, upper) in enumerate(pairs):
                part = flux[d, at, :] * (upper - lower)
                both = upper + lower
                drift = part if drift is None else drift + part
                spread = both if spread is None else spread + both
            value = here - drift + diffusivity[m] * (spread - 6.0 * here) + stoichiometry[m] * burning[v]
            store(m, v, value)


WIDE = 640


def reduce_tables():
    l = np.arange(LANES)[:, None]
    c = np.arange(WIDE)[None, :]
    e, cell = c // 64, c % 64
    live = c < 576
    along_x = (l // 32 * 8 + l % 16 // 2 == cell % 32) & live
    along_y = [(l // 16 + 8 * a == e) & (l % 16 // 2 == cell % 8) & live for a in range(2)]
    along_z = (l % 16 == e) & (l // 32 == cell % 4) & live
    side = np.concatenate([along_x, along_y[0], along_y[1]], axis=0)
    return jnp.asarray(side, F32), jnp.asarray(along_z, F32)


def wide_iota(axis):
    return lax.broadcasted_iota(jnp.int32, (ROWS, WIDE), axis)


def times(x, w):
    return jnp.dot(x, w, precision=lax.Precision.HIGHEST, preferred_element_type=F32)


def put_pair(out, s, base, first, second):
    moved = pltpu.roll(second, 64, 1)
    out[pl.ds(s, 1), pl.ds(base, 512)] = first[:, 0:512]
    out[pl.ds(s, 1), pl.ds(base + 512, 128)] = first[:, 512:640] + moved[:, 0:128]
    out[pl.ds(s, 1), pl.ds(base + 640, 512)] = moved[:, 128:640]


def middle_kernel(
    info, levels, near, rates, diffusivity, stoichiometry, own, other, held, up_own, up_other, down_own, down_other,
    out, up, down, table,
    raw, mid, done, rest, old, flux, metas, sems,
):
    layer, core = info[0], info[1]
    index = grow_index()
    incoming = ((up_own, up_other), (down_own, down_other))
    copies = []
    for way in range(2):
        for half in range(2):
            k = way * 2 + half
            copies.append(
                pltpu.make_async_copy(incoming[way][half].at[4, pl.ds(0, 8), :], metas.at[k], sems.at[k])
            )
            copies[-1].start()
            put(rest, (way, half), chunks(incoming[way][half], 4))

    def fine_of(b):
        return levels[layer * 8 + spot(b, core)] == 1

    for half, ref_in in enumerate((own, other)):

        @pl.loop(0, 4)
        def _(i):
            for m in range(9):
                put(old, (half * 4 + i, m), chunks(ref_in, i * PER_BLOCK + 27 + m))

    for copy in copies:
        copy.wait()
    for way in range(2):
        for b in range(8):
            for q in range(6):
                table[way * 8 + b, q] = metas[way * 2 + b // 4, b % 4, 8 + q].astype(jnp.int32)
    arrive(info, levels, table, core, incoming, raw, mid, done)

    @pl.loop(0, 4)
    def _(b):
        @pl.when(fine_of(b))
        def _():
            below, above = spot(near[b, 4], core), spot(near[b, 5], core)

            @pl.loop(0, 4)
            def _(v):
                at = chunk_at(v)
                g = z_section(lambda p: held[b, p, at, :], done[0, below, at, :], done[1, above, at, :], depth_of())
                post, j = collide(g, lambda k: rates[k])
                for p in range(27):
                    out[b * PER_BLOCK + p, at, :] = post[p]
                for d in range(3):
                    flux[d, at, :] = j[d] * (0.5 / 216.0)

            def store(m, v, value):
                out[b * PER_BLOCK + 27 + m, pl.ds(8 * v, 8), :] = value

            species_step(
                old, b, [spot(near[b, q], core) for q in range(4)], face_reader(done, rest, below, above), flux,
                [levels[near[b, q]] for q in range(6)], diffusivity, stoichiometry, store,
            )

        @pl.when(jnp.logical_not(fine_of(b)))
        def _():
            for p in range(27):
                for v in range(4):
                    line = own[b * PER_BLOCK + 27 + p // 8, pl.ds(p % 8 * 4 + v, 1), :]
                    out[b * PER_BLOCK + p, pl.ds(8 * v, 8), :] = grow_row(line, index)
            for m in range(9):
                put(out, (b * PER_BLOCK + 27 + m,), [jnp.zeros((CHUNK, LANES), F32)] * 4)

    pack_faces(out, up, down)
    row, lane = iota(CHUNK, 0), iota(CHUNK, 1)

    @pl.loop(0, 4)
    def _(v):
        at = chunk_at(v)
        for ref, digit, start in ((up, 2, 15), (down, 0, 0)):
            merged = None
            for b in range(4):
                fields = [
                    0.125 * (own[b * PER_BLOCK + 3 * e + digit, at, :] + out[b * PER_BLOCK + 3 * e + digit, at, :])
                    for e in range(9)
                ]
                total = pack_into(fields, 0, start, lane % 16)
                total = total + pltpu.roll(total, CHUNK - 2, 0)
                total = total + roll_lanes(total, -16)
                if b % 2:
                    total = pltpu.roll(total, 2, 0)
                if b // 2:
                    total = roll_lanes(total, 16)
                here = jnp.logical_and(row // 2 % 2 == b % 2, lane // 16 % 2 == b // 2)
                merged = total if merged is None else jnp.where(here, total, merged)
            ref[5, at, :] = merged


def depth_of():
    return iota(CHUNK, 1) % 16


def second_plane_kernel(
    info, levels, near, own, other, own_before, other_before, tables, dest, sides_out, mid, faces, edge_x, edge_y
):
    layer, core = info[0], info[1]

    def fine_of(b):
        return levels[layer * 8 + spot(b, core)] == 1

    sections_xy((own, other), faces, mid, dest, near, core, fine_of)
    group, odd = iota(CHUNK, 1) // 16, iota(CHUNK, 0) % 2 == 1
    for half, (one, two) in enumerate(((own_before, own), (other_before, other))):

        @pl.loop(0, 4)
        def _(i):
            b = half * 4 + i

            def total(p, at):
                return one[i * PER_BLOCK + p, at, :] + two[i * PER_BLOCK + p, at, :]

            @pl.when(fine_of(b))
            def _():
                for side in range(2):
                    at = pl.ds(30, 2) if side == 0 else pl.ds(0, 2)
                    for e in range(9):
                        edge_x[b, side, pl.ds(2 * e, 2), :] = total(18 + e if side == 0 else e, at)
                    edge_x[b, side, pl.ds(18, 14), :] = jnp.zeros((14, LANES), F32)
                for v in range(4):
                    at = pl.ds(8 * v, 8)
                    packs = [None, None]
                    for e in range(9):
                        p_low = 9 * (e // 3) + e % 3
                        slot = e % 8
                        high = roll_lanes(total(p_low + 6, at), 16 * (slot - 7))
                        both = jnp.where(odd, high, roll_lanes(total(p_low, at), 16 * slot))
                        held_pack = packs[e // 8]
                        packs[e // 8] = both if held_pack is None else jnp.where(group == slot, both, held_pack)
                    for a in range(2):
                        edge_y[b, a, at, :] = packs[a]

    row, col = wide_iota(0), wide_iota(1)
    e_of, cell = col // 64, col % 64
    keep_x = jnp.logical_and(row // 2 == e_of, row % 2 == cell // 32)
    keep_y = row // 4 == cell // 8
    odd_row = row % 2 == 1
    for s in range(4):
        coarse = jnp.logical_not(fine_of(s))

        @pl.when(coarse)
        def _(s=s):
            fine = [levels[near[s, q]] == 1 for q in range(4)]
            at = [spot(near[s, q], core) for q in range(4)]
            rows = []
            for q in range(2):
                spread = times(jnp.where(fine[q], 0.125 * edge_x[at[q], q], 0.0), tables[0:128, :])
                rows.append(jnp.sum(jnp.where(keep_x, spread, 0.0), axis=0, keepdims=True))
            put_pair(sides_out, s, 0, rows[0], rows[1])
            rows = []
            for q in (2, 3):
                spread = times(jnp.where(fine[q], 0.125 * edge_y[at[q], 0], 0.0), tables[128:256, :])
                spread += times(jnp.where(fine[q], 0.125 * edge_y[at[q], 1], 0.0), tables[256:384, :])
                keep = jnp.logical_and(keep_y, odd_row if q == 2 else jnp.logical_not(odd_row))
                rows.append(jnp.sum(jnp.where(keep, spread, 0.0), axis=0, keepdims=True))
            put_pair(sides_out, s, 1152, rows[0], rows[1])

        @pl.when(jnp.logical_not(coarse))
        def _(s=s):
            sides_out[pl.ds(s, 1), :] = jnp.zeros((1, 2304), F32)


def end_kernel(
    info, levels, near, table, diffusivity, stoichiometry, held, own, other,
    up_own, up_other, down_own, down_other, sides, weights, pop, scal,
    pop_out, scal_out, returned,
    raw, mid, done, rest, returning, species, pops, scals, flux, sems,
):
    layer, core = info[0], info[1]
    incoming = ((up_own, up_other), (down_own, down_other))
    for half, ref_in in enumerate((own, other)):

        @pl.loop(0, 4)
        def _(i):
            for m in range(9):
                put(species, (half * 4 + i, m), chunks(ref_in, i * PER_BLOCK + 27 + m))

        for way in range(2):
            put(rest, (way, half), chunks(incoming[way][half], 4))
            put(returning, (way, half), chunks(incoming[way][half], 5))

    arrive(info, levels, table, core, incoming, raw, mid, done)
    depth = iota(CHUNK, 1) % 16
    row, col = wide_iota(0), wide_iota(1)
    keep = row // 4 * 2 + row % 2 == col % 64 // 4
    slim, wide = iota(ROWS, 0), iota(ROWS, 1)

    def fine_of(s):
        return levels[layer * 8 + core * 4 + s] == 1

    copies = []
    for v in range(4):
        at = pl.ds(8 * v, 8)

        @pl.loop(0, 4)
        def _(s):
            rows = pl.ds(32 * v + s, 8, stride=4)

            @pl.when(fine_of(s))
            def _():
                below, above = spot(near[s, 4], core), spot(near[s, 5], core)
                g = z_section(lambda p: held[s, p, at, :], done[0, below, at, :], done[1, above, at, :], depth)
                for p in range(27):
                    pops[p, rows, :] = g[p]
                m = forward_moments(g)
                for d, i in enumerate((9, 3, 1)):
                    flux[s, d, at, :] = m[i] * (0.5 / 216.0)

            @pl.when(jnp.logical_not(fine_of(s)))
            def _():
                for p in range(27):
                    pops[p, rows, :] = pop[p, rows, :]

        rows = pl.ds(32 * v, 32)
        copies.append(pltpu.make_async_copy(pops.at[:, rows, :], pop_out.at[:, rows, :], sems.at[v]))
        copies[-1].start()

    @pl.loop(0, 4)
    def _(s):
        @pl.when(fine_of(s))
        def _():
            def store(m, v, value):
                scals[m, pl.ds(32 * v + s, 8, stride=4), :] = value

            species_step(
                species, s, [spot(near[s, q], core) for q in range(4)],
                face_reader(done, rest, spot(near[s, 4], core), spot(near[s, 5], core)), flux.at[s],
                [levels[near[s, q]] for q in range(6)], diffusivity, stoichiometry, store,
            )

        @pl.when(jnp.logical_not(fine_of(s)))
        def _():
            for v in range(4):
                at = pl.ds(32 * v + s, 8, stride=4)
                for m in range(9):
                    scals[m, at, :] = scal[m, at, :]

    copies.append(pltpu.make_async_copy(scals, scal_out, sems.at[4]))
    copies[-1].start()
    returned[:, 0:2304] = sides[...]
    for s in range(4):
        coarse = levels[layer * 8 + core * 4 + s] != 1

        @pl.when(coarse)
        def _(s=s):
            rows = []
            for way in range(2):
                m = spot(near[s, 4 + way], core)
                here = jnp.logical_and(slim // 2 % 2 == m % 2, wide // 16 % 2 == m % 4 // 2)
                here = jnp.logical_and(here, levels[near[s, 4 + way]] == 1)
                face = jnp.where(here, returning[way, m // 4], 0.0)
                rows.append(jnp.sum(jnp.where(keep, times(face, weights[...]), 0.0), axis=0, keepdims=True))
            put_pair(returned, s, 2304, rows[0], rows[1])

        @pl.when(jnp.logical_not(coarse))
        def _(s=s):
            returned[pl.ds(s, 1), pl.ds(2304, 1152)] = jnp.zeros((1, 1152), F32)

    for copy in copies:
        copy.wait()


def specs(kinds):
    table = {
        "s": pl.BlockSpec(memory_space=pltpu.SMEM),
        "v": pl.BlockSpec(memory_space=pltpu.VMEM),
        "h": pl.BlockSpec(memory_space=pltpu.HBM),
    }
    return [table[kind] for kind in kinds]


def call(kernel, kinds, outs, out_kinds, scratch, name, megabytes, flops):
    return pl.pallas_call(
        kernel,
        in_specs=specs(kinds),
        out_specs=specs(out_kinds),
        out_shape=outs,
        scratch_shapes=scratch,
        name=name,
        compiler_params=pltpu.CompilerParams(vmem_limit_bytes=megabytes << 20),
        cost_estimate=pl.CostEstimate(flops=flops, transcendentals=0, bytes_accessed=8 << 20),
    )


def interleave(x):
    blocks, n, cells = x.shape
    x = x.reshape(blocks, n, cells // LANES, LANES)
    return jnp.transpose(x, (1, 2, 0, 3)).reshape(n, cells // LANES * blocks, LANES)


def separate(x):
    n, rows, _ = x.shape
    x = jnp.transpose(x.reshape(n, rows // 4, 4, LANES), (2, 0, 1, 3))
    return x.reshape(4, n, rows // 4 * LANES)


def local(
    populations, scalars, coarse_old, coarse_new, levels, neighbours, relax_rates, diffusivity, stoichiometry
):
    devices = lax.axis_size("blk")
    me = lax.axis_index("blk")
    layer, layers = me // 2, devices // 2
    info = jnp.stack([layer, me % 2, (layer + layers - 1) % layers, (layer + 1) % layers]).astype(jnp.int32)
    swap = [(i, i ^ 1) for i in range(devices)]
    rise = [(i, (i + 2) % devices) for i in range(devices)]
    fall = [(i, (i - 2) % devices) for i in range(devices)]

    def move(x, pairs):
        return lax.ppermute(x, "blk", pairs)

    def vmem(*lead):
        return pltpu.VMEM((*lead, ROWS, LANES), F32)

    full = (ROWS, LANES)
    pop, scal = interleave(populations), interleave(scalars)
    old, new = interleave(coarse_old), interleave(coarse_new)
    side_table, z_table = reduce_tables()
    fields = FIELDS - 1
    semaphores = pltpu.SemaphoreType.DMA
    own, up, down = call(
        begin_kernel,
        "shhhhhhh",
        [shape_of(FIELDS, *full), shape_of(5, *full), shape_of(5, *full)],
        "vvv",
        [pltpu.VMEM(x.shape, F32) for x in (pop, scal, old, new)]
        + [pltpu.SMEM(x.shape, x.dtype) for x in (levels, neighbours, relax_rates)]
        + [semaphores((10,))],
        "begin",
        12,
        1 << 27,
    )(info, *[pltpu.with_memory_space_constraint(x, pltpu.HBM) for x in (levels, neighbours, relax_rates, pop, scal, old, new)])
    other = move(own, swap)
    up, down = move(up, rise), move(down, fall)
    face = pltpu.VMEM((8, 27, CHUNK, LANES), F32)
    held, near = call(
        plane_kernel,
        "sssvv",
        [shape_of(4, 27, *full), jax.ShapeDtypeStruct((8, 6), jnp.int32)],
        "vs",
        [vmem(8, 27), face, pltpu.SMEM((8, LANES), F32), semaphores],
        "plane",
        12,
        1 << 27,
    )(info, levels, neighbours, own, other)
    held, up, down = lax.optimization_barrier((held, up, down))
    landing = [vmem(2, 8), vmem(2, 8), vmem(2, 8), vmem(2, 2)]
    own_next, up_next, down_next, table = call(
        middle_kernel,
        "ssssssvvvvvvv",
        [shape_of(fields, *full), shape_of(6, *full), shape_of(6, *full), jax.ShapeDtypeStruct((16, 6), jnp.int32)],
        "vvvs",
        landing + [vmem(8, 9), vmem(3), pltpu.SMEM((4, 8, LANES), F32), semaphores((4,))],
        "middle",
        14,
        1 << 28,
    )(
        info, levels, near, relax_rates, diffusivity, stoichiometry, own, other, held,
        up, move(up, swap), down, move(down, swap),
    )
    other_next = move(own_next, swap)
    up, down = move(up_next, rise), move(down_next, fall)
    held, sides = call(
        second_plane_kernel,
        "sssvvvvv",
        [shape_of(4, 27, *full), shape_of(4, 2304)],
        "vv",
        [vmem(8, 27), face, vmem(8, 2), vmem(8, 2)],
        "plane2",
        14,
        1 << 27,
    )(info, levels, near, own_next, other_next, own, other, side_table)
    held, sides, up, down = lax.optimization_barrier((held, sides, up, down))
    pop_out, scal_out, returned = call(
        end_kernel,
        "ssssssvvvvvvvvvvv",
        [shape_of(27, 128, LANES), shape_of(9, 128, LANES), shape_of(4, 3456)],
        "hhv",
        landing
        + [vmem(2, 2), vmem(8, 9), pltpu.VMEM(pop.shape, F32), pltpu.VMEM(scal.shape, F32), vmem(4, 3), semaphores((5,))],
        "end",
        16,
        1 << 27,
    )(
        info, levels, neighbours, table, diffusivity, stoichiometry, held, own_next, other_next,
        up, move(up, swap), down, move(down, swap), sides, z_table, pop, scal,
    )
    return separate(pop_out), separate(scal_out), returned


def solution(mesh):
    in_specs = (
        P("blk", None, None), P("blk", None, None), P("blk", None, None), P("blk", None, None),
        P(), P("blk", None), P(), P(), P(),
    )
    out_specs = (P("blk", None, None), P("blk", None, None), P("blk", None))
    return jax.shard_map(local, mesh=mesh, in_specs=in_specs, out_specs=out_specs, check_vma=False)
```

```python
import jax
import jax.numpy as jnp
import numpy as np
from jax import lax
from jax.experimental import pallas as pl
from jax.experimental.pallas import tpu as pltpu
from jax.sharding import PartitionSpec as P

F32 = jnp.float32
VEL = [(a, b, c) for a in (-1, 0, 1) for b in (-1, 0, 1) for c in (-1, 0, 1)]
ROWS, LANES = 32, 128
CHUNK = 8


def shape_of(*dims):
    return jax.ShapeDtypeStruct(dims, F32)


def iota(rows, axis):
    return lax.broadcasted_iota(jnp.int32, (rows, LANES), axis)


def chunk_at(v):
    return pl.ds(pl.multiple_of(v * CHUNK, CHUNK), CHUNK)


def roll_lanes(x, by):
    if isinstance(by, int):
        by = by % LANES
        if by == 0:
            return x
    return pltpu.roll(x, by, 1)


def forward_moments(values):
    out = list(values)
    for stride in (9, 3, 1):
        for i in range(27):
            if (i // stride) % 3 == 0:
                low, mid, high = out[i], out[i + stride], out[i + 2 * stride]
                both = low + high
                out[i] = both + 4.0 * mid
                out[i + stride] = high - low
                out[i + 2 * stride] = both
    return out


def plus(x, y):
    if x is None:
        return y
    return x if y is None else x + y


def minus(x, y):
    if y is None:
        return x
    return -y if x is None else x - y


def backward_moments(values):
    out = list(values)
    for stride in (9, 3, 1):
        for i in range(27):
            if (i // stride) % 3 == 0:
                m0, m1, m2 = out[i], out[i + stride], out[i + 2 * stride]
                out[i] = minus(m2, m1)
                out[i + stride] = minus(m0, m2)
                out[i + 2 * stride] = plus(m1, m2)
    return out


def collide(g, rate):
    m = forward_moments(g)
    rho = m[0]
    j = (m[9], m[3], m[1])
    square = [x * x * (1.0 / 72.0) for x in j]
    relaxed = [None] * 27
    for k in range(27):
        digits = (k // 9, (k // 3) % 3, k % 3)
        odd = [d for d in range(3) if digits[d] == 1]
        twos = [d for d in range(3) if digits[d] == 2]
        if k in (0, 9, 3, 1):
            continue
        if not odd:
            level = rho
            for d in twos:
                level = level + square[d]
        elif len(odd) == 1:
            level = j[odd[0]]
        elif len(odd) == 2:
            level = j[odd[0]] * j[odd[1]] * (1.0 / 216.0)
        else:
            level = None
        if level is not None and twos:
            level = level * (3.0 ** -len(twos))
        relaxed[k] = minus(m[k], level) * (rate(k) * (1.0 / 64.0))
    back = backward_moments(relaxed)
    post = []
    for i, c in enumerate(VEL):
        factor = 2.0 ** sum(abs(x) for x in c)
        post.append(g[i] - (back[i] if factor == 1.0 else factor * back[i]))
    return post, j


def grow_index():
    r, l = iota(CHUNK, 0), iota(CHUNK, 1)
    return (r // 4) % 2 * 64 + r % 2 * 32 + l // 32 * 8 + l % 16 // 2


def grow_row(row, index):
    return jnp.take_along_axis(jnp.broadcast_to(row, (CHUNK, LANES)), index, axis=1)


PER_BLOCK = 36
FIELDS = 4 * PER_BLOCK + 1


def begin_kernel(
    info, levels_in, near_in, rates_in, pop, scal, old, new, out, up, down,
    pops, scals, olds, news, levels, near, rates, sems,
):
    layer, core = info[0], info[1]
    small = [
        pltpu.make_async_copy(a, b, sems.at[7 + i])
        for i, (a, b) in enumerate(((levels_in, levels), (near_in, near), (rates_in, rates)))
    ]
    for copy in small:
        copy.start()
    copies = []
    for v in range(4):
        rows = pl.ds(32 * v, 32)
        copies.append(pltpu.make_async_copy(pop.at[:, rows, :], pops.at[:, rows, :], sems.at[v]))
    copies.append(pltpu.make_async_copy(old, olds, sems.at[4]))
    copies.append(pltpu.make_async_copy(new, news, sems.at[5]))
    copies.append(pltpu.make_async_copy(scal, scals, sems.at[6]))
    for copy in copies:
        copy.start()
    index = grow_index()
    for copy in small:
        copy.wait()
    row, lane = iota(CHUNK, 0), iota(CHUNK, 1)
    meta = jnp.zeros((CHUNK, LANES), F32)
    for b in range(4):
        for q in range(6):
            here = jnp.logical_and(row == b, lane == q + 8)
            meta = jnp.where(here, near[b, q].astype(F32), meta)
    out[FIELDS - 1, 0:8, :] = meta

    def fine_of(b):
        return levels[layer * 8 + core * 4 + b] == 1

    for v in range(4):
        copies[v].wait()

        @pl.loop(0, 4)
        def _(b):
            @pl.when(fine_of(b))
            def _():
                at = pl.ds(8 * v, 8)
                from_rows = pl.ds(32 * v + b, 8, stride=4)
                post, _j = collide([pops[p, from_rows, :] for p in range(27)], lambda k: rates[k])
                for p in range(27):
                    out[b * PER_BLOCK + p, at, :] = post[p]

    for copy in copies[4:]:
        copy.wait()

    @pl.loop(0, 4)
    def _(b):
        @pl.when(fine_of(b))
        def _():
            for m in range(9):
                for v in range(4):
                    out[b * PER_BLOCK + 27 + m, pl.ds(8 * v, 8), :] = scals[m, pl.ds(32 * v + b, 8, stride=4), :]

        @pl.when(jnp.logical_not(fine_of(b)))
        def _():
            for p in range(27):
                for v in range(4):
                    before = olds[p, pl.ds(4 * v + b, 1), :]
                    after = news[p, pl.ds(4 * v + b, 1), :]
                    out[b * PER_BLOCK + 27 + p // 8, pl.ds(p % 8 * 4 + v, 1), :] = 0.5 * (before + after)
                    out[b * PER_BLOCK + p, pl.ds(8 * v, 8), :] = grow_row(before, index)


    pack_faces(out, up, down, meta)


def pack_faces(out, up, down, meta=None):
    lane = iota(CHUNK, 1) % 16

    @pl.loop(0, 4)
    def _(v):
        at = chunk_at(v)
        for ref, digit, start in ((up, 2, 15), (down, 0, 0)):
            for b in range(4):
                fields = [out[b * PER_BLOCK + 3 * e + digit, at, :] for e in range(9)]
                fields += [out[b * PER_BLOCK + 27 + e, at, :] for e in range(7)]
                ref[b, at, :] = pack_into(fields, 0, start, lane)
            rest = pack_into([out[b * PER_BLOCK + 34 + e, at, :] for b in range(4) for e in range(2)], 0, start, lane)
            ref[4, at, :] = rest if meta is None else jnp.where(lane < 8, rest, meta)


def spot(block, core):
    return (block % 8) ^ (core * 4)


def y_up(own, beside, even, group):
    turned = jnp.where(even, pltpu.roll(beside, CHUNK - 1, 0), pltpu.roll(own, 1, 0))
    return roll_lanes(jnp.where(group < 7, own, turned), 16)


def y_down(own, beside, even, group):
    turned = jnp.where(even, pltpu.roll(own, CHUNK - 1, 0), pltpu.roll(beside, 1, 0))
    return roll_lanes(jnp.where(group > 0, own, turned), -16)


def chunks(ref, *lead):
    return [ref[(*lead, pl.ds(8 * v, 8), slice(None))] for v in range(4)]


def x_up(own, beyond, row):
    turned = [pltpu.roll(x, 2, 0) for x in own]
    before = [beyond] + turned[:3]
    return [jnp.where(row < 2, a, b) for a, b in zip(before, turned)]


def x_down(own, beyond, row):
    turned = [pltpu.roll(x, CHUNK - 2, 0) for x in own]
    after = turned[1:] + [beyond]
    return [jnp.where(row >= 6, a, b) for a, b in zip(after, turned)]


def put(ref, lead, values):
    for v in range(4):
        ref[(*lead, pl.ds(8 * v, 8), slice(None))] = values[v]


def sections_xy(refs, faces, mid, dest, near, core, fine_of):
    row = iota(CHUNK, 0)
    even = row % 2 == 0
    group = iota(CHUNK, 1) // 16

    for half, ref in enumerate(refs):

        @pl.loop(0, 4)
        def _(i):
            for p, c in enumerate(VEL):
                if c[0] == 1:
                    faces[half * 4 + i, p] = pltpu.roll(ref[i * PER_BLOCK + p, pl.ds(24, 8), :], 2, 0)
                elif c[0] == -1:
                    faces[half * 4 + i, p] = pltpu.roll(ref[i * PER_BLOCK + p, pl.ds(0, 8), :], CHUNK - 2, 0)

    for half, ref in enumerate(refs):

        @pl.loop(0, 4)
        def _(i):
            b = half * 4 + i
            fine = fine_of(b)
            fields = [p for p in range(27) if half == 0 or VEL[p][1] != 0]

            @pl.when(fine)
            def _():
                low, high = spot(near[b, 0], core), spot(near[b, 1], core)
                for p in fields:
                    values = chunks(ref, i * PER_BLOCK + p)
                    if VEL[p][0] == 1:
                        values = x_up(values, faces[low, p], row)
                    elif VEL[p][0] == -1:
                        values = x_down(values, faces[high, p], row)
                    put(mid, (b, p), values)

            @pl.when(jnp.logical_not(fine))
            def _():
                for p in fields:
                    if VEL[p][1] != 0:
                        put(mid, (b, p), chunks(ref, i * PER_BLOCK + p))

    @pl.loop(0, 4)
    def _(b):
        @pl.when(fine_of(b))
        def _():
            low, high = spot(near[b, 2], core), spot(near[b, 3], core)
            for p, c in enumerate(VEL):
                for v in range(4):
                    at = pl.ds(8 * v, 8)
                    value = mid[b, p, at, :]
                    if c[1] == 1:
                        value = y_up(value, mid[low, p, at, :], even, group)
                    elif c[1] == -1:
                        value = y_down(value, mid[high, p, at, :], even, group)
                    dest[b, p, at, :] = value


def pack_into(fields, first_slot, start, lane):
    out = None
    for e, field in enumerate(fields):
        slot = first_slot + e
        moved = roll_lanes(field, slot - start)
        out = moved if out is None else jnp.where(lane == slot, moved, out)
    return out


def plane_kernel(info, levels, own, other, dest, table, mid, faces, meta, sem):
    layer, core = info[0], info[1]
    row = iota(CHUNK, 0)
    both = jnp.where(row < 4, own[FIELDS - 1, 0:8, :], pltpu.roll(other[FIELDS - 1, 0:8, :], 4, 0))
    meta[...] = roll_lanes(both, -8).astype(jnp.int32)
    copy = pltpu.make_async_copy(meta, table, sem)
    copy.start()
    copy.wait()

    def fine_of(b):
        return levels[layer * 8 + spot(b, core)] == 1

    sections_xy((own, other), faces, mid, dest, table, core, fine_of)


def arrive(info, levels, table, core, incoming, raw, mid, done):
    row, slot = iota(CHUNK, 0), iota(CHUNK, 1) % 16
    even, group = row % 2 == 0, iota(CHUNK, 1) // 16
    x_plus, x_minus = jnp.logical_and(slot >= 6, slot < 9), slot < 3
    y_plus = jnp.logical_and(slot < 9, slot % 3 == 2)
    y_minus = jnp.logical_and(slot < 9, slot % 3 == 0)
    for way in range(2):
        for half in range(2):
            for i in range(4):
                put(raw, (way, half * 4 + i), chunks(incoming[way][half], i))

    blocks = [(way, b) for way in range(2) for b in range(8)]
    fine = [levels[info[2 + way] * 8 + spot(b, core)] == 1 for way, b in blocks]

    def beside(way, b, q):
        return spot(table[b, 16 * way + 8 + q], core)

    for (way, b), flag in zip(blocks, fine):
        own = chunks(raw, way, b)
        before = x_up(own, pltpu.roll(raw[way, beside(way, b, 0), pl.ds(24, 8), :], 2, 0), row)
        after = x_down(own, pltpu.roll(raw[way, beside(way, b, 1), pl.ds(0, 8), :], CHUNK - 2, 0), row)
        to_plus, to_minus = jnp.logical_and(x_plus, flag), jnp.logical_and(x_minus, flag)
        put(mid, (way, b), [jnp.where(to_plus, x, jnp.where(to_minus, y, z)) for x, y, z in zip(before, after, own)])
    for (way, b), flag in zip(blocks, fine):
        low, high = beside(way, b, 2), beside(way, b, 3)
        to_plus, to_minus = jnp.logical_and(y_plus, flag), jnp.logical_and(y_minus, flag)
        for v in range(4):
            at = pl.ds(8 * v, 8)
            here = mid[way, b, at, :]
            before = y_up(here, mid[way, low, at, :], even, group)
            after = y_down(here, mid[way, high, at, :], even, group)
            done[way, b, at, :] = jnp.where(to_plus, before, jnp.where(to_minus, after, here))


def face_reader(done, rest, below, above):
    def faces(m, at):
        if m < 7:
            slot = 9 + m
            return roll_lanes(done[0, below, at, :], -slot), roll_lanes(done[1, above, at, :], 15 - slot)
        low = LANES - 2 * (below % 4) - (m - 7)
        high = (LANES + 15 - 2 * (above % 4) - (m - 7)) % LANES
        return pltpu.roll(rest[0, below // 4, at, :], low, 1), pltpu.roll(rest[1, above // 4, at, :], high, 1)

    return faces


def z_section(h, up, down, depth):
    g = []
    for p, c in enumerate(VEL):
        e = p // 3
        value = h(p)
        if c[2] == 1:
            value = jnp.where(depth == 0, roll_lanes(up, -e), roll_lanes(value, 1))
        elif c[2] == -1:
            value = jnp.where(depth == 15, roll_lanes(down, 15 - e), roll_lanes(value, -1))
        g.append(value)
    return g


def species_step(y_ref, b, sides, faces, flux, flags, diffusivity, stoichiometry, store):
    row, lanes = iota(CHUNK, 0), iota(CHUNK, 1)
    even = row % 2 == 0
    group, depth = lanes // 16, lanes % 16

    def gone(edge, q):
        return jnp.logical_and(edge, flags[q] != 1)

    lost = [
        gone(row < 2, 0), gone(row >= 6, 1),
        gone(jnp.logical_and(even, group == 0), 2), gone(jnp.logical_and(jnp.logical_not(even), group == 7), 3),
        gone(depth == 0, 4), gone(depth == 15, 5),
    ]
    burning = [
        a * c * jnp.exp(4.0 * (t - 1.0))
        for a, c, t in zip(chunks(y_ref, b, 0), chunks(y_ref, b, 1), chunks(y_ref, b, 8))
    ]
    for m in range(9):
        y = chunks(y_ref, b, m)
        low_x = pltpu.roll(y_ref[sides[0], m, pl.ds(24, 8), :], 2, 0)
        high_x = pltpu.roll(y_ref[sides[1], m, pl.ds(0, 8), :], CHUNK - 2, 0)
        lower_x, upper_x = x_up(y, low_x, row), x_down(y, high_x, row)
        lower_x[0] = jnp.where(lost[0], y[0], lower_x[0])
        upper_x[3] = jnp.where(lost[1], y[3], upper_x[3])
        for v in range(4):
            at = pl.ds(8 * v, 8)
            here = y[v]
            z_low, z_high = faces(m, at)
            pairs = [
                (lower_x[v], upper_x[v]),
                (
                    jnp.where(lost[2], here, y_up(here, y_ref[sides[2], m, at, :], even, group)),
                    jnp.where(lost[3], here, y_down(here, y_ref[sides[3], m, at, :], even, group)),
                ),
                (
                    jnp.where(lost[4], here, jnp.where(depth == 0, z_low, roll_lanes(here, 1))),
                    jnp.where(lost[5], here, jnp.where(depth == 15, z_high, roll_lanes(here, -1))),
                ),
            ]
            drift = spread = None
            for d, (lower, upper) in enumerate(pairs):
                part = flux[d, at, :] * (upper - lower)
                both = upper + lower
                drift = part if drift is None else drift + part
                spread = both if spread is None else spread + both
            value = here - drift + diffusivity[m] * (spread - 6.0 * here) + stoichiometry[m] * burning[v]
            store(m, v, value)


WIDE = 640


def reduce_tables():
    l = np.arange(LANES)[:, None]
    c = np.arange(WIDE)[None, :]
    e, cell = c // 64, c % 64
    live = c < 576
    along_x = (l // 32 * 8 + l % 16 // 2 == cell % 32) & live
    along_y = [(l // 16 + 8 * a == e) & (l % 16 // 2 == cell % 8) & live for a in range(2)]
    along_z = (l % 16 == e) & (l // 32 == cell % 4) & live
    side = np.concatenate([along_x, along_y[0], along_y[1]], axis=0)
    return jnp.asarray(side, jnp.bfloat16), jnp.asarray(along_z, jnp.bfloat16)


def wide_iota(axis):
    return lax.broadcasted_iota(jnp.int32, (ROWS, WIDE), axis)


def times(x, w):
    total = None
    for _ in range(3):
        part = x.astype(jnp.bfloat16)
        x = x - part.astype(F32)
        product = jnp.dot(part, w, preferred_element_type=F32)
        total = product if total is None else total + product
    return total


def column_sums(spread, k, keep):
    return jnp.sum(jnp.where(keep, spread[pl.ds(k * ROWS, ROWS), :], 0.0), axis=0, keepdims=True)


def put_pair(out, s, base, first, second):
    moved = pltpu.roll(second, 64, 1)
    out[pl.ds(s, 1), pl.ds(base, 512)] = first[:, 0:512]
    out[pl.ds(s, 1), pl.ds(base + 512, 128)] = first[:, 512:640] + moved[:, 0:128]
    out[pl.ds(s, 1), pl.ds(base + 640, 512)] = moved[:, 128:640]


def middle_kernel(
    info, levels, near, rates, diffusivity, stoichiometry, own, other, held, up_own, up_other, down_own, down_other,
    up_before, down_before, out, up, down, table,
    raw, mid, done, rest, old, flux, whole, sem,
):
    layer, core = info[0], info[1]
    index = grow_index()
    incoming = ((up_own, up_other), (down_own, down_other))
    row, lane = iota(CHUNK, 0), iota(CHUNK, 1)
    below, above = [
        jnp.where(row < 4, one[4, pl.ds(0, 8), :], pltpu.roll(two[4, pl.ds(0, 8), :], 4, 0)) for one, two in incoming
    ]
    whole[...] = jnp.where(lane < 16, below, roll_lanes(above, 16)).astype(jnp.int32)
    copy = pltpu.make_async_copy(whole, table, sem)
    copy.start()
    for way in range(2):
        for half in range(2):
            put(rest, (way, half), chunks(incoming[way][half], 4))

    def fine_of(b):
        return levels[layer * 8 + spot(b, core)] == 1

    for half, ref_in in enumerate((own, other)):

        @pl.loop(0, 4)
        def _(i):
            for m in range(9):
                put(old, (half * 4 + i, m), chunks(ref_in, i * PER_BLOCK + 27 + m))

    copy.wait()
    arrive(info, levels, table, core, incoming, raw, mid, done)

    @pl.loop(0, 4)
    def _(b):
        @pl.when(fine_of(b))
        def _():
            below, above = spot(near[b, 4], core), spot(near[b, 5], core)

            @pl.loop(0, 4)
            def _(v):
                at = chunk_at(v)
                g = z_section(lambda p: held[b, p, at, :], done[0, below, at, :], done[1, above, at, :], depth_of())
                post, j = collide(g, lambda k: rates[k])
                for p in range(27):
                    out[b * PER_BLOCK + p, at, :] = post[p]
                for d in range(3):
                    flux[d, at, :] = j[d] * (0.5 / 216.0)

            def store(m, v, value):
                out[b * PER_BLOCK + 27 + m, pl.ds(8 * v, 8), :] = value

            species_step(
                old, b, [spot(near[b, q], core) for q in range(4)], face_reader(done, rest, below, above), flux,
                [levels[near[b, q]] for q in range(6)], diffusivity, stoichiometry, store,
            )

        @pl.when(jnp.logical_not(fine_of(b)))
        def _():
            for p in range(27):
                for v in range(4):
                    line = own[b * PER_BLOCK + 27 + p // 8, pl.ds(p % 8 * 4 + v, 1), :]
                    out[b * PER_BLOCK + p, pl.ds(8 * v, 8), :] = grow_row(line, index)
            for m in range(9):
                put(out, (b * PER_BLOCK + 27 + m,), [jnp.zeros((CHUNK, LANES), F32)] * 4)

    pack_faces(out, up, down)
    row, lane = iota(CHUNK, 0), iota(CHUNK, 1)

    @pl.loop(0, 4)
    def _(v):
        at = chunk_at(v)
        for ref, before in ((up, up_before), (down, down_before)):
            merged = None
            for b in range(4):
                total = 0.125 * (before[b, at, :] + ref[b, at, :])
                total = total + pltpu.roll(total, CHUNK - 2, 0)
                total = total + roll_lanes(total, -16)
                if b % 2:
                    total = pltpu.roll(total, 2, 0)
                if b // 2:
                    total = roll_lanes(total, 16)
                here = jnp.logical_and(row // 2 % 2 == b % 2, lane // 16 % 2 == b // 2)
                merged = total if merged is None else jnp.where(here, total, merged)
            ref[5, at, :] = merged


def depth_of():
    return iota(CHUNK, 1) % 16


def second_plane_kernel(
    info, levels, near, own, other, own_before, other_before, tables, dest, sides_out, mid, faces, edge_x, edge_y,
    needed, picked_x, picked_y, spread,
):
    layer, core = info[0], info[1]

    def fine_of(b):
        return levels[layer * 8 + spot(b, core)] == 1

    sections_xy((own, other), faces, mid, dest, near, core, fine_of)
    for b in range(8):
        needed[b] = 0
    for s in range(4):
        for q in range(4):

            @pl.when(jnp.logical_not(fine_of(s)))
            def _(s=s, q=q):
                needed[spot(near[s, q], core)] = 1

    group, odd = iota(CHUNK, 1) // 16, iota(CHUNK, 0) % 2 == 1
    for half, (one, two) in enumerate(((own_before, own), (other_before, other))):

        @pl.loop(0, 4)
        def _(i):
            b = half * 4 + i

            def total(p, at):
                return one[i * PER_BLOCK + p, at, :] + two[i * PER_BLOCK + p, at, :]

            @pl.when(jnp.logical_and(fine_of(b), needed[b] == 1))
            def _():
                for side in range(2):
                    at = pl.ds(30, 2) if side == 0 else pl.ds(0, 2)
                    for e in range(9):
                        edge_x[b, side, pl.ds(2 * e, 2), :] = total(18 + e if side == 0 else e, at)
                    edge_x[b, side, pl.ds(18, 14), :] = jnp.zeros((14, LANES), F32)
                for v in range(4):
                    at = pl.ds(8 * v, 8)
                    packs = [None, None]
                    for e in range(9):
                        p_low = 9 * (e // 3) + e % 3
                        slot = e % 8
                        high = roll_lanes(total(p_low + 6, at), 16 * (slot - 7))
                        both = jnp.where(odd, high, roll_lanes(total(p_low, at), 16 * slot))
                        held_pack = packs[e // 8]
                        packs[e // 8] = both if held_pack is None else jnp.where(group == slot, both, held_pack)
                    for a in range(2):
                        edge_y[b, a, at, :] = packs[a]

    row, col = wide_iota(0), wide_iota(1)
    e_of, cell = col // 64, col % 64
    keep_x = jnp.logical_and(row // 2 == e_of, row % 2 == cell // 32)
    keep_y = row // 4 == cell // 8
    odd_row = row % 2 == 1
    any_coarse = jnp.logical_not(jnp.logical_and(jnp.logical_and(fine_of(0), fine_of(1)), jnp.logical_and(fine_of(2), fine_of(3))))
    sides_out[...] = jnp.zeros((4, 2304), F32)

    @pl.when(any_coarse)
    def _():
        for q in range(4):
            for s in range(4):
                live = jnp.logical_and(jnp.logical_not(fine_of(s)), levels[near[s, q]] == 1)
                m = spot(near[s, q], core)
                rows = pl.ds((q % 2 * 4 + s) * ROWS, ROWS)
                if q < 2:
                    picked_x[rows, :] = jnp.where(live, 0.125 * edge_x[m, q], 0.0)
                else:
                    for a in range(2):
                        picked_y[rows, pl.ds(a * LANES, LANES)] = jnp.where(live, 0.125 * edge_y[m, a], 0.0)
        for pair, picked, weights in ((0, picked_x, tables[0:128, :]), (1, picked_y, tables[128:384, :])):
            spread[...] = times(picked[...], weights)
            for s in range(4):
                keeps = (keep_x, keep_x)
                if pair:
                    keeps = (jnp.logical_and(keep_y, odd_row), jnp.logical_and(keep_y, jnp.logical_not(odd_row)))
                put_pair(
                    sides_out, s, pair * 1152,
                    column_sums(spread, s, keeps[0]), column_sums(spread, 4 + s, keeps[1]),
                )


def end_kernel(
    info, levels, near, table, diffusivity, stoichiometry, held, own, other,
    up_own, up_other, down_own, down_other, sides, weights, pop, scal,
    pop_out, scal_out, returned,
    raw, mid, done, rest, returning, species, pops, scals, flux, picked, spread, sems,
):
    layer, core = info[0], info[1]
    incoming = ((up_own, up_other), (down_own, down_other))
    for half, ref_in in enumerate((own, other)):

        @pl.loop(0, 4)
        def _(i):
            for m in range(9):
                put(species, (half * 4 + i, m), chunks(ref_in, i * PER_BLOCK + 27 + m))

        for way in range(2):
            put(rest, (way, half), chunks(incoming[way][half], 4))
            put(returning, (way, half), chunks(incoming[way][half], 5))

    arrive(info, levels, table, core, incoming, raw, mid, done)
    depth = iota(CHUNK, 1) % 16
    row, col = wide_iota(0), wide_iota(1)
    keep = row // 4 * 2 + row % 2 == col % 64 // 4
    slim, wide = iota(ROWS, 0), iota(ROWS, 1)

    def fine_of(s):
        return levels[layer * 8 + core * 4 + s] == 1

    copies = []
    for v in range(4):
        at = pl.ds(8 * v, 8)

        @pl.loop(0, 4)
        def _(s):
            rows = pl.ds(32 * v + s, 8, stride=4)

            @pl.when(fine_of(s))
            def _():
                below, above = spot(near[s, 4], core), spot(near[s, 5], core)
                g = z_section(lambda p: held[s, p, at, :], done[0, below, at, :], done[1, above, at, :], depth)
                for p in range(27):
                    pops[p, rows, :] = g[p]
                m = forward_moments(g)
                for d, i in enumerate((9, 3, 1)):
                    flux[s, d, at, :] = m[i] * (0.5 / 216.0)

            @pl.when(jnp.logical_not(fine_of(s)))
            def _():
                for p in range(27):
                    pops[p, rows, :] = pop[p, rows, :]

        rows = pl.ds(32 * v, 32)
        copies.append(pltpu.make_async_copy(pops.at[:, rows, :], pop_out.at[:, rows, :], sems.at[v]))
        copies[-1].start()

    @pl.loop(0, 4)
    def _(s):
        @pl.when(fine_of(s))
        def _():
            def store(m, v, value):
                scals[m, pl.ds(32 * v + s, 8, stride=4), :] = value

            species_step(
                species, s, [spot(near[s, q], core) for q in range(4)],
                face_reader(done, rest, spot(near[s, 4], core), spot(near[s, 5], core)), flux.at[s],
                [levels[near[s, q]] for q in range(6)], diffusivity, stoichiometry, store,
            )

        @pl.when(jnp.logical_not(fine_of(s)))
        def _():
            for v in range(4):
                at = pl.ds(32 * v + s, 8, stride=4)
                for m in range(9):
                    scals[m, at, :] = scal[m, at, :]

    copies.append(pltpu.make_async_copy(scals, scal_out, sems.at[4]))
    copies[-1].start()
    returned[:, 0:2304] = sides[...]
    returned[:, 2304:3456] = jnp.zeros((4, 1152), F32)
    any_coarse = jnp.logical_not(jnp.logical_and(jnp.logical_and(fine_of(0), fine_of(1)), jnp.logical_and(fine_of(2), fine_of(3))))

    @pl.when(any_coarse)
    def _():
        for way in range(2):
            for s in range(4):
                m = spot(near[s, 4 + way], core)
                here = jnp.logical_and(slim // 2 % 2 == m % 2, wide // 16 % 2 == m % 4 // 2)
                live = jnp.logical_and(jnp.logical_not(fine_of(s)), levels[near[s, 4 + way]] == 1)
                face = jnp.where(jnp.logical_and(here, live), returning[way, m // 4], 0.0)
                picked[pl.ds((way * 4 + s) * ROWS, ROWS), :] = face
        spread[...] = times(picked[...], weights[...])
        for s in range(4):
            put_pair(returned, s, 2304, column_sums(spread, s, keep), column_sums(spread, 4 + s, keep))

    for copy in copies:
        copy.wait()


def specs(kinds):
    table = {
        "s": pl.BlockSpec(memory_space=pltpu.SMEM),
        "v": pl.BlockSpec(memory_space=pltpu.VMEM),
        "h": pl.BlockSpec(memory_space=pltpu.HBM),
    }
    return [table[kind] for kind in kinds]


def call(kernel, kinds, outs, out_kinds, scratch, name, megabytes, flops):
    return pl.pallas_call(
        kernel,
        in_specs=specs(kinds),
        out_specs=specs(out_kinds),
        out_shape=outs,
        scratch_shapes=scratch,
        name=name,
        compiler_params=pltpu.CompilerParams(vmem_limit_bytes=megabytes << 20),
        cost_estimate=pl.CostEstimate(flops=flops, transcendentals=0, bytes_accessed=8 << 20),
    )


def interleave(x):
    blocks, n, cells = x.shape
    x = x.reshape(blocks, n, cells // LANES, LANES)
    return jnp.transpose(x, (1, 2, 0, 3)).reshape(n, cells // LANES * blocks, LANES)


def separate(x):
    n, rows, _ = x.shape
    x = jnp.transpose(x.reshape(n, rows // 4, 4, LANES), (2, 0, 1, 3))
    return x.reshape(4, n, rows // 4 * LANES)


def local(
    populations, scalars, coarse_old, coarse_new, levels, neighbours, relax_rates, diffusivity, stoichiometry
):
    devices = lax.axis_size("blk")
    me = lax.axis_index("blk")
    layer, layers = me // 2, devices // 2
    info = jnp.stack([layer, me % 2, (layer + layers - 1) % layers, (layer + 1) % layers]).astype(jnp.int32)
    swap = [(i, i ^ 1) for i in range(devices)]
    rise = [(i, (i + 2) % devices) for i in range(devices)]
    fall = [(i, (i - 2) % devices) for i in range(devices)]

    def move(x, pairs):
        return lax.ppermute(x, "blk", pairs)

    def vmem(*lead):
        return pltpu.VMEM((*lead, ROWS, LANES), F32)

    full = (ROWS, LANES)
    pop, scal = interleave(populations), interleave(scalars)
    old, new = interleave(coarse_old), interleave(coarse_new)
    side_table, z_table = reduce_tables()
    fields = FIELDS - 1
    semaphores = pltpu.SemaphoreType.DMA
    own, up, down = call(
        begin_kernel,
        "shhhhhhh",
        [shape_of(FIELDS, *full), shape_of(5, *full), shape_of(5, *full)],
        "vvv",
        [pltpu.VMEM(x.shape, F32) for x in (pop, scal, old, new)]
        + [pltpu.SMEM(x.shape, x.dtype) for x in (levels, neighbours, relax_rates)]
        + [semaphores((10,))],
        "begin",
        12,
        1 << 27,
    )(info, *[pltpu.with_memory_space_constraint(x, pltpu.HBM) for x in (levels, neighbours, relax_rates, pop, scal, old, new)])
    other = move(own, swap)
    up_sent, down_sent = up, down
    up, down = move(up, rise), move(down, fall)
    face = pltpu.VMEM((8, 27, CHUNK, LANES), F32)
    held, near = call(
        plane_kernel,
        "ssvv",
        [shape_of(4, 27, *full), jax.ShapeDtypeStruct((CHUNK, LANES), jnp.int32)],
        "vs",
        [vmem(8, 27), face, pltpu.VMEM((CHUNK, LANES), jnp.int32), semaphores],
        "plane",
        12,
        1 << 27,
    )(info, levels, own, other)
    held, up, down = lax.optimization_barrier((held, up, down))
    landing = [vmem(2, 8), vmem(2, 8), vmem(2, 8), vmem(2, 2)]
    own_next, up_next, down_next, table = call(
        middle_kernel,
        "ssssssvvvvvvvvv",
        [shape_of(fields, *full), shape_of(6, *full), shape_of(6, *full), jax.ShapeDtypeStruct((CHUNK, LANES), jnp.int32)],
        "vvvs",
        landing + [vmem(8, 9), vmem(3), pltpu.VMEM((CHUNK, LANES), jnp.int32), semaphores],
        "middle",
        14,
        1 << 28,
    )(
        info, levels, near, relax_rates, diffusivity, stoichiometry, own, other, held,
        up, move(up, swap), down, move(down, swap), up_sent, down_sent,
    )
    other_next = move(own_next, swap)
    up, down = move(up_next, rise), move(down_next, fall)
    held, sides = call(
        second_plane_kernel,
        "sssvvvvv",
        [shape_of(4, 27, *full), shape_of(4, 2304)],
        "vv",
        [vmem(8, 27), face, vmem(8, 2), vmem(8, 2), pltpu.SMEM((8,), jnp.int32)]
        + [pltpu.VMEM((8 * ROWS, LANES), F32), pltpu.VMEM((8 * ROWS, 2 * LANES), F32), pltpu.VMEM((8 * ROWS, WIDE), F32)],
        "plane2",
        14,
        1 << 27,
    )(info, levels, near, own_next, other_next, own, other, side_table)
    held, sides, up, down = lax.optimization_barrier((held, sides, up, down))
    pop_out, scal_out, returned = call(
        end_kernel,
        "ssssssvvvvvvvvvvv",
        [shape_of(27, 128, LANES), shape_of(9, 128, LANES), shape_of(4, 3456)],
        "hhv",
        landing
        + [vmem(2, 2), vmem(8, 9), pltpu.VMEM(pop.shape, F32), pltpu.VMEM(scal.shape, F32), vmem(4, 3)]
        + [pltpu.VMEM((8 * ROWS, LANES), F32), pltpu.VMEM((8 * ROWS, WIDE), F32), semaphores((5,))],
        "end",
        16,
        1 << 27,
    )(
        info, levels, neighbours, table, diffusivity, stoichiometry, held, own_next, other_next,
        up, move(up, swap), down, move(down, swap), sides, z_table, pop, scal,
    )
    return separate(pop_out), separate(scal_out), returned


def solution(mesh):
    in_specs = (
        P("blk", None, None), P("blk", None, None), P("blk", None, None), P("blk", None, None),
        P(), P("blk", None), P(), P(), P(),
    )
    out_specs = (P("blk", None, None), P("blk", None, None), P("blk", None))
    return jax.shard_map(local, mesh=mesh, in_specs=in_specs, out_specs=out_specs, check_vma=False)
```

```python
import jax
import jax.numpy as jnp
import numpy as np
from jax import lax
from jax.experimental import pallas as pl
from jax.experimental.pallas import tpu as pltpu
from jax.sharding import PartitionSpec as P

F32 = jnp.float32
VEL = [(a, b, c) for a in (-1, 0, 1) for b in (-1, 0, 1) for c in (-1, 0, 1)]
ROWS, LANES = 32, 128
CHUNK = 8


def shape_of(*dims):
    return jax.ShapeDtypeStruct(dims, F32)


def iota(rows, axis):
    return lax.broadcasted_iota(jnp.int32, (rows, LANES), axis)


def chunk_at(v):
    return pl.ds(pl.multiple_of(v * CHUNK, CHUNK), CHUNK)


def roll_lanes(x, by):
    if isinstance(by, int):
        by = by % LANES
        if by == 0:
            return x
    return pltpu.roll(x, by, 1)


def forward_moments(values):
    out = list(values)
    for stride in (9, 3, 1):
        for i in range(27):
            if (i // stride) % 3 == 0:
                low, mid, high = out[i], out[i + stride], out[i + 2 * stride]
                both = low + high
                out[i] = both + 4.0 * mid
                out[i + stride] = high - low
                out[i + 2 * stride] = both
    return out


def plus(x, y):
    if x is None:
        return y
    return x if y is None else x + y


def minus(x, y):
    if y is None:
        return x
    return -y if x is None else x - y


def backward_moments(values):
    out = list(values)
    for stride in (9, 3, 1):
        for i in range(27):
            if (i // stride) % 3 == 0:
                m0, m1, m2 = out[i], out[i + stride], out[i + 2 * stride]
                out[i] = minus(m2, m1)
                out[i + stride] = minus(m0, m2)
                out[i + 2 * stride] = plus(m1, m2)
    return out


def collide(g, rate):
    m = forward_moments(g)
    rho = m[0]
    j = (m[9], m[3], m[1])
    square = [x * x * (1.0 / 72.0) for x in j]
    relaxed = [None] * 27
    for k in range(27):
        digits = (k // 9, (k // 3) % 3, k % 3)
        odd = [d for d in range(3) if digits[d] == 1]
        twos = [d for d in range(3) if digits[d] == 2]
        if k in (0, 9, 3, 1):
            continue
        if not odd:
            level = rho
            for d in twos:
                level = level + square[d]
        elif len(odd) == 1:
            level = j[odd[0]]
        elif len(odd) == 2:
            level = j[odd[0]] * j[odd[1]] * (1.0 / 216.0)
        else:
            level = None
        if level is not None and twos:
            level = level * (3.0 ** -len(twos))
        relaxed[k] = minus(m[k], level) * (rate(k) * (1.0 / 64.0))
    back = backward_moments(relaxed)
    post = []
    for i, c in enumerate(VEL):
        factor = 2.0 ** sum(abs(x) for x in c)
        post.append(g[i] - (back[i] if factor == 1.0 else factor * back[i]))
    return post, j


def grow_index():
    r, l = iota(CHUNK, 0), iota(CHUNK, 1)
    return (r // 4) % 2 * 64 + r % 2 * 32 + l // 32 * 8 + l % 16 // 2


def grow_row(row, index):
    return jnp.take_along_axis(jnp.broadcast_to(row, (CHUNK, LANES)), index, axis=1)


PER_BLOCK = 36
FIELDS = 4 * PER_BLOCK + 1


def fetch(sources, targets, sems, first=0):
    copies = [pltpu.make_async_copy(a, b, sems.at[first + i]) for i, (a, b) in enumerate(zip(sources, targets))]
    for copy in copies:
        copy.start()

    def ready():
        for copy in copies:
            copy.wait()

    return ready


def begin_kernel(
    info_in, levels_in, near_in, rates_in, pop, scal, old, new, out, up, down,
    pops, scals, olds, news, info, levels, near, rates, sems,
):
    ready = fetch((info_in, levels_in, near_in, rates_in), (info, levels, near, rates), sems, 7)
    copies = []
    for v in range(4):
        rows = pl.ds(32 * v, 32)
        copies.append(pltpu.make_async_copy(pop.at[:, rows, :], pops.at[:, rows, :], sems.at[v]))
    copies.append(pltpu.make_async_copy(old, olds, sems.at[4]))
    copies.append(pltpu.make_async_copy(new, news, sems.at[5]))
    copies.append(pltpu.make_async_copy(scal, scals, sems.at[6]))
    for copy in copies:
        copy.start()
    index = grow_index()
    ready()
    layer, core = info[0], info[1]
    row, lane = iota(CHUNK, 0), iota(CHUNK, 1)
    meta = jnp.zeros((CHUNK, LANES), F32)
    for b in range(4):
        for q in range(6):
            here = jnp.logical_and(row == b, lane == q + 8)
            meta = jnp.where(here, near[b, q].astype(F32), meta)
    out[FIELDS - 1, 0:8, :] = meta

    def fine_of(b):
        return levels[layer * 8 + core * 4 + b] == 1

    for v in range(4):
        copies[v].wait()

        @pl.loop(0, 4)
        def _(b):
            @pl.when(fine_of(b))
            def _():
                at = pl.ds(8 * v, 8)
                from_rows = pl.ds(32 * v + b, 8, stride=4)
                post, _j = collide([pops[p, from_rows, :] for p in range(27)], lambda k: rates[k])
                for p in range(27):
                    out[b * PER_BLOCK + p, at, :] = post[p]

    for copy in copies[4:]:
        copy.wait()

    @pl.loop(0, 4)
    def _(b):
        @pl.when(fine_of(b))
        def _():
            for m in range(9):
                for v in range(4):
                    out[b * PER_BLOCK + 27 + m, pl.ds(8 * v, 8), :] = scals[m, pl.ds(32 * v + b, 8, stride=4), :]

        @pl.when(jnp.logical_not(fine_of(b)))
        def _():
            for p in range(27):
                for v in range(4):
                    before = olds[p, pl.ds(4 * v + b, 1), :]
                    after = news[p, pl.ds(4 * v + b, 1), :]
                    out[b * PER_BLOCK + 27 + p // 8, pl.ds(p % 8 * 4 + v, 1), :] = 0.5 * (before + after)
                    out[b * PER_BLOCK + p, pl.ds(8 * v, 8), :] = grow_row(before, index)


    pack_faces(out, up, down, meta)


def pack_faces(out, up, down, meta=None):
    lane = iota(CHUNK, 1) % 16

    @pl.loop(0, 4)
    def _(v):
        at = chunk_at(v)
        for ref, digit, start in ((up, 2, 15), (down, 0, 0)):
            for b in range(4):
                fields = [out[b * PER_BLOCK + 3 * e + digit, at, :] for e in range(9)]
                fields += [out[b * PER_BLOCK + 27 + e, at, :] for e in range(7)]
                ref[b, at, :] = pack_into(fields, 0, start, lane)
            rest = pack_into([out[b * PER_BLOCK + 34 + e, at, :] for b in range(4) for e in range(2)], 0, start, lane)
            ref[4, at, :] = rest if meta is None else jnp.where(lane < 8, rest, meta)


def spot(block, core):
    return (block % 8) ^ (core * 4)


def y_up(own, beside, even, group):
    turned = jnp.where(even, pltpu.roll(beside, CHUNK - 1, 0), pltpu.roll(own, 1, 0))
    return roll_lanes(jnp.where(group < 7, own, turned), 16)


def y_down(own, beside, even, group):
    turned = jnp.where(even, pltpu.roll(own, CHUNK - 1, 0), pltpu.roll(beside, 1, 0))
    return roll_lanes(jnp.where(group > 0, own, turned), -16)


def chunks(ref, *lead):
    return [ref[(*lead, pl.ds(8 * v, 8), slice(None))] for v in range(4)]


def x_up(own, beyond, row):
    turned = [pltpu.roll(x, 2, 0) for x in own]
    before = [beyond] + turned[:3]
    return [jnp.where(row < 2, a, b) for a, b in zip(before, turned)]


def x_down(own, beyond, row):
    turned = [pltpu.roll(x, CHUNK - 2, 0) for x in own]
    after = turned[1:] + [beyond]
    return [jnp.where(row >= 6, a, b) for a, b in zip(after, turned)]


def put(ref, lead, values):
    for v in range(4):
        ref[(*lead, pl.ds(8 * v, 8), slice(None))] = values[v]


def sections_xy(refs, faces, mid, dest, info, levels, near, ready):
    row = iota(CHUNK, 0)
    even = row % 2 == 0
    group = iota(CHUNK, 1) // 16

    for half, ref in enumerate(refs):

        @pl.loop(0, 4)
        def _(i):
            for p, c in enumerate(VEL):
                if c[0] == 1:
                    faces[half * 4 + i, p] = pltpu.roll(ref[i * PER_BLOCK + p, pl.ds(24, 8), :], 2, 0)
                elif c[0] == -1:
                    faces[half * 4 + i, p] = pltpu.roll(ref[i * PER_BLOCK + p, pl.ds(0, 8), :], CHUNK - 2, 0)

    ready()
    core = info[1]
    fine_of = fine_in(info, levels)

    for half, ref in enumerate(refs):

        @pl.loop(0, 4)
        def _(i):
            b = half * 4 + i
            fine = fine_of(b)
            fields = [p for p in range(27) if half == 0 or VEL[p][1] != 0]

            @pl.when(fine)
            def _():
                low, high = spot(near[b, 0], core), spot(near[b, 1], core)
                for p in fields:
                    values = chunks(ref, i * PER_BLOCK + p)
                    if VEL[p][0] == 1:
                        values = x_up(values, faces[low, p], row)
                    elif VEL[p][0] == -1:
                        values = x_down(values, faces[high, p], row)
                    put(mid, (b, p), values)

            @pl.when(jnp.logical_not(fine))
            def _():
                for p in fields:
                    if VEL[p][1] != 0:
                        put(mid, (b, p), chunks(ref, i * PER_BLOCK + p))

    @pl.loop(0, 4)
    def _(b):
        @pl.when(fine_of(b))
        def _():
            low, high = spot(near[b, 2], core), spot(near[b, 3], core)
            for p, c in enumerate(VEL):
                for v in range(4):
                    at = pl.ds(8 * v, 8)
                    value = mid[b, p, at, :]
                    if c[1] == 1:
                        value = y_up(value, mid[low, p, at, :], even, group)
                    elif c[1] == -1:
                        value = y_down(value, mid[high, p, at, :], even, group)
                    dest[b, p, at, :] = value


def pack_into(fields, first_slot, start, lane):
    out = None
    for e, field in enumerate(fields):
        slot = first_slot + e
        moved = roll_lanes(field, slot - start)
        out = moved if out is None else jnp.where(lane == slot, moved, out)
    return out


def fine_in(info, levels):
    return lambda b: levels[info[0] * 8 + spot(b, info[1])] == 1


def plane_kernel(
    info_in, levels_in, diffusivity_in, stoichiometry_in, own, other, dest, table, parts,
    mid, faces, old, info, levels, near, diffusivity, stoichiometry, sems,
):
    row = iota(CHUNK, 0)
    both = jnp.where(row < 4, own[FIELDS - 1, 0:8, :], pltpu.roll(other[FIELDS - 1, 0:8, :], 4, 0))
    table[...] = roll_lanes(both, -8).astype(jnp.int32)
    ready = fetch(
        (info_in, levels_in, table, diffusivity_in, stoichiometry_in), (info, levels, near, diffusivity, stoichiometry), sems
    )
    gather_species((own, other), old)
    sections_xy((own, other), faces, mid, dest, info, levels, near, ready)
    species_begin(old, parts, info, levels, near, diffusivity, stoichiometry)


def settle(incoming, raw):
    for way in range(2):
        for half in range(2):
            for i in range(4):
                put(raw, (way, half * 4 + i), chunks(incoming[way][half], i))


def arrive(info, levels, table, core, raw, mid, done):
    row, slot = iota(CHUNK, 0), iota(CHUNK, 1) % 16
    even, group = row % 2 == 0, iota(CHUNK, 1) // 16
    x_plus, x_minus = jnp.logical_and(slot >= 6, slot < 9), slot < 3
    y_plus = jnp.logical_and(slot < 9, slot % 3 == 2)
    y_minus = jnp.logical_and(slot < 9, slot % 3 == 0)
    blocks = [(way, b) for way in range(2) for b in range(8)]
    fine = [levels[info[2 + way] * 8 + spot(b, core)] == 1 for way, b in blocks]

    def beside(way, b, q):
        return spot(table[b, 16 * way + 8 + q], core)

    for (way, b), flag in zip(blocks, fine):
        own = chunks(raw, way, b)
        before = x_up(own, pltpu.roll(raw[way, beside(way, b, 0), pl.ds(24, 8), :], 2, 0), row)
        after = x_down(own, pltpu.roll(raw[way, beside(way, b, 1), pl.ds(0, 8), :], CHUNK - 2, 0), row)
        to_plus, to_minus = jnp.logical_and(x_plus, flag), jnp.logical_and(x_minus, flag)
        put(mid, (way, b), [jnp.where(to_plus, x, jnp.where(to_minus, y, z)) for x, y, z in zip(before, after, own)])
    for (way, b), flag in zip(blocks, fine):
        low, high = beside(way, b, 2), beside(way, b, 3)
        to_plus, to_minus = jnp.logical_and(y_plus, flag), jnp.logical_and(y_minus, flag)
        for v in range(4):
            at = pl.ds(8 * v, 8)
            here = mid[way, b, at, :]
            before = y_up(here, mid[way, low, at, :], even, group)
            after = y_down(here, mid[way, high, at, :], even, group)
            done[way, b, at, :] = jnp.where(to_plus, before, jnp.where(to_minus, after, here))


def face_reader(done, rest, below, above):
    def faces(m, at):
        if m < 7:
            slot = 9 + m
            return roll_lanes(done[0, below, at, :], -slot), roll_lanes(done[1, above, at, :], 15 - slot)
        low = LANES - 2 * (below % 4) - (m - 7)
        high = (LANES + 15 - 2 * (above % 4) - (m - 7)) % LANES
        return pltpu.roll(rest[0, below // 4, at, :], low, 1), pltpu.roll(rest[1, above // 4, at, :], high, 1)

    return faces


def z_section(h, up, down, depth):
    g = []
    for p, c in enumerate(VEL):
        e = p // 3
        value = h(p)
        if c[2] == 1:
            value = jnp.where(depth == 0, roll_lanes(up, -e), roll_lanes(value, 1))
        elif c[2] == -1:
            value = jnp.where(depth == 15, roll_lanes(down, 15 - e), roll_lanes(value, -1))
        g.append(value)
    return g


def gather_species(halves, old):
    for half, ref_in in enumerate(halves):

        @pl.loop(0, 4)
        def _(i):
            for m in range(9):
                put(old, (half * 4 + i, m), chunks(ref_in, i * PER_BLOCK + 27 + m))


def species_begin(y_ref, parts, info, levels, near, diffusivity, stoichiometry):
    row, lanes = iota(CHUNK, 0), iota(CHUNK, 1)
    even = row % 2 == 0
    group, depth = lanes // 16, lanes % 16
    fine_of = fine_in(info, levels)

    @pl.loop(0, 4)
    def _(b):
        @pl.when(fine_of(b))
        def _():
            def gone(edge, q):
                return jnp.logical_and(edge, levels[near[b, q]] != 1)

            lost = [
                gone(row < 2, 0), gone(row >= 6, 1),
                gone(jnp.logical_and(even, group == 0), 2),
                gone(jnp.logical_and(jnp.logical_not(even), group == 7), 3),
            ]
            sides = [spot(near[b, q], info[1]) for q in range(4)]
            burning = [
                x * y * jnp.exp(4.0 * (t - 1.0))
                for x, y, t in zip(chunks(y_ref, b, 0), chunks(y_ref, b, 1), chunks(y_ref, b, 8))
            ]
            for m in range(9):
                y = chunks(y_ref, b, m)
                low_x = pltpu.roll(y_ref[sides[0], m, pl.ds(24, 8), :], 2, 0)
                high_x = pltpu.roll(y_ref[sides[1], m, pl.ds(0, 8), :], CHUNK - 2, 0)
                lower_x, upper_x = x_up(y, low_x, row), x_down(y, high_x, row)
                lower_x[0] = jnp.where(lost[0], y[0], lower_x[0])
                upper_x[3] = jnp.where(lost[1], y[3], upper_x[3])
                for v in range(4):
                    at = pl.ds(8 * v, 8)
                    here = y[v]
                    pairs = [
                        (lower_x[v], upper_x[v]),
                        (
                            jnp.where(lost[2], here, y_up(here, y_ref[sides[2], m, at, :], even, group)),
                            jnp.where(lost[3], here, y_down(here, y_ref[sides[3], m, at, :], even, group)),
                        ),
                        (
                            jnp.where(depth == 0, here, roll_lanes(here, 1)),
                            jnp.where(depth == 15, here, roll_lanes(here, -1)),
                        ),
                    ]
                    spread = None
                    for d, (lower, upper) in enumerate(pairs):
                        parts[b * PER_BLOCK + 9 + 9 * d + m, at, :] = upper - lower
                        both = upper + lower
                        spread = both if spread is None else spread + both
                    parts[b * PER_BLOCK + m, at, :] = (
                        here + diffusivity[m] * (spread - 6.0 * here) + stoichiometry[m] * burning[v]
                    )


def species_end(parts, b, y_of, faces, flux, flags, diffusivity, store):
    depth = iota(CHUNK, 1) % 16
    at_low = jnp.logical_and(depth == 0, flags[0] == 1)
    at_high = jnp.logical_and(depth == 15, flags[1] == 1)
    for v in range(4):
        at = pl.ds(8 * v, 8)
        flow = [flux[d, at, :] for d in range(3)]
        for m in range(9):
            here = y_of(m, at)
            low, high = faces(m, at)
            low = jnp.where(at_low, low - here, 0.0)
            high = jnp.where(at_high, high - here, 0.0)
            base, along_x, along_y, along_z = (parts[b * PER_BLOCK + 9 * kind + m, at, :] for kind in range(4))
            drift = flow[0] * along_x + flow[1] * along_y + flow[2] * (along_z + (high - low))
            store(m, v, base - drift + diffusivity[m] * (low + high))


WIDE = 640


def reduce_tables():
    l = np.arange(LANES)[:, None]
    c = np.arange(WIDE)[None, :]
    e, cell = c // 64, c % 64
    live = c < 576
    along_x = (l // 32 * 8 + l % 16 // 2 == cell % 32) & live
    along_y = [(l // 16 + 8 * a == e) & (l % 16 // 2 == cell % 8) & live for a in range(2)]
    along_z = (l % 16 == e) & (l // 32 == cell % 4) & live
    side = np.concatenate([along_x, along_y[0], along_y[1]], axis=0)
    return jnp.asarray(side, jnp.bfloat16), jnp.asarray(along_z, jnp.bfloat16)


def wide_iota(axis):
    return lax.broadcasted_iota(jnp.int32, (ROWS, WIDE), axis)


def times(x, w):
    total = None
    for _ in range(3):
        part = x.astype(jnp.bfloat16)
        x = x - part.astype(F32)
        product = jnp.dot(part, w, preferred_element_type=F32)
        total = product if total is None else total + product
    return total


def column_sums(spread, k, keep):
    return jnp.sum(jnp.where(keep, spread[pl.ds(k * ROWS, ROWS), :], 0.0), axis=0, keepdims=True)


def put_pair(out, s, base, first, second):
    moved = pltpu.roll(second, 64, 1)
    out[pl.ds(s, 1), pl.ds(base, 512)] = first[:, 0:512]
    out[pl.ds(s, 1), pl.ds(base + 512, 128)] = first[:, 512:640] + moved[:, 0:128]
    out[pl.ds(s, 1), pl.ds(base + 640, 512)] = moved[:, 128:640]


def middle_kernel(
    info_in, levels_in, near_in, rates_in, diffusivity_in, own, held, parts, up_own, up_other, down_own, down_other,
    out, up, down, table,
    raw, mid, done, rest, flux,
    info, levels, near, rates, diffusivity, far, sems,
):
    index = grow_index()
    incoming = ((up_own, up_other), (down_own, down_other))
    row, lane = iota(CHUNK, 0), iota(CHUNK, 1)
    below, above = [
        jnp.where(row < 4, one[4, pl.ds(0, 8), :], pltpu.roll(two[4, pl.ds(0, 8), :], 4, 0)) for one, two in incoming
    ]
    table[...] = jnp.where(lane < 16, below, roll_lanes(above, 16)).astype(jnp.int32)
    ready = fetch(
        (info_in, levels_in, near_in, rates_in, diffusivity_in, table),
        (info, levels, near, rates, diffusivity, far),
        sems,
    )
    settle(incoming, raw)
    for way in range(2):
        for half in range(2):
            put(rest, (way, half), chunks(incoming[way][half], 4))

    ready()
    core = info[1]
    fine_of = fine_in(info, levels)
    arrive(info, levels, far, core, raw, mid, done)

    @pl.loop(0, 4)
    def _(b):
        @pl.when(fine_of(b))
        def _():
            below, above = spot(near[b, 4], core), spot(near[b, 5], core)

            @pl.loop(0, 4)
            def _(v):
                at = chunk_at(v)
                g = z_section(lambda p: held[b, p, at, :], done[0, below, at, :], done[1, above, at, :], depth_of())
                post, j = collide(g, lambda k: rates[k])
                for p in range(27):
                    out[b * PER_BLOCK + p, at, :] = post[p]
                for d in range(3):
                    flux[d, at, :] = j[d] * (0.5 / 216.0)

            def store(m, v, value):
                out[b * PER_BLOCK + 27 + m, pl.ds(8 * v, 8), :] = value

            species_end(
                parts, b, lambda m, at: own[b * PER_BLOCK + 27 + m, at, :], face_reader(done, rest, below, above), flux,
                [levels[near[b, q]] for q in (4, 5)], diffusivity, store,
            )

        @pl.when(jnp.logical_not(fine_of(b)))
        def _():
            for p in range(27):
                for v in range(4):
                    line = own[b * PER_BLOCK + 27 + p // 8, pl.ds(p % 8 * 4 + v, 1), :]
                    out[b * PER_BLOCK + p, pl.ds(8 * v, 8), :] = grow_row(line, index)
            for m in range(9):
                put(out, (b * PER_BLOCK + 27 + m,), [jnp.zeros((CHUNK, LANES), F32)] * 4)

    pack_faces(out, up, down)


def depth_of():
    return iota(CHUNK, 1) % 16


def second_plane_kernel(
    info_in, levels_in, near_in, diffusivity_in, stoichiometry_in, own, other, own_before, other_before, tables,
    dest, sides_out, parts,
    mid, faces, old, edge_x, edge_y, needed, picked_x, picked_y, spread,
    info, levels, near, diffusivity, stoichiometry, sems,
):
    ready = fetch(
        (info_in, levels_in, near_in, diffusivity_in, stoichiometry_in), (info, levels, near, diffusivity, stoichiometry), sems
    )
    gather_species((own, other), old)
    sections_xy((own, other), faces, mid, dest, info, levels, near, ready)
    species_begin(old, parts, info, levels, near, diffusivity, stoichiometry)
    core = info[1]
    fine_of = fine_in(info, levels)
    for b in range(8):
        needed[b] = 0
    for s in range(4):
        for q in range(4):

            @pl.when(jnp.logical_not(fine_of(s)))
            def _(s=s, q=q):
                needed[spot(near[s, q], core)] = 1

    group, odd = iota(CHUNK, 1) // 16, iota(CHUNK, 0) % 2 == 1
    for half, (one, two) in enumerate(((own_before, own), (other_before, other))):

        @pl.loop(0, 4)
        def _(i):
            b = half * 4 + i

            def total(p, at):
                return one[i * PER_BLOCK + p, at, :] + two[i * PER_BLOCK + p, at, :]

            @pl.when(jnp.logical_and(fine_of(b), needed[b] == 1))
            def _():
                for side in range(2):
                    at = pl.ds(30, 2) if side == 0 else pl.ds(0, 2)
                    for e in range(9):
                        edge_x[b, side, pl.ds(2 * e, 2), :] = total(18 + e if side == 0 else e, at)
                    edge_x[b, side, pl.ds(18, 14), :] = jnp.zeros((14, LANES), F32)
                for v in range(4):
                    at = pl.ds(8 * v, 8)
                    packs = [None, None]
                    for e in range(9):
                        p_low = 9 * (e // 3) + e % 3
                        slot = e % 8
                        high = roll_lanes(total(p_low + 6, at), 16 * (slot - 7))
                        both = jnp.where(odd, high, roll_lanes(total(p_low, at), 16 * slot))
                        held_pack = packs[e // 8]
                        packs[e // 8] = both if held_pack is None else jnp.where(group == slot, both, held_pack)
                    for a in range(2):
                        edge_y[b, a, at, :] = packs[a]

    row, col = wide_iota(0), wide_iota(1)
    e_of, cell = col // 64, col % 64
    keep_x = jnp.logical_and(row // 2 == e_of, row % 2 == cell // 32)
    keep_y = row // 4 == cell // 8
    odd_row = row % 2 == 1
    any_coarse = jnp.logical_not(jnp.logical_and(jnp.logical_and(fine_of(0), fine_of(1)), jnp.logical_and(fine_of(2), fine_of(3))))
    sides_out[...] = jnp.zeros((4, 2304), F32)

    @pl.when(any_coarse)
    def _():
        for q in range(4):
            for s in range(4):
                live = jnp.logical_and(jnp.logical_not(fine_of(s)), levels[near[s, q]] == 1)
                m = spot(near[s, q], core)
                rows = pl.ds((q % 2 * 4 + s) * ROWS, ROWS)
                if q < 2:
                    picked_x[rows, :] = jnp.where(live, 0.125 * edge_x[m, q], 0.0)
                else:
                    for a in range(2):
                        picked_y[rows, pl.ds(a * LANES, LANES)] = jnp.where(live, 0.125 * edge_y[m, a], 0.0)
        for pair, picked, weights in ((0, picked_x, tables[0:128, :]), (1, picked_y, tables[128:384, :])):
            spread[...] = times(picked[...], weights)
            for s in range(4):
                keeps = (keep_x, keep_x)
                if pair:
                    keeps = (jnp.logical_and(keep_y, odd_row), jnp.logical_and(keep_y, jnp.logical_not(odd_row)))
                put_pair(
                    sides_out, s, pair * 1152,
                    column_sums(spread, s, keeps[0]), column_sums(spread, 4 + s, keeps[1]),
                )


def end_kernel(
    info_in, levels_in, near_in, far_in, diffusivity_in, held, own, parts,
    up_own, up_other, down_own, down_other, up_own_before, up_other_before, down_own_before, down_other_before,
    sides, weights, pop, scal,
    pop_out, scal_out, returned_out,
    raw, mid, done, rest, before, pops, scals, returned, flux, picked, spread,
    info, levels, near, far, diffusivity, sems,
):
    ready = fetch(
        (info_in, levels_in, near_in, far_in, diffusivity_in), (info, levels, near, far, diffusivity), sems, 6
    )
    incoming = ((up_own, up_other), (down_own, down_other))
    for way in range(2):
        for half in range(2):
            put(rest, (way, half), chunks(incoming[way][half], 4))
    settle(((up_own_before, up_other_before), (down_own_before, down_other_before)), before)
    settle(incoming, raw)
    ready()
    core = info[1]
    fine_of = fine_in(info, levels)
    arrive(info, levels, far, core, raw, mid, done)
    depth = iota(CHUNK, 1) % 16
    row, col = wide_iota(0), wide_iota(1)
    keep = row // 4 * 2 + row % 2 == col % 64 // 4
    copies = []
    for v in range(4):
        at = pl.ds(8 * v, 8)

        @pl.loop(0, 4)
        def _(s):
            rows = pl.ds(32 * v + s, 8, stride=4)

            @pl.when(fine_of(s))
            def _():
                below, above = spot(near[s, 4], core), spot(near[s, 5], core)
                g = z_section(lambda p: held[s, p, at, :], done[0, below, at, :], done[1, above, at, :], depth)
                for p in range(27):
                    pops[p, rows, :] = g[p]
                m = forward_moments(g)
                for d, i in enumerate((9, 3, 1)):
                    flux[s, d, at, :] = m[i] * (0.5 / 216.0)

            @pl.when(jnp.logical_not(fine_of(s)))
            def _():
                for p in range(27):
                    pops[p, rows, :] = pop[p, rows, :]

        rows = pl.ds(32 * v, 32)
        copies.append(pltpu.make_async_copy(pops.at[:, rows, :], pop_out.at[:, rows, :], sems.at[v]))
        copies[-1].start()

    returned[:, 0:2304] = sides[...]
    returned[:, 2304:3456] = jnp.zeros((4, 1152), F32)
    any_coarse = jnp.logical_not(jnp.logical_and(jnp.logical_and(fine_of(0), fine_of(1)), jnp.logical_and(fine_of(2), fine_of(3))))

    @pl.when(any_coarse)
    def _():
        for way in range(2):
            for s in range(4):
                m = spot(near[s, 4 + way], core)
                live = jnp.logical_and(jnp.logical_not(fine_of(s)), levels[near[s, 4 + way]] == 1)
                face = jnp.where(live, 0.125 * (before[way, m] + raw[way, m]), 0.0)
                picked[pl.ds((way * 4 + s) * ROWS, ROWS), :] = face
        spread[...] = times(picked[...], weights[...])
        for s in range(4):
            put_pair(returned, s, 2304, column_sums(spread, s, keep), column_sums(spread, 4 + s, keep))

    copies.append(pltpu.make_async_copy(returned, returned_out, sems.at[5]))
    copies[-1].start()

    @pl.loop(0, 4)
    def _(s):
        @pl.when(fine_of(s))
        def _():
            def store(m, v, value):
                scals[m, pl.ds(32 * v + s, 8, stride=4), :] = value

            species_end(
                parts, s, lambda m, at: own[s * PER_BLOCK + 27 + m, at, :],
                face_reader(done, rest, spot(near[s, 4], core), spot(near[s, 5], core)), flux.at[s],
                [levels[near[s, q]] for q in (4, 5)], diffusivity, store,
            )

        @pl.when(jnp.logical_not(fine_of(s)))
        def _():
            for v in range(4):
                at = pl.ds(32 * v + s, 8, stride=4)
                for m in range(9):
                    scals[m, at, :] = scal[m, at, :]

    copies.append(pltpu.make_async_copy(scals, scal_out, sems.at[4]))
    copies[-1].start()
    for copy in copies:
        copy.wait()


def specs(kinds):
    table = {
        "s": pl.BlockSpec(memory_space=pltpu.SMEM),
        "v": pl.BlockSpec(memory_space=pltpu.VMEM),
        "h": pl.BlockSpec(memory_space=pltpu.HBM),
        "a": pl.BlockSpec(memory_space=pl.ANY),
    }
    return [table[kind] for kind in kinds]


def call(kernel, kinds, outs, out_kinds, scratch, name, megabytes, flops):
    return pl.pallas_call(
        kernel,
        in_specs=specs(kinds),
        out_specs=specs(out_kinds),
        out_shape=outs,
        scratch_shapes=scratch,
        name=name,
        compiler_params=pltpu.CompilerParams(vmem_limit_bytes=megabytes << 20),
        cost_estimate=pl.CostEstimate(flops=flops, transcendentals=0, bytes_accessed=8 << 20),
    )


def interleave(x):
    blocks, n, cells = x.shape
    x = x.reshape(blocks, n, cells // LANES, LANES)
    return jnp.transpose(x, (1, 2, 0, 3)).reshape(n, cells // LANES * blocks, LANES)


def separate(x):
    n, rows, _ = x.shape
    x = jnp.transpose(x.reshape(n, rows // 4, 4, LANES), (2, 0, 1, 3))
    return x.reshape(4, n, rows // 4 * LANES)


def local(
    populations, scalars, coarse_old, coarse_new, levels, neighbours, relax_rates, diffusivity, stoichiometry
):
    devices = lax.axis_size("blk")
    me = lax.axis_index("blk")
    layer, layers = me // 2, devices // 2
    info = jnp.stack([layer, me % 2, (layer + layers - 1) % layers, (layer + 1) % layers]).astype(jnp.int32)
    swap = [(i, i ^ 1) for i in range(devices)]
    rise = [(i, (i + 2) % devices) for i in range(devices)]
    fall = [(i, (i - 2) % devices) for i in range(devices)]

    def move(x, pairs):
        return lax.ppermute(x, "blk", pairs)

    def vmem(*lead):
        return pltpu.VMEM((*lead, ROWS, LANES), F32)

    full = (ROWS, LANES)
    pop, scal = interleave(populations), interleave(scalars)
    old, new = interleave(coarse_old), interleave(coarse_new)
    side_table, z_table = reduce_tables()
    fields = FIELDS - 1
    semaphores = pltpu.SemaphoreType.DMA
    own, up, down = call(
        begin_kernel,
        "ahhhhhhh",
        [shape_of(FIELDS, *full), shape_of(5, *full), shape_of(5, *full)],
        "vvv",
        [pltpu.VMEM(x.shape, F32) for x in (pop, scal, old, new)]
        + [pltpu.SMEM(x.shape, x.dtype) for x in (info, levels, neighbours, relax_rates)]
        + [semaphores((11,))],
        "begin",
        12,
        1 << 27,
    )(info, *[pltpu.with_memory_space_constraint(x, pltpu.HBM) for x in (levels, neighbours, relax_rates, pop, scal, old, new)])
    other = move(own, swap)
    up, down = move(up, rise), move(down, fall)
    face = pltpu.VMEM((8, 27, CHUNK, LANES), F32)
    table_shape = jax.ShapeDtypeStruct((CHUNK, LANES), jnp.int32)

    def smem(*arrays):
        return [pltpu.SMEM(x.shape, x.dtype) for x in arrays]

    held, near, parts = call(
        plane_kernel,
        "aaaavv",
        [shape_of(4, 27, *full), table_shape, shape_of(4 * PER_BLOCK, *full)],
        "vvv",
        [vmem(8, 27), face, vmem(8, 9)]
        + smem(info, levels, table_shape, diffusivity, stoichiometry) + [semaphores((5,))],
        "plane",
        12,
        1 << 27,
    )(info, levels, diffusivity, stoichiometry, own, other)
    held, up, down = lax.optimization_barrier((held, up, down))
    arrived = (up, move(up, swap), down, move(down, swap))
    landing = [vmem(2, 8), vmem(2, 8), vmem(2, 8), vmem(2, 2)]
    own_next, up_next, down_next, table = call(
        middle_kernel,
        "aaaaavvvvvvv",
        [shape_of(fields, *full), shape_of(5, *full), shape_of(5, *full), table_shape],
        "vvvv",
        landing
        + [vmem(3)]
        + smem(info, levels, table_shape, relax_rates, diffusivity, table_shape)
        + [semaphores((6,))],
        "middle",
        14,
        1 << 28,
    )(
        info, levels, near, relax_rates, diffusivity, own, held, parts, *arrived
    )
    other_next = move(own_next, swap)
    up, down = move(up_next, rise), move(down_next, fall)
    held, sides, parts = call(
        second_plane_kernel,
        "aaaaavvvvv",
        [shape_of(4, 27, *full), shape_of(4, 2304), shape_of(4 * PER_BLOCK, *full)],
        "vvv",
        [vmem(8, 27), face, vmem(8, 9), vmem(8, 2), vmem(8, 2), pltpu.SMEM((8,), jnp.int32)]
        + [pltpu.VMEM((8 * ROWS, LANES), F32), pltpu.VMEM((8 * ROWS, 2 * LANES), F32), pltpu.VMEM((8 * ROWS, WIDE), F32)]
        + smem(info, levels, table_shape, diffusivity, stoichiometry) + [semaphores((5,))],
        "plane2",
        14,
        1 << 27,
    )(info, levels, near, diffusivity, stoichiometry, own_next, other_next, own, other, side_table)
    held, sides, up, down = lax.optimization_barrier((held, sides, up, down))
    pop_out, scal_out, returned = call(
        end_kernel,
        "aaaaa" + "v" * 15,
        [shape_of(27, 128, LANES), shape_of(9, 128, LANES), shape_of(4, 3456)],
        "hhh",
        landing
        + [vmem(2, 8), pltpu.VMEM(pop.shape, F32), pltpu.VMEM(scal.shape, F32)]
        + [pltpu.VMEM((4, 3456), F32), vmem(4, 3)]
        + [pltpu.VMEM((8 * ROWS, LANES), F32), pltpu.VMEM((8 * ROWS, WIDE), F32)]
        + smem(info, levels, table_shape, table_shape, diffusivity) + [semaphores((11,))],
        "end",
        16,
        1 << 27,
    )(
        info, levels, near, table, diffusivity, held, own_next, parts,
        up, move(up, swap), down, move(down, swap), *arrived, sides, z_table, pop, scal,
    )
    return separate(pop_out), separate(scal_out), returned


def solution(mesh):
    in_specs = (
        P("blk", None, None), P("blk", None, None), P("blk", None, None), P("blk", None, None),
        P(), P("blk", None), P(), P(), P(),
    )
    out_specs = (P("blk", None, None), P("blk", None, None), P("blk", None))
    return jax.shard_map(local, mesh=mesh, in_specs=in_specs, out_specs=out_specs, check_vma=False)
```

```python
import jax
import jax.numpy as jnp
import numpy as np
from jax import lax
from jax.experimental import pallas as pl
from jax.experimental.pallas import tpu as pltpu
from jax.sharding import PartitionSpec as P

F32 = jnp.float32
VEL = [(a, b, c) for a in (-1, 0, 1) for b in (-1, 0, 1) for c in (-1, 0, 1)]
ROWS, LANES = 32, 128
CHUNK = 8


def shape_of(*dims):
    return jax.ShapeDtypeStruct(dims, F32)


def iota(rows, axis):
    return lax.broadcasted_iota(jnp.int32, (rows, LANES), axis)


def chunk_at(v):
    return pl.ds(pl.multiple_of(v * CHUNK, CHUNK), CHUNK)


def roll_lanes(x, by):
    if isinstance(by, int):
        by = by % LANES
        if by == 0:
            return x
    return pltpu.roll(x, by, 1)


def forward_moments(values):
    out = list(values)
    for stride in (9, 3, 1):
        for i in range(27):
            if (i // stride) % 3 == 0:
                low, mid, high = out[i], out[i + stride], out[i + 2 * stride]
                both = low + high
                out[i] = both + 4.0 * mid
                out[i + stride] = high - low
                out[i + 2 * stride] = both
    return out


def plus(x, y):
    if x is None:
        return y
    return x if y is None else x + y


def minus(x, y):
    if y is None:
        return x
    return -y if x is None else x - y


def backward_moments(values):
    out = list(values)
    for stride in (9, 3, 1):
        for i in range(27):
            if (i // stride) % 3 == 0:
                m0, m1, m2 = out[i], out[i + stride], out[i + 2 * stride]
                out[i] = minus(m2, m1)
                out[i + stride] = minus(m0, m2)
                out[i + 2 * stride] = plus(m1, m2)
    return out


def collide(g, rate):
    m = forward_moments(g)
    rho = m[0]
    j = (m[9], m[3], m[1])
    square = [x * x * (1.0 / 72.0) for x in j]
    relaxed = [None] * 27
    for k in range(27):
        digits = (k // 9, (k // 3) % 3, k % 3)
        odd = [d for d in range(3) if digits[d] == 1]
        twos = [d for d in range(3) if digits[d] == 2]
        if k in (0, 9, 3, 1):
            continue
        if not odd:
            level = rho
            for d in twos:
                level = level + square[d]
        elif len(odd) == 1:
            level = j[odd[0]]
        elif len(odd) == 2:
            level = j[odd[0]] * j[odd[1]] * (1.0 / 216.0)
        else:
            level = None
        if level is not None and twos:
            level = level * (3.0 ** -len(twos))
        relaxed[k] = minus(m[k], level) * (rate(k) * (1.0 / 64.0))
    back = backward_moments(relaxed)
    post = []
    for i, c in enumerate(VEL):
        factor = 2.0 ** sum(abs(x) for x in c)
        post.append(g[i] - (back[i] if factor == 1.0 else factor * back[i]))
    return post, j


def grow_index():
    r, l = iota(CHUNK, 0), iota(CHUNK, 1)
    return (r // 4) % 2 * 64 + r % 2 * 32 + l // 32 * 8 + l % 16 // 2


def grow_row(row, index):
    return jnp.take_along_axis(jnp.broadcast_to(row, (CHUNK, LANES)), index, axis=1)


PER_BLOCK = 36
FIELDS = 4 * PER_BLOCK + 1


def fetch(sources, targets, sems, first=0):
    copies = [pltpu.make_async_copy(a, b, sems.at[first + i]) for i, (a, b) in enumerate(zip(sources, targets))]
    for copy in copies:
        copy.start()

    def ready():
        for copy in copies:
            copy.wait()

    return ready


def begin_kernel(
    info_in, levels_in, near_in, rates_in, pop, scal, old, new, out, up, down,
    pops, scals, olds, news, info, levels, near, rates, sems,
):
    ready = fetch((info_in, levels_in, near_in, rates_in), (info, levels, near, rates), sems, 7)
    copies = []
    for v in range(4):
        rows = pl.ds(32 * v, 32)
        copies.append(pltpu.make_async_copy(pop.at[:, rows, :], pops.at[:, rows, :], sems.at[v]))
    copies.append(pltpu.make_async_copy(old, olds, sems.at[4]))
    copies.append(pltpu.make_async_copy(new, news, sems.at[5]))
    copies.append(pltpu.make_async_copy(scal, scals, sems.at[6]))
    for copy in copies:
        copy.start()
    index = grow_index()
    ready()
    layer, core = info[0], info[1]
    row, lane = iota(CHUNK, 0), iota(CHUNK, 1)
    meta = jnp.zeros((CHUNK, LANES), F32)
    for b in range(4):
        for q in range(6):
            here = jnp.logical_and(row == b, lane == q + 8)
            meta = jnp.where(here, near[b, q].astype(F32), meta)
    out[FIELDS - 1, 0:8, :] = meta

    def fine_of(b):
        return levels[layer * 8 + core * 4 + b] == 1

    for v in range(4):
        copies[v].wait()

        @pl.loop(0, 4)
        def _(b):
            @pl.when(fine_of(b))
            def _():
                at = pl.ds(8 * v, 8)
                from_rows = pl.ds(32 * v + b, 8, stride=4)
                post, _j = collide([pops[p, from_rows, :] for p in range(27)], lambda k: rates[k])
                for p in range(27):
                    out[b * PER_BLOCK + p, at, :] = post[p]

    for copy in copies[4:]:
        copy.wait()

    @pl.loop(0, 4)
    def _(b):
        @pl.when(fine_of(b))
        def _():
            for m in range(9):
                for v in range(4):
                    out[b * PER_BLOCK + 27 + m, pl.ds(8 * v, 8), :] = scals[m, pl.ds(32 * v + b, 8, stride=4), :]

        @pl.when(jnp.logical_not(fine_of(b)))
        def _():
            for p in range(27):
                for v in range(4):
                    before = olds[p, pl.ds(4 * v + b, 1), :]
                    after = news[p, pl.ds(4 * v + b, 1), :]
                    out[b * PER_BLOCK + 27 + p // 8, pl.ds(p % 8 * 4 + v, 1), :] = 0.5 * (before + after)
                    out[b * PER_BLOCK + p, pl.ds(8 * v, 8), :] = grow_row(before, index)


    pack_faces(out, up, down, meta)


def pack_faces(out, up, down, meta=None):
    lane = iota(CHUNK, 1) % 16

    @pl.loop(0, 4)
    def _(v):
        at = chunk_at(v)
        for ref, digit, start in ((up, 2, 15), (down, 0, 0)):
            for b in range(4):
                fields = [out[b * PER_BLOCK + 3 * e + digit, at, :] for e in range(9)]
                fields += [out[b * PER_BLOCK + 27 + e, at, :] for e in range(7)]
                ref[b, at, :] = pack_into(fields, 0, start, lane)
            rest = pack_into([out[b * PER_BLOCK + 34 + e, at, :] for b in range(4) for e in range(2)], 0, start, lane)
            ref[4, at, :] = rest if meta is None else jnp.where(lane < 8, rest, meta)


def spot(block, core):
    return (block % 8) ^ (core * 4)


def y_up(own, beside, even, group):
    turned = jnp.where(even, pltpu.roll(beside, CHUNK - 1, 0), pltpu.roll(own, 1, 0))
    return roll_lanes(jnp.where(group < 7, own, turned), 16)


def y_down(own, beside, even, group):
    turned = jnp.where(even, pltpu.roll(own, CHUNK - 1, 0), pltpu.roll(beside, 1, 0))
    return roll_lanes(jnp.where(group > 0, own, turned), -16)


def chunks(ref, *lead):
    return [ref[(*lead, pl.ds(8 * v, 8), slice(None))] for v in range(4)]


def x_up(own, beyond, row):
    turned = [pltpu.roll(x, 2, 0) for x in own]
    before = [beyond] + turned[:3]
    return [jnp.where(row < 2, a, b) for a, b in zip(before, turned)]


def x_down(own, beyond, row):
    turned = [pltpu.roll(x, CHUNK - 2, 0) for x in own]
    after = turned[1:] + [beyond]
    return [jnp.where(row >= 6, a, b) for a, b in zip(after, turned)]


def put(ref, lead, values):
    for v in range(4):
        ref[(*lead, pl.ds(8 * v, 8), slice(None))] = values[v]


def sections_xy(refs, faces, mid, dest, info, levels, near, ready):
    row = iota(CHUNK, 0)
    even = row % 2 == 0
    group = iota(CHUNK, 1) // 16

    for half, ref in enumerate(refs):

        @pl.loop(0, 4)
        def _(i):
            for p, c in enumerate(VEL):
                if c[0] == 1:
                    faces[half * 4 + i, p] = pltpu.roll(ref[i * PER_BLOCK + p, pl.ds(24, 8), :], 2, 0)
                elif c[0] == -1:
                    faces[half * 4 + i, p] = pltpu.roll(ref[i * PER_BLOCK + p, pl.ds(0, 8), :], CHUNK - 2, 0)

    ready()
    core = info[1]
    fine_of = fine_in(info, levels)

    for half, ref in enumerate(refs):

        @pl.loop(0, 4)
        def _(i):
            b = half * 4 + i
            fine = fine_of(b)
            fields = [p for p in range(27) if half == 0 or VEL[p][1] != 0]

            @pl.when(fine)
            def _():
                low, high = spot(near[b, 0], core), spot(near[b, 1], core)
                for p in fields:
                    values = chunks(ref, i * PER_BLOCK + p)
                    if VEL[p][0] == 1:
                        values = x_up(values, faces[low, p], row)
                    elif VEL[p][0] == -1:
                        values = x_down(values, faces[high, p], row)
                    put(mid, (b, p), values)

            @pl.when(jnp.logical_not(fine))
            def _():
                for p in fields:
                    if VEL[p][1] != 0:
                        put(mid, (b, p), chunks(ref, i * PER_BLOCK + p))

    @pl.loop(0, 4)
    def _(b):
        @pl.when(fine_of(b))
        def _():
            low, high = spot(near[b, 2], core), spot(near[b, 3], core)
            for p, c in enumerate(VEL):
                for v in range(4):
                    at = pl.ds(8 * v, 8)
                    value = mid[b, p, at, :]
                    if c[1] == 1:
                        value = y_up(value, mid[low, p, at, :], even, group)
                    elif c[1] == -1:
                        value = y_down(value, mid[high, p, at, :], even, group)
                    dest[b, p, at, :] = value


def pack_into(fields, first_slot, start, lane):
    parts = [(first_slot + e, roll_lanes(field, first_slot + e - start)) for e, field in enumerate(fields)]
    while len(parts) > 1:
        joined = []
        for k in range(0, len(parts) - 1, 2):
            slot = parts[k + 1][0]
            joined.append((parts[k][0], jnp.where(lane < slot, parts[k][1], parts[k + 1][1])))
        parts = joined + parts[len(parts) - len(parts) % 2:]
    return parts[0][1]


def fine_in(info, levels):
    return lambda b: levels[info[0] * 8 + spot(b, info[1])] == 1


def plane_kernel(
    info_in, levels_in, diffusivity_in, stoichiometry_in, own, other, dest, table, parts,
    mid, faces, old, info, levels, near, diffusivity, stoichiometry, sems,
):
    row = iota(CHUNK, 0)
    both = jnp.where(row < 4, own[FIELDS - 1, 0:8, :], pltpu.roll(other[FIELDS - 1, 0:8, :], 4, 0))
    table[...] = roll_lanes(both, -8).astype(jnp.int32)
    ready = fetch(
        (info_in, levels_in, table, diffusivity_in, stoichiometry_in), (info, levels, near, diffusivity, stoichiometry), sems
    )
    gather_species((own, other), old)
    sections_xy((own, other), faces, mid, dest, info, levels, near, ready)
    species_begin(old, parts, info, levels, near, diffusivity, stoichiometry)


def settle(incoming, raw):
    for way in range(2):
        for half in range(2):
            for i in range(4):
                put(raw, (way, half * 4 + i), chunks(incoming[way][half], i))


def arrive(info, levels, table, core, raw, mid, done):
    row, slot = iota(CHUNK, 0), iota(CHUNK, 1) % 16
    even, group = row % 2 == 0, iota(CHUNK, 1) // 16
    x_plus, x_minus = jnp.logical_and(slot >= 6, slot < 9), slot < 3
    y_plus = jnp.logical_and(slot < 9, slot % 3 == 2)
    y_minus = jnp.logical_and(slot < 9, slot % 3 == 0)
    blocks = [(way, b) for way in range(2) for b in range(8)]
    fine = [levels[info[2 + way] * 8 + spot(b, core)] == 1 for way, b in blocks]

    def beside(way, b, q):
        return spot(table[b, 16 * way + 8 + q], core)

    for (way, b), flag in zip(blocks, fine):
        own = chunks(raw, way, b)
        before = x_up(own, pltpu.roll(raw[way, beside(way, b, 0), pl.ds(24, 8), :], 2, 0), row)
        after = x_down(own, pltpu.roll(raw[way, beside(way, b, 1), pl.ds(0, 8), :], CHUNK - 2, 0), row)
        to_plus, to_minus = jnp.logical_and(x_plus, flag), jnp.logical_and(x_minus, flag)
        put(mid, (way, b), [jnp.where(to_plus, x, jnp.where(to_minus, y, z)) for x, y, z in zip(before, after, own)])
    for (way, b), flag in zip(blocks, fine):
        low, high = beside(way, b, 2), beside(way, b, 3)
        to_plus, to_minus = jnp.logical_and(y_plus, flag), jnp.logical_and(y_minus, flag)
        for v in range(4):
            at = pl.ds(8 * v, 8)
            here = mid[way, b, at, :]
            before = y_up(here, mid[way, low, at, :], even, group)
            after = y_down(here, mid[way, high, at, :], even, group)
            done[way, b, at, :] = jnp.where(to_plus, before, jnp.where(to_minus, after, here))


def face_reader(done, rest, below, above):
    def faces(m, at):
        if m < 7:
            slot = 9 + m
            return roll_lanes(done[0, below, at, :], -slot), roll_lanes(done[1, above, at, :], 15 - slot)
        low = LANES - 2 * (below % 4) - (m - 7)
        high = (LANES + 15 - 2 * (above % 4) - (m - 7)) % LANES
        return pltpu.roll(rest[0, below // 4, at, :], low, 1), pltpu.roll(rest[1, above // 4, at, :], high, 1)

    return faces


def z_section(h, up, down, depth):
    g = []
    for p, c in enumerate(VEL):
        e = p // 3
        value = h(p)
        if c[2] == 1:
            value = jnp.where(depth == 0, roll_lanes(up, -e), roll_lanes(value, 1))
        elif c[2] == -1:
            value = jnp.where(depth == 15, roll_lanes(down, 15 - e), roll_lanes(value, -1))
        g.append(value)
    return g


def gather_species(halves, old):
    for half, ref_in in enumerate(halves):

        @pl.loop(0, 4)
        def _(i):
            for m in range(9):
                put(old, (half * 4 + i, m), chunks(ref_in, i * PER_BLOCK + 27 + m))


def species_begin(y_ref, parts, info, levels, near, diffusivity, stoichiometry):
    row, lanes = iota(CHUNK, 0), iota(CHUNK, 1)
    even = row % 2 == 0
    group, depth = lanes // 16, lanes % 16
    fine_of = fine_in(info, levels)

    @pl.loop(0, 4)
    def _(b):
        @pl.when(fine_of(b))
        def _():
            def gone(edge, q):
                return jnp.logical_and(edge, levels[near[b, q]] != 1)

            lost = [
                gone(row < 2, 0), gone(row >= 6, 1),
                gone(jnp.logical_and(even, group == 0), 2),
                gone(jnp.logical_and(jnp.logical_not(even), group == 7), 3),
            ]
            sides = [spot(near[b, q], info[1]) for q in range(4)]
            burning = [
                x * y * jnp.exp(4.0 * (t - 1.0))
                for x, y, t in zip(chunks(y_ref, b, 0), chunks(y_ref, b, 1), chunks(y_ref, b, 8))
            ]
            for m in range(9):
                y = chunks(y_ref, b, m)
                low_x = pltpu.roll(y_ref[sides[0], m, pl.ds(24, 8), :], 2, 0)
                high_x = pltpu.roll(y_ref[sides[1], m, pl.ds(0, 8), :], CHUNK - 2, 0)
                lower_x, upper_x = x_up(y, low_x, row), x_down(y, high_x, row)
                lower_x[0] = jnp.where(lost[0], y[0], lower_x[0])
                upper_x[3] = jnp.where(lost[1], y[3], upper_x[3])
                for v in range(4):
                    at = pl.ds(8 * v, 8)
                    here = y[v]
                    pairs = [
                        (lower_x[v], upper_x[v]),
                        (
                            jnp.where(lost[2], here, y_up(here, y_ref[sides[2], m, at, :], even, group)),
                            jnp.where(lost[3], here, y_down(here, y_ref[sides[3], m, at, :], even, group)),
                        ),
                        (
                            jnp.where(depth == 0, here, roll_lanes(here, 1)),
                            jnp.where(depth == 15, here, roll_lanes(here, -1)),
                        ),
                    ]
                    spread = None
                    for d, (lower, upper) in enumerate(pairs):
                        parts[b * PER_BLOCK + 9 + 9 * d + m, at, :] = upper - lower
                        both = upper + lower
                        spread = both if spread is None else spread + both
                    parts[b * PER_BLOCK + m, at, :] = (
                        here + diffusivity[m] * (spread - 6.0 * here) + stoichiometry[m] * burning[v]
                    )


def species_end(parts, b, y_of, faces, flux, flags, diffusivity, store):
    depth = iota(CHUNK, 1) % 16
    at_low = jnp.logical_and(depth == 0, flags[0] == 1)
    at_high = jnp.logical_and(depth == 15, flags[1] == 1)
    for v in range(4):
        at = pl.ds(8 * v, 8)
        flow = [flux[d, at, :] for d in range(3)]
        for m in range(9):
            here = y_of(m, at)
            low, high = faces(m, at)
            low = jnp.where(at_low, low - here, 0.0)
            high = jnp.where(at_high, high - here, 0.0)
            base, along_x, along_y, along_z = (parts[b * PER_BLOCK + 9 * kind + m, at, :] for kind in range(4))
            drift = flow[0] * along_x + flow[1] * along_y + flow[2] * (along_z + (high - low))
            store(m, v, base - drift + diffusivity[m] * (low + high))


WIDE = 640


def reduce_tables():
    l = np.arange(LANES)[:, None]
    c = np.arange(WIDE)[None, :]
    e, cell = c // 64, c % 64
    live = c < 576
    along_x = (l // 32 * 8 + l % 16 // 2 == cell % 32) & live
    along_y = [(l // 16 + 8 * a == e) & (l % 16 // 2 == cell % 8) & live for a in range(2)]
    along_z = (l % 16 == e) & (l // 32 == cell % 4) & live
    side = np.concatenate([along_x, along_y[0], along_y[1]], axis=0)
    return jnp.asarray(side, jnp.bfloat16), jnp.asarray(along_z, jnp.bfloat16)


def wide_iota(axis):
    return lax.broadcasted_iota(jnp.int32, (ROWS, WIDE), axis)


def times(x, w):
    total = None
    for _ in range(3):
        part = x.astype(jnp.bfloat16)
        x = x - part.astype(F32)
        product = jnp.dot(part, w, preferred_element_type=F32)
        total = product if total is None else total + product
    return total


def column_sums(spread, k, keep):
    return jnp.sum(jnp.where(keep, spread[pl.ds(k * ROWS, ROWS), :], 0.0), axis=0, keepdims=True)


def put_pair(out, s, base, first, second):
    moved = pltpu.roll(second, 64, 1)
    out[pl.ds(s, 1), pl.ds(base, 512)] = first[:, 0:512]
    out[pl.ds(s, 1), pl.ds(base + 512, 128)] = first[:, 512:640] + moved[:, 0:128]
    out[pl.ds(s, 1), pl.ds(base + 640, 512)] = moved[:, 128:640]


def middle_kernel(
    info_in, levels_in, near_in, rates_in, diffusivity_in, own, held, parts, up_own, up_other, down_own, down_other,
    out, up, down, table,
    raw, mid, done, rest, flux, moved,
    info, levels, near, rates, diffusivity, far, sems,
):
    index = grow_index()
    incoming = ((up_own, up_other), (down_own, down_other))
    row, lane = iota(CHUNK, 0), iota(CHUNK, 1)
    below, above = [
        jnp.where(row < 4, one[4, pl.ds(0, 8), :], pltpu.roll(two[4, pl.ds(0, 8), :], 4, 0)) for one, two in incoming
    ]
    table[...] = jnp.where(lane < 16, below, roll_lanes(above, 16)).astype(jnp.int32)
    ready = fetch(
        (info_in, levels_in, near_in, rates_in, diffusivity_in, table),
        (info, levels, near, rates, diffusivity, far),
        sems,
    )
    settle(incoming, raw)
    for way in range(2):
        for half in range(2):
            put(rest, (way, half), chunks(incoming[way][half], 4))

    ready()
    core = info[1]
    fine_of = fine_in(info, levels)
    arrive(info, levels, far, core, raw, mid, done)

    @pl.loop(0, 4)
    def _(b):
        @pl.when(fine_of(b))
        def _():
            below, above = spot(near[b, 4], core), spot(near[b, 5], core)

            for v in range(4):
                at = pl.ds(8 * v, 8)
                g = z_section(lambda p: held[b, p, at, :], done[0, below, at, :], done[1, above, at, :], depth_of())
                for p in range(27):
                    moved[p, at, :] = g[p]

            @pl.loop(0, 4)
            def _(v):
                at = chunk_at(v)
                post, j = collide([moved[p, at, :] for p in range(27)], lambda k: rates[k])
                for p in range(27):
                    out[b * PER_BLOCK + p, at, :] = post[p]
                for d in range(3):
                    flux[d, at, :] = j[d] * (0.5 / 216.0)

            def store(m, v, value):
                out[b * PER_BLOCK + 27 + m, pl.ds(8 * v, 8), :] = value

            species_end(
                parts, b, lambda m, at: own[b * PER_BLOCK + 27 + m, at, :], face_reader(done, rest, below, above), flux,
                [levels[near[b, q]] for q in (4, 5)], diffusivity, store,
            )

        @pl.when(jnp.logical_not(fine_of(b)))
        def _():
            for p in range(27):
                for v in range(4):
                    line = own[b * PER_BLOCK + 27 + p // 8, pl.ds(p % 8 * 4 + v, 1), :]
                    out[b * PER_BLOCK + p, pl.ds(8 * v, 8), :] = grow_row(line, index)
            for m in range(9):
                put(out, (b * PER_BLOCK + 27 + m,), [jnp.zeros((CHUNK, LANES), F32)] * 4)

    pack_faces(out, up, down)


def depth_of():
    return iota(CHUNK, 1) % 16


def second_plane_kernel(
    info_in, levels_in, near_in, diffusivity_in, stoichiometry_in, own, other, own_before, other_before, tables,
    dest, sides_out, parts,
    mid, faces, old, edge_x, edge_y, needed, picked_x, picked_y, spread,
    info, levels, near, diffusivity, stoichiometry, sems,
):
    ready = fetch(
        (info_in, levels_in, near_in, diffusivity_in, stoichiometry_in), (info, levels, near, diffusivity, stoichiometry), sems
    )
    gather_species((own, other), old)
    sections_xy((own, other), faces, mid, dest, info, levels, near, ready)
    species_begin(old, parts, info, levels, near, diffusivity, stoichiometry)
    core = info[1]
    fine_of = fine_in(info, levels)
    for b in range(8):
        needed[b] = 0
    for s in range(4):
        for q in range(4):

            @pl.when(jnp.logical_not(fine_of(s)))
            def _(s=s, q=q):
                needed[spot(near[s, q], core)] = 1

    group, odd = iota(CHUNK, 1) // 16, iota(CHUNK, 0) % 2 == 1
    for half, (one, two) in enumerate(((own_before, own), (other_before, other))):

        @pl.loop(0, 4)
        def _(i):
            b = half * 4 + i

            def total(p, at):
                return one[i * PER_BLOCK + p, at, :] + two[i * PER_BLOCK + p, at, :]

            @pl.when(jnp.logical_and(fine_of(b), needed[b] == 1))
            def _():
                for side in range(2):
                    at = pl.ds(30, 2) if side == 0 else pl.ds(0, 2)
                    for e in range(9):
                        edge_x[b, side, pl.ds(2 * e, 2), :] = total(18 + e if side == 0 else e, at)
                    edge_x[b, side, pl.ds(18, 14), :] = jnp.zeros((14, LANES), F32)
                for v in range(4):
                    at = pl.ds(8 * v, 8)
                    packs = [None, None]
                    for e in range(9):
                        p_low = 9 * (e // 3) + e % 3
                        slot = e % 8
                        high = roll_lanes(total(p_low + 6, at), 16 * (slot - 7))
                        both = jnp.where(odd, high, roll_lanes(total(p_low, at), 16 * slot))
                        held_pack = packs[e // 8]
                        packs[e // 8] = both if held_pack is None else jnp.where(group == slot, both, held_pack)
                    for a in range(2):
                        edge_y[b, a, at, :] = packs[a]

    row, col = wide_iota(0), wide_iota(1)
    e_of, cell = col // 64, col % 64
    keep_x = jnp.logical_and(row // 2 == e_of, row % 2 == cell // 32)
    keep_y = row // 4 == cell // 8
    odd_row = row % 2 == 1
    any_coarse = jnp.logical_not(jnp.logical_and(jnp.logical_and(fine_of(0), fine_of(1)), jnp.logical_and(fine_of(2), fine_of(3))))
    sides_out[...] = jnp.zeros((4, 2304), F32)

    @pl.when(any_coarse)
    def _():
        for q in range(4):
            for s in range(4):
                live = jnp.logical_and(jnp.logical_not(fine_of(s)), levels[near[s, q]] == 1)
                m = spot(near[s, q], core)
                rows = pl.ds((q % 2 * 4 + s) * ROWS, ROWS)
                if q < 2:
                    picked_x[rows, :] = jnp.where(live, 0.125 * edge_x[m, q], 0.0)
                else:
                    for a in range(2):
                        picked_y[rows, pl.ds(a * LANES, LANES)] = jnp.where(live, 0.125 * edge_y[m, a], 0.0)
        for pair, picked, weights in ((0, picked_x, tables[0:128, :]), (1, picked_y, tables[128:384, :])):
            spread[...] = times(picked[...], weights)
            for s in range(4):
                keeps = (keep_x, keep_x)
                if pair:
                    keeps = (jnp.logical_and(keep_y, odd_row), jnp.logical_and(keep_y, jnp.logical_not(odd_row)))
                put_pair(
                    sides_out, s, pair * 1152,
                    column_sums(spread, s, keeps[0]), column_sums(spread, 4 + s, keeps[1]),
                )


def end_kernel(
    info_in, levels_in, near_in, far_in, diffusivity_in, held, own, parts,
    up_own, up_other, down_own, down_other, up_own_before, up_other_before, down_own_before, down_other_before,
    sides, weights, pop, scal,
    pop_out, scal_out, returned_out,
    raw, mid, done, rest, before, pops, scals, returned, flux, picked, spread,
    info, levels, near, far, diffusivity, sems,
):
    ready = fetch(
        (info_in, levels_in, near_in, far_in, diffusivity_in), (info, levels, near, far, diffusivity), sems, 6
    )
    incoming = ((up_own, up_other), (down_own, down_other))
    for way in range(2):
        for half in range(2):
            put(rest, (way, half), chunks(incoming[way][half], 4))
    settle(((up_own_before, up_other_before), (down_own_before, down_other_before)), before)
    settle(incoming, raw)
    ready()
    core = info[1]
    fine_of = fine_in(info, levels)
    arrive(info, levels, far, core, raw, mid, done)
    depth = iota(CHUNK, 1) % 16
    row, col = wide_iota(0), wide_iota(1)
    keep = row // 4 * 2 + row % 2 == col % 64 // 4
    @pl.loop(0, 4)
    def _(s):
        below, above = spot(near[s, 4], core), spot(near[s, 5], core)

        @pl.when(fine_of(s))
        def _():
            for v in range(4):
                at = pl.ds(8 * v, 8)
                g = z_section(lambda p: held[s, p, at, :], done[0, below, at, :], done[1, above, at, :], depth)
                for p in range(27):
                    pops[p, pl.ds(32 * v + s, 8, stride=4), :] = g[p]
                m = forward_moments(g)
                for d, i in enumerate((9, 3, 1)):
                    flux[s, d, at, :] = m[i] * (0.5 / 216.0)

        @pl.when(jnp.logical_not(fine_of(s)))
        def _():
            for v in range(4):
                rows = pl.ds(32 * v + s, 8, stride=4)
                for p in range(27):
                    pops[p, rows, :] = pop[p, rows, :]

    copies = [pltpu.make_async_copy(pops, pop_out, sems.at[0])]
    copies[-1].start()

    @pl.loop(0, 4)
    def _(s):
        @pl.when(fine_of(s))
        def _():
            def store(m, v, value):
                scals[m, pl.ds(32 * v + s, 8, stride=4), :] = value

            species_end(
                parts, s, lambda m, at: own[s * PER_BLOCK + 27 + m, at, :],
                face_reader(done, rest, spot(near[s, 4], core), spot(near[s, 5], core)), flux.at[s],
                [levels[near[s, q]] for q in (4, 5)], diffusivity, store,
            )

        @pl.when(jnp.logical_not(fine_of(s)))
        def _():
            for v in range(4):
                at = pl.ds(32 * v + s, 8, stride=4)
                for m in range(9):
                    scals[m, at, :] = scal[m, at, :]

    copies.append(pltpu.make_async_copy(scals, scal_out, sems.at[4]))
    copies[-1].start()

    returned[:, 0:2304] = sides[...]
    returned[:, 2304:3456] = jnp.zeros((4, 1152), F32)
    any_coarse = jnp.logical_not(jnp.logical_and(jnp.logical_and(fine_of(0), fine_of(1)), jnp.logical_and(fine_of(2), fine_of(3))))

    @pl.when(any_coarse)
    def _():
        for way in range(2):
            for s in range(4):
                m = spot(near[s, 4 + way], core)
                live = jnp.logical_and(jnp.logical_not(fine_of(s)), levels[near[s, 4 + way]] == 1)
                face = jnp.where(live, 0.125 * (before[way, m] + raw[way, m]), 0.0)
                picked[pl.ds((way * 4 + s) * ROWS, ROWS), :] = face
        spread[...] = times(picked[...], weights[...])
        for s in range(4):
            put_pair(returned, s, 2304, column_sums(spread, s, keep), column_sums(spread, 4 + s, keep))

    copies.append(pltpu.make_async_copy(returned, returned_out, sems.at[5]))
    copies[-1].start()

    for copy in copies:
        copy.wait()


def specs(kinds):
    table = {
        "s": pl.BlockSpec(memory_space=pltpu.SMEM),
        "v": pl.BlockSpec(memory_space=pltpu.VMEM),
        "h": pl.BlockSpec(memory_space=pltpu.HBM),
        "a": pl.BlockSpec(memory_space=pl.ANY),
    }
    return [table[kind] for kind in kinds]


def call(kernel, kinds, outs, out_kinds, scratch, name, megabytes, flops):
    return pl.pallas_call(
        kernel,
        in_specs=specs(kinds),
        out_specs=specs(out_kinds),
        out_shape=outs,
        scratch_shapes=scratch,
        name=name,
        compiler_params=pltpu.CompilerParams(vmem_limit_bytes=megabytes << 20),
        cost_estimate=pl.CostEstimate(flops=flops, transcendentals=0, bytes_accessed=8 << 20),
    )


def interleave(x):
    blocks, n, cells = x.shape
    x = x.reshape(blocks, n, cells // LANES, LANES)
    return jnp.transpose(x, (1, 2, 0, 3)).reshape(n, cells // LANES * blocks, LANES)


def separate(x):
    n, rows, _ = x.shape
    x = jnp.transpose(x.reshape(n, rows // 4, 4, LANES), (2, 0, 1, 3))
    return x.reshape(4, n, rows // 4 * LANES)


def local(
    populations, scalars, coarse_old, coarse_new, levels, neighbours, relax_rates, diffusivity, stoichiometry
):
    devices = lax.axis_size("blk")
    me = lax.axis_index("blk")
    layer, layers = me // 2, devices // 2
    info = jnp.stack([layer, me % 2, (layer + layers - 1) % layers, (layer + 1) % layers]).astype(jnp.int32)
    swap = [(i, i ^ 1) for i in range(devices)]
    rise = [(i, (i + 2) % devices) for i in range(devices)]
    fall = [(i, (i - 2) % devices) for i in range(devices)]

    def move(x, pairs):
        return lax.ppermute(x, "blk", pairs)

    def vmem(*lead):
        return pltpu.VMEM((*lead, ROWS, LANES), F32)

    full = (ROWS, LANES)
    pop, scal = interleave(populations), interleave(scalars)
    old, new = interleave(coarse_old), interleave(coarse_new)
    side_table, z_table = reduce_tables()
    fields = FIELDS - 1
    semaphores = pltpu.SemaphoreType.DMA
    own, up, down = call(
        begin_kernel,
        "ahhhhhhh",
        [shape_of(FIELDS, *full), shape_of(5, *full), shape_of(5, *full)],
        "vvv",
        [pltpu.VMEM(x.shape, F32) for x in (pop, scal, old, new)]
        + [pltpu.SMEM(x.shape, x.dtype) for x in (info, levels, neighbours, relax_rates)]
        + [semaphores((11,))],
        "begin",
        12,
        1 << 27,
    )(info, *[pltpu.with_memory_space_constraint(x, pltpu.HBM) for x in (levels, neighbours, relax_rates, pop, scal, old, new)])
    other = move(own, swap)
    up, down = move(up, rise), move(down, fall)
    face = pltpu.VMEM((8, 27, CHUNK, LANES), F32)
    table_shape = jax.ShapeDtypeStruct((CHUNK, LANES), jnp.int32)

    def smem(*arrays):
        return [pltpu.SMEM(x.shape, x.dtype) for x in arrays]

    held, near, parts = call(
        plane_kernel,
        "aaaavv",
        [shape_of(4, 27, *full), table_shape, shape_of(4 * PER_BLOCK, *full)],
        "vvv",
        [vmem(8, 27), face, vmem(8, 9)]
        + smem(info, levels, table_shape, diffusivity, stoichiometry) + [semaphores((5,))],
        "plane",
        12,
        1 << 27,
    )(info, levels, diffusivity, stoichiometry, own, other)
    held, up, down = lax.optimization_barrier((held, up, down))
    arrived = (up, move(up, swap), down, move(down, swap))
    landing = [vmem(2, 8), vmem(2, 8), vmem(2, 8), vmem(2, 2)]
    own_next, up_next, down_next, table = call(
        middle_kernel,
        "aaaaavvvvvvv",
        [shape_of(fields, *full), shape_of(5, *full), shape_of(5, *full), table_shape],
        "vvvv",
        landing
        + [vmem(3), vmem(27)]
        + smem(info, levels, table_shape, relax_rates, diffusivity, table_shape)
        + [semaphores((6,))],
        "middle",
        14,
        1 << 28,
    )(
        info, levels, near, relax_rates, diffusivity, own, held, parts, *arrived
    )
    other_next = move(own_next, swap)
    up, down = move(up_next, rise), move(down_next, fall)
    held, sides, parts = call(
        second_plane_kernel,
        "aaaaavvvvv",
        [shape_of(4, 27, *full), shape_of(4, 2304), shape_of(4 * PER_BLOCK, *full)],
        "vvv",
        [vmem(8, 27), face, vmem(8, 9), vmem(8, 2), vmem(8, 2), pltpu.SMEM((8,), jnp.int32)]
        + [pltpu.VMEM((8 * ROWS, LANES), F32), pltpu.VMEM((8 * ROWS, 2 * LANES), F32), pltpu.VMEM((8 * ROWS, WIDE), F32)]
        + smem(info, levels, table_shape, diffusivity, stoichiometry) + [semaphores((5,))],
        "plane2",
        14,
        1 << 27,
    )(info, levels, near, diffusivity, stoichiometry, own_next, other_next, own, other, side_table)
    held, sides, up, down = lax.optimization_barrier((held, sides, up, down))
    pop_out, scal_out, returned = call(
        end_kernel,
        "aaaaa" + "v" * 15,
        [shape_of(27, 128, LANES), shape_of(9, 128, LANES), shape_of(4, 3456)],
        "hhh",
        landing
        + [vmem(2, 8), pltpu.VMEM(pop.shape, F32), pltpu.VMEM(scal.shape, F32)]
        + [pltpu.VMEM((4, 3456), F32), vmem(4, 3)]
        + [pltpu.VMEM((8 * ROWS, LANES), F32), pltpu.VMEM((8 * ROWS, WIDE), F32)]
        + smem(info, levels, table_shape, table_shape, diffusivity) + [semaphores((11,))],
        "end",
        16,
        1 << 27,
    )(
        info, levels, near, table, diffusivity, held, own_next, parts,
        up, move(up, swap), down, move(down, swap), *arrived, sides, z_table, pop, scal,
    )
    return separate(pop_out), separate(scal_out), returned


def solution(mesh):
    in_specs = (
        P("blk", None, None), P("blk", None, None), P("blk", None, None), P("blk", None, None),
        P(), P("blk", None), P(), P(), P(),
    )
    out_specs = (P("blk", None, None), P("blk", None, None), P("blk", None))
    return jax.shard_map(local, mesh=mesh, in_specs=in_specs, out_specs=out_specs, check_vma=False)
```

```python
import jax
import jax.numpy as jnp
import numpy as np
from jax import lax
from jax.experimental import pallas as pl
from jax.experimental.pallas import tpu as pltpu
from jax.sharding import PartitionSpec as P

F32 = jnp.float32
VEL = [(a, b, c) for a in (-1, 0, 1) for b in (-1, 0, 1) for c in (-1, 0, 1)]
ROWS, LANES = 32, 128
CHUNK = 8


def shape_of(*dims):
    return jax.ShapeDtypeStruct(dims, F32)


def iota(rows, axis):
    return lax.broadcasted_iota(jnp.int32, (rows, LANES), axis)


def chunk_at(v):
    return pl.ds(pl.multiple_of(v * CHUNK, CHUNK), CHUNK)


def roll_lanes(x, by):
    if isinstance(by, int):
        by = by % LANES
        if by == 0:
            return x
    return pltpu.roll(x, by, 1)


def forward_moments(values):
    out = list(values)
    for stride in (9, 3, 1):
        for i in range(27):
            if (i // stride) % 3 == 0:
                low, mid, high = out[i], out[i + stride], out[i + 2 * stride]
                both = low + high
                out[i] = both + 4.0 * mid
                out[i + stride] = high - low
                out[i + 2 * stride] = both
    return out


def plus(x, y):
    if x is None:
        return y
    return x if y is None else x + y


def minus(x, y):
    if y is None:
        return x
    return -y if x is None else x - y


def backward_moments(values):
    out = list(values)
    for stride in (9, 3, 1):
        for i in range(27):
            if (i // stride) % 3 == 0:
                m0, m1, m2 = out[i], out[i + stride], out[i + 2 * stride]
                out[i] = minus(m2, m1)
                out[i + stride] = minus(m0, m2)
                out[i + 2 * stride] = plus(m1, m2)
    return out


def collide(g, rate):
    m = forward_moments(g)
    rho = m[0]
    j = (m[9], m[3], m[1])
    square = [x * x * (1.0 / 72.0) for x in j]
    relaxed = [None] * 27
    for k in range(27):
        digits = (k // 9, (k // 3) % 3, k % 3)
        odd = [d for d in range(3) if digits[d] == 1]
        twos = [d for d in range(3) if digits[d] == 2]
        if k in (0, 9, 3, 1):
            continue
        if not odd:
            level = rho
            for d in twos:
                level = level + square[d]
        elif len(odd) == 1:
            level = j[odd[0]]
        elif len(odd) == 2:
            level = j[odd[0]] * j[odd[1]] * (1.0 / 216.0)
        else:
            level = None
        if level is not None and twos:
            level = level * (3.0 ** -len(twos))
        relaxed[k] = minus(m[k], level) * (rate(k) * (1.0 / 64.0))
    back = backward_moments(relaxed)
    post = []
    for i, c in enumerate(VEL):
        factor = 2.0 ** sum(abs(x) for x in c)
        post.append(g[i] - (back[i] if factor == 1.0 else factor * back[i]))
    return post, j


def grow_index():
    r, l = iota(CHUNK, 0), iota(CHUNK, 1)
    return (r // 4) % 2 * 64 + r % 2 * 32 + l // 32 * 8 + l % 16 // 2


def grow_row(row, index):
    return jnp.take_along_axis(jnp.broadcast_to(row, (CHUNK, LANES)), index, axis=1)


PER_BLOCK = 36
FIELDS = 4 * PER_BLOCK + 1


def fetch(sources, targets, sems, first=0):
    copies = [pltpu.make_async_copy(a, b, sems.at[first + i]) for i, (a, b) in enumerate(zip(sources, targets))]
    for copy in copies:
        copy.start()

    def ready():
        for copy in copies:
            copy.wait()

    return ready


def begin_kernel(
    info_in, levels_in, near_in, rates_in, pop, scal, old, new, out, up, down,
    pops, scals, olds, news, info, levels, near, rates, sems,
):
    ready = fetch((info_in, levels_in, near_in, rates_in), (info, levels, near, rates), sems, 7)
    copies = []
    for v in range(4):
        rows = pl.ds(32 * v, 32)
        copies.append(pltpu.make_async_copy(pop.at[:, rows, :], pops.at[:, rows, :], sems.at[v]))
    copies.append(pltpu.make_async_copy(old, olds, sems.at[4]))
    copies.append(pltpu.make_async_copy(new, news, sems.at[5]))
    copies.append(pltpu.make_async_copy(scal, scals, sems.at[6]))
    for copy in copies:
        copy.start()
    index = grow_index()
    ready()
    layer, core = info[0], info[1]
    row, lane = iota(CHUNK, 0), iota(CHUNK, 1)
    meta = jnp.zeros((CHUNK, LANES), F32)
    for b in range(4):
        for q in range(6):
            here = jnp.logical_and(row == b, lane == q + 8)
            meta = jnp.where(here, near[b, q].astype(F32), meta)
    out[FIELDS - 1, 0:8, :] = meta

    def fine_of(b):
        return levels[layer * 8 + core * 4 + b] == 1

    for v in range(4):
        copies[v].wait()

        @pl.loop(0, 4)
        def _(b):
            @pl.when(fine_of(b))
            def _():
                at = pl.ds(8 * v, 8)
                from_rows = pl.ds(32 * v + b, 8, stride=4)
                post, _j = collide([pops[p, from_rows, :] for p in range(27)], lambda k: rates[k])
                for p in range(27):
                    out[b * PER_BLOCK + p, at, :] = post[p]

    for copy in copies[4:]:
        copy.wait()

    @pl.loop(0, 4)
    def _(b):
        @pl.when(fine_of(b))
        def _():
            for m in range(9):
                for v in range(4):
                    out[b * PER_BLOCK + 27 + m, pl.ds(8 * v, 8), :] = scals[m, pl.ds(32 * v + b, 8, stride=4), :]

        @pl.when(jnp.logical_not(fine_of(b)))
        def _():
            for p in range(27):
                for v in range(4):
                    before = olds[p, pl.ds(4 * v + b, 1), :]
                    after = news[p, pl.ds(4 * v + b, 1), :]
                    out[b * PER_BLOCK + 27 + p // 8, pl.ds(p % 8 * 4 + v, 1), :] = 0.5 * (before + after)
                    out[b * PER_BLOCK + p, pl.ds(8 * v, 8), :] = grow_row(before, index)


    pack_faces(out, up, down, meta)


def pack_faces(out, up, down, meta=None):
    lane = iota(CHUNK, 1) % 16
    for v in range(4):
        at = pl.ds(8 * v, 8)
        for ref, digit, start in ((up, 2, 15), (down, 0, 0)):
            for b in range(4):
                fields = [out[b * PER_BLOCK + 3 * e + digit, at, :] for e in range(9)]
                fields += [out[b * PER_BLOCK + 27 + e, at, :] for e in range(7)]
                ref[b, at, :] = pack_into(fields, 0, start, lane)
            rest = pack_into([out[b * PER_BLOCK + 34 + e, at, :] for b in range(4) for e in range(2)], 0, start, lane)
            ref[4, at, :] = rest if meta is None else jnp.where(lane < 8, rest, meta)


def spot(block, core):
    return (block % 8) ^ (core * 4)


def y_up(own, beside, even, group):
    turned = jnp.where(even, pltpu.roll(beside, CHUNK - 1, 0), pltpu.roll(own, 1, 0))
    return roll_lanes(jnp.where(group < 7, own, turned), 16)


def y_down(own, beside, even, group):
    turned = jnp.where(even, pltpu.roll(own, CHUNK - 1, 0), pltpu.roll(beside, 1, 0))
    return roll_lanes(jnp.where(group > 0, own, turned), -16)


def chunks(ref, *lead):
    return [ref[(*lead, pl.ds(8 * v, 8), slice(None))] for v in range(4)]


def x_up(own, beyond, row):
    turned = [pltpu.roll(x, 2, 0) for x in own]
    before = [beyond] + turned[:3]
    return [jnp.where(row < 2, a, b) for a, b in zip(before, turned)]


def x_down(own, beyond, row):
    turned = [pltpu.roll(x, CHUNK - 2, 0) for x in own]
    after = turned[1:] + [beyond]
    return [jnp.where(row >= 6, a, b) for a, b in zip(after, turned)]


def put(ref, lead, values):
    for v in range(4):
        ref[(*lead, pl.ds(8 * v, 8), slice(None))] = values[v]


def sections_xy(refs, faces, mid, dest, info, levels, near, ready):
    row = iota(CHUNK, 0)
    even = row % 2 == 0
    group = iota(CHUNK, 1) // 16

    for half, ref in enumerate(refs):

        @pl.loop(0, 4)
        def _(i):
            for p, c in enumerate(VEL):
                if c[0] == 1:
                    faces[half * 4 + i, p] = pltpu.roll(ref[i * PER_BLOCK + p, pl.ds(24, 8), :], 2, 0)
                elif c[0] == -1:
                    faces[half * 4 + i, p] = pltpu.roll(ref[i * PER_BLOCK + p, pl.ds(0, 8), :], CHUNK - 2, 0)

    ready()
    core = info[1]
    fine_of = fine_in(info, levels)

    for half, ref in enumerate(refs):

        @pl.loop(0, 4)
        def _(i):
            b = half * 4 + i
            fine = fine_of(b)
            fields = [p for p in range(27) if half == 0 or VEL[p][1] != 0]

            @pl.when(fine)
            def _():
                low, high = spot(near[b, 0], core), spot(near[b, 1], core)
                for p in fields:
                    values = chunks(ref, i * PER_BLOCK + p)
                    if VEL[p][0] == 1:
                        values = x_up(values, faces[low, p], row)
                    elif VEL[p][0] == -1:
                        values = x_down(values, faces[high, p], row)
                    put(mid, (b, p), values)

            @pl.when(jnp.logical_not(fine))
            def _():
                for p in fields:
                    if VEL[p][1] != 0:
                        put(mid, (b, p), chunks(ref, i * PER_BLOCK + p))

    @pl.loop(0, 4)
    def _(b):
        @pl.when(fine_of(b))
        def _():
            low, high = spot(near[b, 2], core), spot(near[b, 3], core)
            for p, c in enumerate(VEL):
                for v in range(4):
                    at = pl.ds(8 * v, 8)
                    value = mid[b, p, at, :]
                    if c[1] == 1:
                        value = y_up(value, mid[low, p, at, :], even, group)
                    elif c[1] == -1:
                        value = y_down(value, mid[high, p, at, :], even, group)
                    dest[b, p, at, :] = value


def pack_into(fields, first_slot, start, lane):
    parts = [(first_slot + e, roll_lanes(field, first_slot + e - start)) for e, field in enumerate(fields)]
    while len(parts) > 1:
        joined = []
        for k in range(0, len(parts) - 1, 2):
            slot = parts[k + 1][0]
            joined.append((parts[k][0], jnp.where(lane < slot, parts[k][1], parts[k + 1][1])))
        parts = joined + parts[len(parts) - len(parts) % 2:]
    return parts[0][1]


def fine_in(info, levels):
    return lambda b: levels[info[0] * 8 + spot(b, info[1])] == 1


def plane_kernel(
    info_in, levels_in, diffusivity_in, stoichiometry_in, own, other, dest, table, parts,
    mid, faces, old, info, levels, near, diffusivity, stoichiometry, sems,
):
    row = iota(CHUNK, 0)
    both = jnp.where(row < 4, own[FIELDS - 1, 0:8, :], pltpu.roll(other[FIELDS - 1, 0:8, :], 4, 0))
    table[...] = roll_lanes(both, -8).astype(jnp.int32)
    ready = fetch(
        (info_in, levels_in, table, diffusivity_in, stoichiometry_in), (info, levels, near, diffusivity, stoichiometry), sems
    )
    gather_species((own, other), old)
    sections_xy((own, other), faces, mid, dest, info, levels, near, ready)
    species_begin(old, parts, info, levels, near, diffusivity, stoichiometry)


def settle(incoming, raw):
    for way in range(2):
        for half in range(2):
            for i in range(4):
                put(raw, (way, half * 4 + i), chunks(incoming[way][half], i))


def arrive(info, levels, table, core, raw, mid, done):
    row, slot = iota(CHUNK, 0), iota(CHUNK, 1) % 16
    even, group = row % 2 == 0, iota(CHUNK, 1) // 16
    x_plus, x_minus = jnp.logical_and(slot >= 6, slot < 9), slot < 3
    y_plus = jnp.logical_and(slot < 9, slot % 3 == 2)
    y_minus = jnp.logical_and(slot < 9, slot % 3 == 0)
    blocks = [(way, b) for way in range(2) for b in range(8)]
    fine = [levels[info[2 + way] * 8 + spot(b, core)] == 1 for way, b in blocks]

    def beside(way, b, q):
        return spot(table[b, 16 * way + 8 + q], core)

    for (way, b), flag in zip(blocks, fine):
        own = chunks(raw, way, b)
        before = x_up(own, pltpu.roll(raw[way, beside(way, b, 0), pl.ds(24, 8), :], 2, 0), row)
        after = x_down(own, pltpu.roll(raw[way, beside(way, b, 1), pl.ds(0, 8), :], CHUNK - 2, 0), row)
        to_plus, to_minus = jnp.logical_and(x_plus, flag), jnp.logical_and(x_minus, flag)
        put(mid, (way, b), [jnp.where(to_plus, x, jnp.where(to_minus, y, z)) for x, y, z in zip(before, after, own)])
    for (way, b), flag in zip(blocks, fine):
        low, high = beside(way, b, 2), beside(way, b, 3)
        to_plus, to_minus = jnp.logical_and(y_plus, flag), jnp.logical_and(y_minus, flag)
        for v in range(4):
            at = pl.ds(8 * v, 8)
            here = mid[way, b, at, :]
            before = y_up(here, mid[way, low, at, :], even, group)
            after = y_down(here, mid[way, high, at, :], even, group)
            done[way, b, at, :] = jnp.where(to_plus, before, jnp.where(to_minus, after, here))


def face_reader(done, rest, below, above):
    def faces(m, at):
        if m < 7:
            slot = 9 + m
            return roll_lanes(done[0, below, at, :], -slot), roll_lanes(done[1, above, at, :], 15 - slot)
        low = LANES - 2 * (below % 4) - (m - 7)
        high = (LANES + 15 - 2 * (above % 4) - (m - 7)) % LANES
        return pltpu.roll(rest[0, below // 4, at, :], low, 1), pltpu.roll(rest[1, above // 4, at, :], high, 1)

    return faces


def z_section(h, up, down, depth):
    g = []
    for p, c in enumerate(VEL):
        e = p // 3
        value = h(p)
        if c[2] == 1:
            value = jnp.where(depth == 0, roll_lanes(up, -e), roll_lanes(value, 1))
        elif c[2] == -1:
            value = jnp.where(depth == 15, roll_lanes(down, 15 - e), roll_lanes(value, -1))
        g.append(value)
    return g


def gather_species(halves, old):
    for half, ref_in in enumerate(halves):

        @pl.loop(0, 4)
        def _(i):
            for m in range(9):
                put(old, (half * 4 + i, m), chunks(ref_in, i * PER_BLOCK + 27 + m))


def species_begin(y_ref, parts, info, levels, near, diffusivity, stoichiometry):
    row, lanes = iota(CHUNK, 0), iota(CHUNK, 1)
    even = row % 2 == 0
    group, depth = lanes // 16, lanes % 16
    fine_of = fine_in(info, levels)

    @pl.loop(0, 4)
    def _(b):
        @pl.when(fine_of(b))
        def _():
            def gone(edge, q):
                return jnp.logical_and(edge, levels[near[b, q]] != 1)

            lost = [
                gone(row < 2, 0), gone(row >= 6, 1),
                gone(jnp.logical_and(even, group == 0), 2),
                gone(jnp.logical_and(jnp.logical_not(even), group == 7), 3),
            ]
            sides = [spot(near[b, q], info[1]) for q in range(4)]
            burning = [
                x * y * jnp.exp(4.0 * (t - 1.0))
                for x, y, t in zip(chunks(y_ref, b, 0), chunks(y_ref, b, 1), chunks(y_ref, b, 8))
            ]
            for m in range(9):
                y = chunks(y_ref, b, m)
                low_x = pltpu.roll(y_ref[sides[0], m, pl.ds(24, 8), :], 2, 0)
                high_x = pltpu.roll(y_ref[sides[1], m, pl.ds(0, 8), :], CHUNK - 2, 0)
                lower_x, upper_x = x_up(y, low_x, row), x_down(y, high_x, row)
                lower_x[0] = jnp.where(lost[0], y[0], lower_x[0])
                upper_x[3] = jnp.where(lost[1], y[3], upper_x[3])
                for v in range(4):
                    at = pl.ds(8 * v, 8)
                    here = y[v]
                    pairs = [
                        (lower_x[v], upper_x[v]),
                        (
                            jnp.where(lost[2], here, y_up(here, y_ref[sides[2], m, at, :], even, group)),
                            jnp.where(lost[3], here, y_down(here, y_ref[sides[3], m, at, :], even, group)),
                        ),
                        (
                            jnp.where(depth == 0, here, roll_lanes(here, 1)),
                            jnp.where(depth == 15, here, roll_lanes(here, -1)),
                        ),
                    ]
                    spread = None
                    for d, (lower, upper) in enumerate(pairs):
                        parts[b * PER_BLOCK + 9 + 9 * d + m, at, :] = upper - lower
                        both = upper + lower
                        spread = both if spread is None else spread + both
                    parts[b * PER_BLOCK + m, at, :] = (
                        here + diffusivity[m] * (spread - 6.0 * here) + stoichiometry[m] * burning[v]
                    )


def species_end(parts, b, y_of, faces, flux, flags, diffusivity, store):
    depth = iota(CHUNK, 1) % 16
    at_low = jnp.logical_and(depth == 0, flags[0] == 1)
    at_high = jnp.logical_and(depth == 15, flags[1] == 1)
    for v in range(4):
        at = pl.ds(8 * v, 8)
        flow = [flux[d, at, :] for d in range(3)]
        for m in range(9):
            here = y_of(m, at)
            low, high = faces(m, at)
            low = jnp.where(at_low, low - here, 0.0)
            high = jnp.where(at_high, high - here, 0.0)
            base, along_x, along_y, along_z = (parts[b * PER_BLOCK + 9 * kind + m, at, :] for kind in range(4))
            drift = flow[0] * along_x + flow[1] * along_y + flow[2] * (along_z + (high - low))
            store(m, v, base - drift + diffusivity[m] * (low + high))


WIDE = 640


def reduce_tables():
    l = np.arange(LANES)[:, None]
    c = np.arange(WIDE)[None, :]
    e, cell = c // 64, c % 64
    live = c < 576
    along_x = (l // 32 * 8 + l % 16 // 2 == cell % 32) & live
    along_y = [(l // 16 + 8 * a == e) & (l % 16 // 2 == cell % 8) & live for a in range(2)]
    along_z = (l % 16 == e) & (l // 32 == cell % 4) & live
    side = np.concatenate([along_x, along_y[0], along_y[1]], axis=0)
    return jnp.asarray(side, jnp.bfloat16), jnp.asarray(along_z, jnp.bfloat16)


def wide_iota(axis):
    return lax.broadcasted_iota(jnp.int32, (ROWS, WIDE), axis)


def times(x, w):
    total = None
    for _ in range(3):
        part = x.astype(jnp.bfloat16)
        x = x - part.astype(F32)
        product = jnp.dot(part, w, preferred_element_type=F32)
        total = product if total is None else total + product
    return total


def column_sums(spread, k, keep):
    return jnp.sum(jnp.where(keep, spread[pl.ds(k * ROWS, ROWS), :], 0.0), axis=0, keepdims=True)


def put_pair(out, s, base, first, second):
    moved = pltpu.roll(second, 64, 1)
    out[pl.ds(s, 1), pl.ds(base, 512)] = first[:, 0:512]
    out[pl.ds(s, 1), pl.ds(base + 512, 128)] = first[:, 512:640] + moved[:, 0:128]
    out[pl.ds(s, 1), pl.ds(base + 640, 512)] = moved[:, 128:640]


def middle_kernel(
    info_in, levels_in, near_in, rates_in, diffusivity_in, own, held, parts, up_own, up_other, down_own, down_other,
    out, up, down, table,
    raw, mid, done, rest, flux, moved,
    info, levels, near, rates, diffusivity, far, sems,
):
    index = grow_index()
    incoming = ((up_own, up_other), (down_own, down_other))
    row, lane = iota(CHUNK, 0), iota(CHUNK, 1)
    below, above = [
        jnp.where(row < 4, one[4, pl.ds(0, 8), :], pltpu.roll(two[4, pl.ds(0, 8), :], 4, 0)) for one, two in incoming
    ]
    table[...] = jnp.where(lane < 16, below, roll_lanes(above, 16)).astype(jnp.int32)
    ready = fetch(
        (info_in, levels_in, near_in, rates_in, diffusivity_in, table),
        (info, levels, near, rates, diffusivity, far),
        sems,
    )
    settle(incoming, raw)
    for way in range(2):
        for half in range(2):
            put(rest, (way, half), chunks(incoming[way][half], 4))

    ready()
    core = info[1]
    fine_of = fine_in(info, levels)
    arrive(info, levels, far, core, raw, mid, done)

    @pl.loop(0, 4)
    def _(b):
        @pl.when(fine_of(b))
        def _():
            below, above = spot(near[b, 4], core), spot(near[b, 5], core)

            for v in range(4):
                at = pl.ds(8 * v, 8)
                g = z_section(lambda p: held[b, p, at, :], done[0, below, at, :], done[1, above, at, :], depth_of())
                for p in range(27):
                    moved[p, at, :] = g[p]

            @pl.loop(0, 4)
            def _(v):
                at = chunk_at(v)
                post, j = collide([moved[p, at, :] for p in range(27)], lambda k: rates[k])
                for p in range(27):
                    out[b * PER_BLOCK + p, at, :] = post[p]
                for d in range(3):
                    flux[d, at, :] = j[d] * (0.5 / 216.0)

            def store(m, v, value):
                out[b * PER_BLOCK + 27 + m, pl.ds(8 * v, 8), :] = value

            species_end(
                parts, b, lambda m, at: own[b * PER_BLOCK + 27 + m, at, :], face_reader(done, rest, below, above), flux,
                [levels[near[b, q]] for q in (4, 5)], diffusivity, store,
            )

        @pl.when(jnp.logical_not(fine_of(b)))
        def _():
            for p in range(27):
                for v in range(4):
                    line = own[b * PER_BLOCK + 27 + p // 8, pl.ds(p % 8 * 4 + v, 1), :]
                    out[b * PER_BLOCK + p, pl.ds(8 * v, 8), :] = grow_row(line, index)
            for m in range(9):
                put(out, (b * PER_BLOCK + 27 + m,), [jnp.zeros((CHUNK, LANES), F32)] * 4)

    pack_faces(out, up, down)


def depth_of():
    return iota(CHUNK, 1) % 16


def second_plane_kernel(
    info_in, levels_in, near_in, diffusivity_in, stoichiometry_in, own, other, own_before, other_before, tables,
    dest, sides_out, parts,
    mid, faces, old, edge_x, edge_y, needed, picked_x, picked_y, spread,
    info, levels, near, diffusivity, stoichiometry, sems,
):
    ready = fetch(
        (info_in, levels_in, near_in, diffusivity_in, stoichiometry_in), (info, levels, near, diffusivity, stoichiometry), sems
    )
    gather_species((own, other), old)
    sections_xy((own, other), faces, mid, dest, info, levels, near, ready)
    species_begin(old, parts, info, levels, near, diffusivity, stoichiometry)
    core = info[1]
    fine_of = fine_in(info, levels)
    for b in range(8):
        needed[b] = 0
    for s in range(4):
        for q in range(4):

            @pl.when(jnp.logical_not(fine_of(s)))
            def _(s=s, q=q):
                needed[spot(near[s, q], core)] = 1

    group, odd = iota(CHUNK, 1) // 16, iota(CHUNK, 0) % 2 == 1
    for half, (one, two) in enumerate(((own_before, own), (other_before, other))):

        @pl.loop(0, 4)
        def _(i):
            b = half * 4 + i

            def total(p, at):
                return one[i * PER_BLOCK + p, at, :] + two[i * PER_BLOCK + p, at, :]

            @pl.when(jnp.logical_and(fine_of(b), needed[b] == 1))
            def _():
                for side in range(2):
                    at = pl.ds(30, 2) if side == 0 else pl.ds(0, 2)
                    for e in range(9):
                        edge_x[b, side, pl.ds(2 * e, 2), :] = total(18 + e if side == 0 else e, at)
                    edge_x[b, side, pl.ds(18, 14), :] = jnp.zeros((14, LANES), F32)
                for v in range(4):
                    at = pl.ds(8 * v, 8)
                    packs = [None, None]
                    for e in range(9):
                        p_low = 9 * (e // 3) + e % 3
                        slot = e % 8
                        high = roll_lanes(total(p_low + 6, at), 16 * (slot - 7))
                        both = jnp.where(odd, high, roll_lanes(total(p_low, at), 16 * slot))
                        held_pack = packs[e // 8]
                        packs[e // 8] = both if held_pack is None else jnp.where(group == slot, both, held_pack)
                    for a in range(2):
                        edge_y[b, a, at, :] = packs[a]

    row, col = wide_iota(0), wide_iota(1)
    e_of, cell = col // 64, col % 64
    keep_x = jnp.logical_and(row // 2 == e_of, row % 2 == cell // 32)
    keep_y = row // 4 == cell // 8
    odd_row = row % 2 == 1
    any_coarse = jnp.logical_not(jnp.logical_and(jnp.logical_and(fine_of(0), fine_of(1)), jnp.logical_and(fine_of(2), fine_of(3))))
    sides_out[...] = jnp.zeros((4, 2304), F32)

    @pl.when(any_coarse)
    def _():
        for q in range(4):
            for s in range(4):
                live = jnp.logical_and(jnp.logical_not(fine_of(s)), levels[near[s, q]] == 1)
                m = spot(near[s, q], core)
                rows = pl.ds((q % 2 * 4 + s) * ROWS, ROWS)
                if q < 2:
                    picked_x[rows, :] = jnp.where(live, 0.125 * edge_x[m, q], 0.0)
                else:
                    for a in range(2):
                        picked_y[rows, pl.ds(a * LANES, LANES)] = jnp.where(live, 0.125 * edge_y[m, a], 0.0)
        for pair, picked, weights in ((0, picked_x, tables[0:128, :]), (1, picked_y, tables[128:384, :])):
            spread[...] = times(picked[...], weights)
            for s in range(4):
                keeps = (keep_x, keep_x)
                if pair:
                    keeps = (jnp.logical_and(keep_y, odd_row), jnp.logical_and(keep_y, jnp.logical_not(odd_row)))
                put_pair(
                    sides_out, s, pair * 1152,
                    column_sums(spread, s, keeps[0]), column_sums(spread, 4 + s, keeps[1]),
                )


def end_kernel(
    info_in, levels_in, near_in, far_in, diffusivity_in, held, own, parts,
    up_own, up_other, down_own, down_other, up_own_before, up_other_before, down_own_before, down_other_before,
    sides, weights, pop, scal,
    pop_out, scal_out, returned_out,
    raw, mid, done, rest, before, pops, scals, returned, flux, picked, spread,
    info, levels, near, far, diffusivity, sems,
):
    ready = fetch(
        (info_in, levels_in, near_in, far_in, diffusivity_in), (info, levels, near, far, diffusivity), sems, 6
    )
    incoming = ((up_own, up_other), (down_own, down_other))
    for way in range(2):
        for half in range(2):
            put(rest, (way, half), chunks(incoming[way][half], 4))
    settle(((up_own_before, up_other_before), (down_own_before, down_other_before)), before)
    settle(incoming, raw)
    ready()
    core = info[1]
    fine_of = fine_in(info, levels)
    arrive(info, levels, far, core, raw, mid, done)
    depth = iota(CHUNK, 1) % 16
    row, col = wide_iota(0), wide_iota(1)
    keep = row // 4 * 2 + row % 2 == col % 64 // 4
    @pl.loop(0, 4)
    def _(s):
        below, above = spot(near[s, 4], core), spot(near[s, 5], core)

        @pl.when(fine_of(s))
        def _():
            for v in range(4):
                at = pl.ds(8 * v, 8)
                g = z_section(lambda p: held[s, p, at, :], done[0, below, at, :], done[1, above, at, :], depth)
                for p in range(27):
                    pops[p, pl.ds(32 * v + s, 8, stride=4), :] = g[p]
                m = forward_moments(g)
                for d, i in enumerate((9, 3, 1)):
                    flux[s, d, at, :] = m[i] * (0.5 / 216.0)

        @pl.when(jnp.logical_not(fine_of(s)))
        def _():
            for v in range(4):
                rows = pl.ds(32 * v + s, 8, stride=4)
                for p in range(27):
                    pops[p, rows, :] = pop[p, rows, :]

    copies = [pltpu.make_async_copy(pops, pop_out, sems.at[0])]
    copies[-1].start()

    @pl.loop(0, 4)
    def _(s):
        @pl.when(fine_of(s))
        def _():
            def store(m, v, value):
                scals[m, pl.ds(32 * v + s, 8, stride=4), :] = value

            species_end(
                parts, s, lambda m, at: own[s * PER_BLOCK + 27 + m, at, :],
                face_reader(done, rest, spot(near[s, 4], core), spot(near[s, 5], core)), flux.at[s],
                [levels[near[s, q]] for q in (4, 5)], diffusivity, store,
            )

        @pl.when(jnp.logical_not(fine_of(s)))
        def _():
            for v in range(4):
                at = pl.ds(32 * v + s, 8, stride=4)
                for m in range(9):
                    scals[m, at, :] = scal[m, at, :]

    copies.append(pltpu.make_async_copy(scals, scal_out, sems.at[4]))
    copies[-1].start()

    returned[:, 0:2304] = sides[...]
    returned[:, 2304:3456] = jnp.zeros((4, 1152), F32)
    any_coarse = jnp.logical_not(jnp.logical_and(jnp.logical_and(fine_of(0), fine_of(1)), jnp.logical_and(fine_of(2), fine_of(3))))

    @pl.when(any_coarse)
    def _():
        for way in range(2):
            for s in range(4):
                m = spot(near[s, 4 + way], core)
                live = jnp.logical_and(jnp.logical_not(fine_of(s)), levels[near[s, 4 + way]] == 1)
                face = jnp.where(live, 0.125 * (before[way, m] + raw[way, m]), 0.0)
                picked[pl.ds((way * 4 + s) * ROWS, ROWS), :] = face
        spread[...] = times(picked[...], weights[...])
        for s in range(4):
            put_pair(returned, s, 2304, column_sums(spread, s, keep), column_sums(spread, 4 + s, keep))

    copies.append(pltpu.make_async_copy(returned, returned_out, sems.at[5]))
    copies[-1].start()

    for copy in copies:
        copy.wait()


def specs(kinds):
    table = {
        "s": pl.BlockSpec(memory_space=pltpu.SMEM),
        "v": pl.BlockSpec(memory_space=pltpu.VMEM),
        "h": pl.BlockSpec(memory_space=pltpu.HBM),
        "a": pl.BlockSpec(memory_space=pl.ANY),
    }
    return [table[kind] for kind in kinds]


def call(kernel, kinds, outs, out_kinds, scratch, name, megabytes, flops):
    return pl.pallas_call(
        kernel,
        in_specs=specs(kinds),
        out_specs=specs(out_kinds),
        out_shape=outs,
        scratch_shapes=scratch,
        name=name,
        compiler_params=pltpu.CompilerParams(vmem_limit_bytes=megabytes << 20),
        cost_estimate=pl.CostEstimate(flops=flops, transcendentals=0, bytes_accessed=8 << 20),
    )


def interleave(x):
    blocks, n, cells = x.shape
    x = x.reshape(blocks, n, cells // LANES, LANES)
    return jnp.transpose(x, (1, 2, 0, 3)).reshape(n, cells // LANES * blocks, LANES)


def separate(x):
    n, rows, _ = x.shape
    x = jnp.transpose(x.reshape(n, rows // 4, 4, LANES), (2, 0, 1, 3))
    return x.reshape(4, n, rows // 4 * LANES)


def local(
    populations, scalars, coarse_old, coarse_new, levels, neighbours, relax_rates, diffusivity, stoichiometry
):
    devices = lax.axis_size("blk")
    me = lax.axis_index("blk")
    layer, layers = me // 2, devices // 2
    info = jnp.stack([layer, me % 2, (layer + layers - 1) % layers, (layer + 1) % layers]).astype(jnp.int32)
    swap = [(i, i ^ 1) for i in range(devices)]
    rise = [(i, (i + 2) % devices) for i in range(devices)]
    fall = [(i, (i - 2) % devices) for i in range(devices)]

    def move(x, pairs):
        return lax.ppermute(x, "blk", pairs)

    def vmem(*lead):
        return pltpu.VMEM((*lead, ROWS, LANES), F32)

    full = (ROWS, LANES)
    pop, scal = interleave(populations), interleave(scalars)
    old, new = interleave(coarse_old), interleave(coarse_new)
    side_table, z_table = reduce_tables()
    fields = FIELDS - 1
    semaphores = pltpu.SemaphoreType.DMA
    own, up, down = call(
        begin_kernel,
        "ahhhhhhh",
        [shape_of(FIELDS, *full), shape_of(5, *full), shape_of(5, *full)],
        "vvv",
        [pltpu.VMEM(x.shape, F32) for x in (pop, scal, old, new)]
        + [pltpu.SMEM(x.shape, x.dtype) for x in (info, levels, neighbours, relax_rates)]
        + [semaphores((11,))],
        "begin",
        12,
        1 << 27,
    )(info, *[pltpu.with_memory_space_constraint(x, pltpu.HBM) for x in (levels, neighbours, relax_rates, pop, scal, old, new)])
    other = move(own, swap)
    up, down = move(up, rise), move(down, fall)
    face = pltpu.VMEM((8, 27, CHUNK, LANES), F32)
    table_shape = jax.ShapeDtypeStruct((CHUNK, LANES), jnp.int32)

    def smem(*arrays):
        return [pltpu.SMEM(x.shape, x.dtype) for x in arrays]

    held, near, parts = call(
        plane_kernel,
        "aaaavv",
        [shape_of(4, 27, *full), table_shape, shape_of(4 * PER_BLOCK, *full)],
        "vvv",
        [vmem(8, 27), face, vmem(8, 9)]
        + smem(info, levels, table_shape, diffusivity, stoichiometry) + [semaphores((5,))],
        "plane",
        12,
        1 << 27,
    )(info, levels, diffusivity, stoichiometry, own, other)
    held, up = lax.optimization_barrier((held, up))
    held, down = lax.optimization_barrier((held, down))
    arrived = (up, move(up, swap), down, move(down, swap))
    landing = [vmem(2, 8), vmem(2, 8), vmem(2, 8), vmem(2, 2)]
    own_next, up_next, down_next, table = call(
        middle_kernel,
        "aaaaavvvvvvv",
        [shape_of(fields, *full), shape_of(5, *full), shape_of(5, *full), table_shape],
        "vvvv",
        landing
        + [vmem(3), vmem(27)]
        + smem(info, levels, table_shape, relax_rates, diffusivity, table_shape)
        + [semaphores((6,))],
        "middle",
        14,
        1 << 28,
    )(
        info, levels, near, relax_rates, diffusivity, own, held, parts, *arrived
    )
    other_next = move(own_next, swap)
    up, down = move(up_next, rise), move(down_next, fall)
    held, sides, parts = call(
        second_plane_kernel,
        "aaaaavvvvv",
        [shape_of(4, 27, *full), shape_of(4, 2304), shape_of(4 * PER_BLOCK, *full)],
        "vvv",
        [vmem(8, 27), face, vmem(8, 9), vmem(8, 2), vmem(8, 2), pltpu.SMEM((8,), jnp.int32)]
        + [pltpu.VMEM((8 * ROWS, LANES), F32), pltpu.VMEM((8 * ROWS, 2 * LANES), F32), pltpu.VMEM((8 * ROWS, WIDE), F32)]
        + smem(info, levels, table_shape, diffusivity, stoichiometry) + [semaphores((5,))],
        "plane2",
        14,
        1 << 27,
    )(info, levels, near, diffusivity, stoichiometry, own_next, other_next, own, other, side_table)
    held, sides, up = lax.optimization_barrier((held, sides, up))
    held, sides, down = lax.optimization_barrier((held, sides, down))
    pop_out, scal_out, returned = call(
        end_kernel,
        "aaaaa" + "v" * 15,
        [shape_of(27, 128, LANES), shape_of(9, 128, LANES), shape_of(4, 3456)],
        "hhh",
        landing
        + [vmem(2, 8), pltpu.VMEM(pop.shape, F32), pltpu.VMEM(scal.shape, F32)]
        + [pltpu.VMEM((4, 3456), F32), vmem(4, 3)]
        + [pltpu.VMEM((8 * ROWS, LANES), F32), pltpu.VMEM((8 * ROWS, WIDE), F32)]
        + smem(info, levels, table_shape, table_shape, diffusivity) + [semaphores((11,))],
        "end",
        16,
        1 << 27,
    )(
        info, levels, near, table, diffusivity, held, own_next, parts,
        up, move(up, swap), down, move(down, swap), *arrived, sides, z_table, pop, scal,
    )
    return separate(pop_out), separate(scal_out), returned


def solution(mesh):
    in_specs = (
        P("blk", None, None), P("blk", None, None), P("blk", None, None), P("blk", None, None),
        P(), P("blk", None), P(), P(), P(),
    )
    out_specs = (P("blk", None, None), P("blk", None, None), P("blk", None))
    return jax.shard_map(local, mesh=mesh, in_specs=in_specs, out_specs=out_specs, check_vma=False)
```
